32 devices in a mesh: rows: 8 (over y, x, core), seq: 4 (over z).
Axes of the slice: x: 2, y: 2, z: 4, core: 2. Of those that a mesh axis runs over, the one named last changes fastest.
Arguments:
- tokens: bfloat16 [8, 1024, 512], P('rows', 'seq'), may hold values from -6 to 6
- segment_ids: int32 [8, 1024], P('rows', 'seq'), may hold values from 0 to 3, as said below
- prenorm_gain: float32 [512], replicated, may hold values from 0.5 to 1.5
- prenorm_shift: float32 [512], replicated, may hold values from -3 to 3
- query_proj: bfloat16 [512, 512], replicated, may hold values from -1 to 1
- query_bias: float32 [512], replicated, may hold values from -3 to 3
- key_proj: bfloat16 [512, 512], replicated, may hold values from -1 to 1
- value_proj: bfloat16 [512, 512], replicated, may hold values from -0.25 to 0.25
- value_bias: float32 [512], replicated, may hold values from -3 to 3
- output_proj: bfloat16 [512, 512], replicated, may hold values from -1 to 1
- output_bias: float32 [512], replicated, may hold values from -3 to 3
- midnorm_gain: float32 [512], replicated, may hold values from 0.5 to 1.5
- midnorm_shift: float32 [512], replicated, may hold values from -3 to 3
- inner_proj: bfloat16 [512, 2048], replicated, may hold values from -0.25 to 0.25
- inner_bias: float32 [2048], replicated, may hold values from -3 to 3
- outer_proj: bfloat16 [2048, 512], replicated, may hold values from -0.125 to 0.125
- outer_bias: float32 [512], replicated, may hold values from -3 to 3
- upstream: bfloat16 [8, 1024, 512], P('rows', 'seq'), may hold values from -6 to 6
Outputs:
- layer_output: bfloat16 [8, 1024, 512], P('rows', 'seq')
- input_grad: bfloat16 [8, 1024, 512], P('rows', 'seq')
- prenorm_gain_gradient: float32 [512], replicated
- prenorm_shift_gradient: float32 [512], replicated
- query_grad: float32 [512, 512], replicated
- querybias_grad: float32 [512], replicated
- key_grad: float32 [512, 512], replicated
- value_grad: float32 [512, 512], replicated
- valuebias_grad: float32 [512], replicated
- output_grad: float32 [512, 512], replicated
- outputbias_grad: float32 [512], replicated
- midgain_grad: float32 [512], replicated
- midshift_grad: float32 [512], replicated
- inner_grad: float32 [512, 2048], replicated
- innerbias_grad: float32 [2048], replicated
- outer_grad: float32 [2048, 512], replicated
- outerbias_grad: float32 [512], replicated
The draws below stay inside these ranges and needn't reach their ends.
Inputs may be any that keep to these rules, and one draw needn't show every extreme that they name: `segment_ids`: in each row the ids never fall until a tail of 1 to 128 padding positions with id 0; the last position before the tail has id 3.
All inputs are finite; a program needn't handle non-finite values.
Results may differ from the reference program's by a relative error of at most 0.011.
Values may be sent and summed in bfloat16 or wider, within the bound.
A program may use at most 128 MiB of HBM per device.

```python
import math
import jax
import jax.numpy as jnp
from jax import lax

D = 512
HEADS = 8
HEAD_DIM = 64
FF = 2048
NR = 16
SEGS = 3
ROWS = 8
LEN = 1024


def draw_segment_ids(key, part):
    key_pad, key_cut = jax.random.split(jax.random.fold_in(key, 17))
    padding = jax.random.randint(key_pad, (ROWS, 1), 1, LEN // 8 + 1)
    cuts = jax.random.randint(key_cut, (ROWS, SEGS - 1), 1, LEN - LEN // 8)
    positions = jnp.arange(LEN, dtype=jnp.int32)[None, :]
    passed = jnp.sum((positions[:, :, None] >= cuts[:, None, :]).astype(jnp.int32), axis=2)
    labels = 1 + passed
    return jnp.where(positions >= LEN - padding, 0, labels).astype(jnp.int32)


def draw_tokens(key, part):
    key_anchor, key_jitter = jax.random.split(jax.random.fold_in(key, 23))
    spacing = 4 * NR
    anchor_count = LEN // spacing + 2
    anchors = jax.random.truncated_normal(key_anchor, -3.0, 3.0, (ROWS, anchor_count, D), jnp.float32)
    jitter = 0.5 * jax.random.truncated_normal(key_jitter, -4.0, 4.0, (ROWS, LEN, D), jnp.float32)
    positions = jnp.arange(LEN, dtype=jnp.int32)
    anchor_index = (positions // spacing).astype(jnp.int32)
    fraction = (positions % spacing).astype(jnp.float32) / spacing
    anchor_low = jnp.take(anchors, anchor_index, axis=1)
    anchor_high = jnp.take(anchors, anchor_index + 1, axis=1)
    smooth = anchor_low + fraction[None, :, None] * (anchor_high - anchor_low)
    return jnp.clip(smooth + jitter, -6.0, 6.0).astype(jnp.bfloat16)


def paired_projections(key):
    key_shared, key_private = jax.random.split(jax.random.fold_in(key, 41))
    shared = jax.random.truncated_normal(key_shared, -4.0, 4.0, (D, D), jnp.float32)
    private = jax.random.truncated_normal(key_private, -4.0, 4.0, (D, D), jnp.float32)
    factor = 1.0 / math.sqrt(D)
    query_part = jnp.clip(shared * factor, -1.0, 1.0)
    key_part = jnp.clip((0.8 * shared + 0.6 * private) * factor, -1.0, 1.0)
    return (query_part, key_part)


def draw_query_proj(key, part):
    return paired_projections(key)[0].astype(jnp.bfloat16)


def draw_key_proj(key, part):
    return paired_projections(key)[1].astype(jnp.bfloat16)


def levels(rng, dims, pieces, least, top_value):
    loudness, own = 1.0, jax.random.fold_in(rng, 6)
    for axis_at, parts in pieces:
        steps = jnp.exp(jax.random.uniform(jax.random.fold_in(own, axis_at), (parts,), jnp.float32, least / len(pieces), top_value / len(pieces)))
        loudness = loudness * jnp.repeat(steps, dims[axis_at] // parts).reshape([-1 if axis == axis_at else 1 for axis in range(len(dims))])
    return loudness


def noise(key, dims, width, most, cuts=(), kind=jnp.bfloat16):
    values = width * jax.random.normal(key, dims, jnp.float32)
    if cuts:
        values = values * levels(key, dims, cuts, -0.22, 0.18)
    return jnp.clip(values, -most, most).astype(kind)


def setup_inputs(seed: int = 0) -> dict:
    seeds = jax.random.split(jax.random.key(seed), 19)
    tokens = draw_tokens(jax.random.fold_in(seeds[18], 71), 0)
    segment_ids = draw_segment_ids(jax.random.fold_in(seeds[18], 71), 0)
    prenorm_gain = jnp.clip(1.0 + 0.1 * jax.random.normal(seeds[2], (D,), jnp.float32), 0.5, 1.5)
    prenorm_shift = noise(seeds[3], (D,), 0.5, 3.0, (), jnp.float32)
    query_proj = draw_query_proj(jax.random.fold_in(seeds[18], 71), 0)
    query_bias = noise(seeds[5], (D,), 0.5, 3.0, (), jnp.float32)
    key_proj = draw_key_proj(jax.random.fold_in(seeds[18], 71), 0)
    value_proj = noise(seeds[7], (D, D), D ** -0.5, 0.25)
    value_bias = noise(seeds[8], (D,), 0.5, 3.0, (), jnp.float32)
    output_proj = noise(seeds[9], (D, D), (D // 16) ** -0.5, 1.0)
    output_bias = noise(seeds[10], (D,), 0.5, 3.0, (), jnp.float32)
    midnorm_gain = jnp.clip(1.0 + 0.1 * jax.random.normal(seeds[11], (D,), jnp.float32), 0.5, 1.5)
    midnorm_shift = noise(seeds[12], (D,), 0.5, 3.0, (), jnp.float32)
    inner_proj = noise(seeds[13], (D, FF), D ** -0.5, 0.25)
    inner_bias = noise(seeds[14], (FF,), 0.5, 3.0, (), jnp.float32)
    outer_proj = noise(seeds[15], (FF, D), FF ** -0.5, 0.125)
    outer_bias = noise(seeds[16], (D,), 0.5, 3.0, (), jnp.float32)
    upstream = noise(seeds[17], (ROWS, LEN, D), 1.0, 6.0, ((0, 8), (1, 4)))
    return dict(tokens=tokens, segment_ids=segment_ids, prenorm_gain=prenorm_gain, prenorm_shift=prenorm_shift, query_proj=query_proj, query_bias=query_bias, key_proj=key_proj, value_proj=value_proj, value_bias=value_bias, output_proj=output_proj, output_bias=output_bias, midnorm_gain=midnorm_gain, midnorm_shift=midnorm_shift, inner_proj=inner_proj, inner_bias=inner_bias, outer_proj=outer_proj, outer_bias=outer_bias, upstream=upstream)


LOG_TWO = math.log(2.0)
EPSILON = 1e-05
HIGHEST = lax.Precision.HIGHEST

@jax.custom_vjp
def low(v):
    return lax.optimization_barrier(v.astype(jnp.bfloat16)).astype(jnp.float32)

@jax.custom_vjp
def low_back(v):
    return v

def low_keep(v):
    return (low(v), None)

def low_pass(kept, grad):
    return (grad,)

def back_keep(v):
    return (v, None)

def back_low(kept, grad):
    return (low(grad),)
low.defvjp(low_keep, low_pass)
low_back.defvjp(back_keep, back_low)

def normalize(values, gain, shift):
    center = values - lax.optimization_barrier(jnp.mean(values, axis=-1, keepdims=True))
    spread = lax.optimization_barrier(jnp.mean(center * center, axis=-1, keepdims=True))
    return center * lax.rsqrt(spread + EPSILON) * gain + shift

def windows_of(coarse, count):
    padded = jnp.pad(coarse, ((NR, NR), (0, 0)))
    window_width = coarse.shape[1]
    before = padded[:count * NR].reshape(count, NR, window_width)
    middle = padded[NR:NR + count * NR].reshape(count, NR, window_width)
    after = padded[2 * NR:2 * NR + count * NR].reshape(count, NR, window_width)
    return jnp.concatenate([before, middle, after], axis=1)

def level_mask(level, segments, coarse_ids, length):
    block = NR * 2 ** level
    coarse_count = coarse_ids.shape[0]
    positions = jnp.arange(length, dtype=jnp.int32)
    offsets = jnp.arange(3 * NR, dtype=jnp.int32)
    key_index = (positions // block - 1)[:, None] * NR + offsets[None, :]
    valid = (key_index >= 0) & (key_index < coarse_count)
    key_ids = jnp.take(coarse_ids, jnp.clip(key_index, 0, coarse_count - 1))
    mask = valid & (key_ids == segments[:, None])
    if level > 0:
        distant = jnp.abs(key_index // (NR // 2) - (positions // (block // 2))[:, None]) > 1
        mask = mask & (key_ids != 0) & distant
    return mask

def row_forward(params, row_tokens, segments):
    pre_gain, pre_shift, query_proj, query_bias, key_proj, value_proj, value_bias, output_proj, output_bias, mid_gain, mid_shift, inner_proj, inner_bias, outer_proj, outer_bias = params
    length = row_tokens.shape[0]
    top = (length // NR).bit_length() - 2
    normed = low(normalize(row_tokens, pre_gain, pre_shift))
    query = low(low_back(jnp.dot(normed, query_proj, precision=HIGHEST) + query_bias))
    keys = low(low_back(jnp.dot(normed, key_proj, precision=HIGHEST)))
    values = low(low_back(jnp.dot(normed, value_proj, precision=HIGHEST) + value_bias))
    current = jnp.concatenate([keys, values], axis=1)
    current_ids = segments
    level_data = [current]
    level_ids = [segments]
    for level in range(1, top + 1):
        pairs = current.reshape(-1, 2, 2 * D)
        current = 0.5 * (pairs[:, 0] + pairs[:, 1])
        halves = current_ids.reshape(-1, 2)
        current_ids = jnp.where(halves[:, 0] == halves[:, 1], halves[:, 0], 0)
        level_data.append(low(current))
        level_ids.append(current_ids)
    scale = 1.0 / math.sqrt(HEAD_DIM)
    heads_query = query.reshape(length, HEADS, HEAD_DIM)
    scores = []
    masks = []
    value_windows = []
    for level in range(top + 1):
        block = NR * 2 ** level
        count = length // block
        window = windows_of(level_data[level], count)
        key_window = window[:, :, :D].reshape(count, 3 * NR, HEADS, HEAD_DIM)
        value_windows.append(window[:, :, D:].reshape(count, 3 * NR, HEADS, HEAD_DIM))
        query_blocks = heads_query.reshape(count, block, HEADS, HEAD_DIM)
        raw = jnp.einsum('bqhd,bkhd->bqhk', query_blocks, key_window, precision=HIGHEST)
        scores.append(low_back(raw.reshape(length, HEADS, 3 * NR)) * scale + level * LOG_TWO)
        masks.append(level_mask(level, segments, level_ids[level], length)[:, None, :])
    every_score = jnp.concatenate(scores, axis=2)
    every_mask = jnp.concatenate(masks, axis=2)
    masked = jnp.where(every_mask, every_score, -1e+30)
    peak = lax.optimization_barrier(jnp.max(masked, axis=2, keepdims=True))
    total = lax.optimization_barrier(jnp.sum(jnp.where(every_mask, jnp.exp(masked - peak), 0.0), axis=2, keepdims=True))
    norm_log = peak + jnp.log(total)
    prob = low(jnp.where(every_mask, jnp.exp(masked - norm_log), 0.0))
    attended = jnp.zeros((length, HEADS, HEAD_DIM), jnp.float32)
    for level in range(top + 1):
        block = NR * 2 ** level
        count = length // block
        part = prob[:, :, level * 3 * NR:(level + 1) * 3 * NR].reshape(count, block, HEADS, 3 * NR)
        mixed = jnp.einsum('bqhk,bkhd->bqhd', part, value_windows[level], precision=HIGHEST)
        attended = attended + mixed.reshape(length, HEADS, HEAD_DIM)
    attended = low(low_back(attended.reshape(length, D)))
    mid = row_tokens + low_back(jnp.dot(attended, output_proj, precision=HIGHEST) + output_bias)
    second = low(normalize(mid, mid_gain, mid_shift))
    pre = low_back(jnp.dot(second, inner_proj, precision=HIGHEST) + inner_bias)
    act = low(jax.nn.gelu(pre, approximate=True))
    return mid + jnp.dot(act, outer_proj, precision=HIGHEST) + outer_bias

def reference(tokens, segment_ids, prenorm_gain, prenorm_shift, query_proj, query_bias, key_proj, value_proj, value_bias, output_proj, output_bias, midnorm_gain, midnorm_shift, inner_proj, inner_bias, outer_proj, outer_bias, upstream):
    params = tuple((item.astype(jnp.float32) for item in (prenorm_gain, prenorm_shift, query_proj, query_bias, key_proj, value_proj, value_bias, output_proj, output_bias, midnorm_gain, midnorm_shift, inner_proj, inner_bias, outer_proj, outer_bias)))

    def one_row(carry, row):
        row_tokens, segments, row_grad = row

        def forward(weights, inputs):
            return row_forward(weights, inputs, segments)
        result, pullback = jax.vjp(forward, params, row_tokens.astype(jnp.float32))
        weight_grads, token_grads = pullback(row_grad.astype(jnp.float32))
        carry = jax.tree.map(jnp.add, carry, weight_grads)
        return (carry, (result.astype(jnp.bfloat16), token_grads.astype(jnp.bfloat16)))
    initial = jax.tree.map(jnp.zeros_like, params)
    sums, (outputs, grads) = lax.scan(one_row, initial, (tokens, segment_ids, upstream))
    return (outputs, grads, sums[0], sums[1], sums[2], sums[3], sums[4], sums[5], sums[6], sums[7], sums[8], sums[9], sums[10], sums[11], sums[12], sums[13], sums[14])
```

```python
import functools
import math

import jax
import jax.numpy as jnp
from jax import lax
from jax.experimental import pallas as pl
from jax.experimental.pallas import tpu as pltpu
from jax.sharding import PartitionSpec as P

HEADS = 8
HEAD_DIM = 64
NR = 16
LANES = 128
LOG_TWO = math.log(2.0)
EPSILON = 1e-05
MASKED = -1e30
F32 = jnp.float32
BF16 = jnp.bfloat16
MESH = pl.DeviceIdType.MESH

VEC_ROWS = 16
V_PREG, V_PRES, V_QB, V_VB, V_OB, V_MIDG, V_MIDS, V_OUTB, V_INNB = 0, 1, 2, 3, 4, 5, 6, 7, 8


def dot(a, b):
    return jnp.dot(a, b, preferred_element_type=F32)


def dot_nt(a, b):
    return lax.dot_general(a, b, (((1,), (1,)), ((), ())), preferred_element_type=F32)


def dot_tn(a, b):
    return lax.dot_general(a, b, (((0,), (0,)), ((), ())), preferred_element_type=F32)


def iota(shape, dim):
    return lax.broadcasted_iota(jnp.int32, shape, dim)


def mean(x):
    return jnp.mean(x, axis=-1, keepdims=True)


def total(x):
    return jnp.sum(x, axis=0, keepdims=True)


class Plan:
    def __init__(self, rows, seq, span, width, hidden):
        self.rows, self.seq, self.span, self.width, self.hidden = rows, seq, span, width, hidden
        self.near = (span // NR).bit_length() - 1
        self.length = span * seq
        self.top = (self.length // NR).bit_length() - 2
        self.chunk = 128
        self.chunks = span // self.chunk
        self.far = list(range(self.near + 1, self.top + 1))
        self.level_row = [0]
        at = 0
        for level in range(1, self.near + 1):
            self.level_row.append(at)
            at += span >> level
        self.far_row = at
        for level in self.far:
            self.level_row.append(at)
            at += span >> level
        self.coarse_rows = self.far_row + NR
        self.id_row = NR - 2
        self.slot, self.slot_len = [], []
        at = 0
        for level in range(self.top + 1):
            n = 2 * NR + max(self.chunk >> level, NR)
            self.slot.append(at)
            self.slot_len.append(n)
            at += n
        self.used = at
        self.slots = -(-at // LANES) * LANES
        self.far_slot = self.slot[self.near + 1]
        self.far_slots = self.slots - self.far_slot
        self.edge = NR * (self.near + 1)
        self.grad_rows = 4 * width + 2 * hidden
        ffn = hidden
        self.parts = [(0, ffn), (ffn, ffn + width), (2 * ffn + width, 3 * width)]
        self.counts = [2, 2, rows // 4, seq]
        self.swap = rows // 4 == 2
        self.scatter = []
        for off, n in self.parts:
            per = n // (2 * 2 * (rows // 4))
            self.scatter.append(per % (NR * seq) == 0)


def sequence(*steps):
    for step in steps:
        step()


def layer_kernel(
    plan,
    tok_hbm, ids_ref, vec_ref, inb_ref, wq_hbm, wk_hbm, wv_hbm, wo_hbm, w1_hbm, w2_hbm, up_hbm,
    out_ref, gin_ref, red_ref, vout_ref,
    tok, up, wq, wk, wv, wo, w1, w2, n1, n2, mid, racc, dsec, first, second, qh, att, dah, dq,
    level, edge, halo, farg, slots, levs, bias, probs, dslots, own, hsend, hrecv, fsend, frecv,
    coarse, dkv, grads, recv0, recv1, recv2, recv3, vstage, vrecv0, vrecv1, vrecv2, vrecv3, stats,
    in_sem, halo_send, halo_recv, far_send, far_recv, back_send, back_recv, fback_send, fback_recv,
    rs_send, rs_recv, ag_send, ag_recv, vec_send, vec_recv,
):
    span, width, hidden = plan.span, plan.width, plan.hidden
    seq, near, top = plan.seq, plan.near, plan.top
    tile = hidden // w1.shape[0]
    tiles = w1.shape[0]
    pairs = width // LANES
    blocks = 2 * pairs
    row_id, seq_id = lax.axis_index("rows"), lax.axis_index("seq")
    start = seq_id * span

    core = row_id % 2
    if plan.swap:
        stride_a, stride_b = 2 + 2 * core, 4 - 2 * core
    else:
        stride_a, stride_b = 2, 4
    count = plan.counts
    index = [
        core,
        (row_id // stride_a) % count[1],
        (row_id // stride_b) % count[2],
        seq_id,
    ]

    def peer(digit, k):
        other = (index[digit] + k) % count[digit]
        if digit == 3:
            return other, (row_id, other)
        stride = [1, stride_a, stride_b][digit]
        return other, (row_id + (other - index[digit]) * stride, seq_id)

    def remote(src, dst, send, recv, device):
        return pltpu.make_async_remote_copy(
            src_ref=src, dst_ref=dst, send_sem=send, recv_sem=recv,
            device_id=device, device_id_type=MESH,
        )

    loads = []

    def load(src, dst):
        copy = pltpu.make_async_copy(src, dst, in_sem.at[len(loads)])
        copy.start()
        loads.append(copy)
        return copy

    load_tok = load(tok_hbm.at[0], tok)
    load_q = load(wq_hbm, wq)
    load_k = load(wk_hbm, wk)
    load_v = load(wv_hbm, wv)
    load_up = load(up_hbm.at[0], up)
    load_o = load(wo_hbm, wo)
    load_1 = [load(w1_hbm.at[:, t * tile : (t + 1) * tile], w1.at[t]) for t in range(tiles)]
    load_2 = load(w2_hbm, w2)

    halo[...] = jnp.zeros_like(halo)
    hrecv[...] = jnp.zeros_like(hrecv)
    vstage[0] = jnp.zeros((VEC_ROWS, width), F32)

    barrier = pltpu.get_barrier_semaphore()
    greeted = 0
    for digit in range(4):
        for k in range(1, count[digit]):
            _, device = peer(digit, k)
            pl.semaphore_signal(barrier, inc=1, device_id=device, device_id_type=MESH)
            greeted += 1

    def vec(row):
        return vec_ref[row : row + 1, :]

    load_tok.wait()
    x = tok[...].astype(F32)
    center = x - mean(x)
    rstd = lax.rsqrt(mean(center * center) + EPSILON)
    normed = center * rstd
    n1[...] = normed
    stats[0] = jnp.broadcast_to(rstd, (span, LANES))
    first[...] = (normed * vec(0) + vec(1)).astype(BF16)
    load_k.wait()
    keys = dot(first[...], wk[...]).astype(BF16)
    load_v.wait()
    values = (dot(first[...], wv[...]) + vec(3)).astype(BF16)
    for b in range(pairs):
        level[b, :span] = keys[:, b * LANES : (b + 1) * LANES]
        level[pairs + b, :span] = values[:, b * LANES : (b + 1) * LANES]

    def averaging(rows_dim):
        shape = (plan.coarse_rows, span) if rows_dim == 0 else (span, plan.coarse_rows)
        r, p = iota(shape, rows_dim), iota(shape, 1 - rows_dim)
        matrix = jnp.zeros(shape, F32)
        for lv in range(1, top + 1):
            at = plan.level_row[lv]
            hit = (r - at == (p >> lv)) & (r >= at) & (r < at + (span >> lv))
            matrix = jnp.where(hit, 0.5**lv, matrix)
        return matrix.astype(BF16)

    matrix = averaging(0)
    ids_f = ids_ref[...].astype(F32)
    ids_wide = jnp.concatenate([ids_f, jnp.zeros((1, 2 * width - span), F32)], axis=1)
    far_at = plan.far_row
    for half, kv in enumerate((keys, values)):
        mixed = dot(matrix, kv)
        for b in range(pairs):
            level[half * pairs + b, span : span + far_at] = mixed[
                :far_at, b * LANES : (b + 1) * LANES
            ].astype(BF16)
        ids_half = jnp.broadcast_to(ids_wide[:, half * width : (half + 1) * width], (NR, width))
        farg[seq_id, :, half * width : (half + 1) * width] = jnp.where(
            iota((NR, width), 0) == plan.id_row, ids_half, mixed[far_at:]
        ).astype(BF16)

    def level_start(lv):
        return 0 if lv == 0 else span + plan.level_row[lv]

    for lv in range(near + 1):
        at, n = level_start(lv), span >> lv
        edge[0, :, lv * NR : (lv + 1) * NR] = level[:, at : at + NR]
        edge[1, :, lv * NR : (lv + 1) * NR] = level[:, at + n - NR : at + n]

    pl.semaphore_wait(barrier, greeted)

    def far_copy(k):
        _, device = peer(3, k)
        return remote(
            farg.at[seq_id], farg.at[seq_id], far_send.at[k - 1], far_recv.at[k - 1], device
        )

    def halo_copy(src, dst, send, recv, side):
        step = 2 * side - 1
        return remote(
            src.at[side], dst.at[1 - side], send.at[side], recv.at[1 - side],
            (row_id, seq_id + step),
        )

    def halo_start(src, dst, send, recv):
        @pl.when(seq_id > 0)
        def _():
            halo_copy(src, dst, send, recv, 0).start()

        @pl.when(seq_id < seq - 1)
        def _():
            halo_copy(src, dst, send, recv, 1).start()

    def halo_wait(src, dst, send, recv):
        @pl.when(seq_id > 0)
        def _():
            remote(
                src.at[0], dst.at[0], send.at[0], recv.at[0], (row_id, seq_id - 1)
            ).wait()

        @pl.when(seq_id < seq - 1)
        def _():
            remote(
                src.at[1], dst.at[1], send.at[1], recv.at[1], (row_id, seq_id + 1)
            ).wait()

    halo_start(edge, halo, halo_send, halo_recv)
    for k in range(1, seq):
        far_copy(k).start()

    load_q.wait()
    query = ((dot(first[...], wq[...]) + vec(2)).astype(BF16) * (1.0 / math.sqrt(HEAD_DIM))).astype(
        BF16
    )
    for b in range(pairs):
        qh[b] = query[:, b * LANES : (b + 1) * LANES]

    def slot_pieces(c):
        pieces = []
        for lv in range(near + 1):
            at, n = level_start(lv), span >> lv
            per = plan.chunk >> lv
            s0 = plan.slot[lv]
            if per >= NR:
                low, high = c * per - NR, c * per + per + NR
            else:
                low, high = -NR, n + NR
            if low < 0:
                pieces.append((s0, "low", lv * NR, NR))
                s0, low = s0 + NR, 0
            inner = min(high, n)
            pieces.append((s0, "own", at + low, inner - low))
            s0 += inner - low
            if high > n:
                pieces.append((s0, "high", lv * NR, NR))
        return pieces

    halo_wait(edge, halo, halo_send, halo_recv)
    for c in range(plan.chunks):
        for s0, kind, at, n in slot_pieces(c):
            if kind == "own":
                slots[c, :, s0 : s0 + n] = level[:, at : at + n]
            else:
                slots[c, :, s0 : s0 + n] = halo[0 if kind == "low" else 1, :, at : at + n]
    for k in range(1, seq):
        far_copy(k).wait()

    def far_select():
        pieces = []
        for lv in plan.far:
            per_log = (span >> lv).bit_length() - 1
            first_row = plan.level_row[lv] - plan.far_row
            j = (start // (NR << lv) - 1) * NR + iota((3 * NR, seq * NR), 0)
            column = (j >> per_log) * NR + (j & ((1 << per_log) - 1)) + first_row
            pieces.append((column == iota((3 * NR, seq * NR), 1)).astype(F32))
        rest = plan.far_slots - 3 * NR * len(plan.far)
        if rest:
            pieces.append(jnp.zeros((rest, seq * NR), F32))
        return jnp.concatenate(pieces, axis=0).astype(BF16)

    select = far_select()
    far_values = dot(select, farg[...].reshape(seq * NR, 2 * width)).astype(BF16)
    for c in range(plan.chunks):
        for b in range(blocks):
            slots[c, b, plan.far_slot :] = far_values[:, b * LANES : (b + 1) * LANES]

    row_ids = [farg[s].astype(F32)[plan.id_row : plan.id_row + 1, :span] for s in range(seq)]
    current = jnp.concatenate(row_ids, axis=1)
    level_ids = [current]
    for lv in range(1, top + 1):
        shifted = pltpu.roll(current, plan.length - (1 << (lv - 1)), 1)
        current = jnp.where(current == shifted, current, 0.0)
        level_ids.append(current)
    level_ids += [jnp.zeros_like(current)] * (8 - len(level_ids))
    stacked = jnp.concatenate(level_ids, axis=0).astype(BF16)
    for s in range(seq):
        levs[s] = stacked[:, s * span : (s + 1) * span]

    ids_rows = jnp.broadcast_to(ids_f, (8, span)).astype(BF16)
    slot_at = iota((1, plan.slots), 1)
    slot_level = jnp.zeros((1, plan.slots), jnp.int32)
    for lv in range(1, top + 1):
        slot_level = slot_level + (slot_at >= plan.slot[lv]).astype(jnp.int32)
    for c in range(plan.chunks):
        origin = start + c * plan.chunk
        j = slot_at
        for lv in range(top + 1):
            if (plan.chunk >> lv) >= NR:
                base = origin // (1 << lv) - NR
            else:
                base = (origin // (NR << lv) - 1) * NR
            here = slot_at - plan.slot[lv] + base
            j = here if lv == 0 else jnp.where(slot_level == lv, here, j)
        j = jnp.where(slot_at < plan.used, j, -1)
        goal = j << slot_level

        def gather_ids(s, found):
            hot = iota((span, plan.slots), 0) + s * span == goal
            return found + dot(levs[s], hot.astype(F32).astype(BF16))

        found = lax.fori_loop(0, seq, gather_ids, jnp.zeros((8, plan.slots), F32))
        own_level = iota((8, plan.slots), 0) == slot_level
        key_id = jnp.sum(jnp.where(own_level, found, 0.0), axis=0, keepdims=True)
        mine = (iota((plan.chunk, span), 1) == iota((plan.chunk, span), 0) + c * plan.chunk)
        query_id = dot_nt(mine.astype(F32).astype(BF16), ids_rows)[:, :1]
        inside = (goal >= 0) & (goal < plan.length) & (j >= 0)
        usable = inside & ((slot_level == 0) | (key_id > 0.5))
        key_id = jnp.where(usable, key_id, -1.0)
        position = origin + iota((plan.chunk, plan.slots), 0)
        off_block = (j >> 4) - (position >> (slot_level + 4))
        off_half = (j >> 3) - (position >> (slot_level + 3))
        reach = jnp.where(slot_level == 0, -1, 1)
        counted = (key_id == query_id) & (jnp.abs(off_block) <= 1) & (jnp.abs(off_half) > reach)
        bias[c] = jnp.where(counted, slot_level.astype(F32) * LOG_TWO, MASKED)

    lane = iota((1, LANES), 1)
    low_half = (lane < HEAD_DIM).astype(F32).astype(BF16)
    high_half = (lane >= HEAD_DIM).astype(F32).astype(BF16)
    low_lanes = iota((plan.chunk, LANES), 1) < HEAD_DIM

    def two_heads(block):
        return jnp.concatenate([block * low_half, block * high_half], axis=0)

    def merge_heads(both):
        return jnp.where(low_lanes, both[: plan.chunk], both[plan.chunk :])

    def chunk_rows(c):
        return pl.ds(pl.multiple_of(c * plan.chunk, plan.chunk), plan.chunk)

    def pair_lanes(b):
        return pl.ds(pl.multiple_of(b * LANES, LANES), LANES)

    def attend(i, carry):
        c, b = i // pairs, i % pairs
        q2 = two_heads(qh[b, chunk_rows(c)])
        offset = bias[c]
        score = dot_nt(q2, slots[c, b]) + jnp.concatenate([offset, offset], axis=0)
        peak = jnp.max(score, axis=1, keepdims=True)
        raised = jnp.exp(score - peak)
        prob = raised * (1.0 / jnp.sum(raised, axis=1, keepdims=True))
        low = prob.astype(BF16)
        probs[i] = low
        att[chunk_rows(c), pair_lanes(b)] = merge_heads(dot(low, slots[c, pairs + b])).astype(BF16)
        return carry

    lax.fori_loop(0, plan.chunks * pairs, attend, 0)

    received = [recv0, recv1, recv2, recv3]
    starts = [recv0.shape[1], recv1.shape[1], recv2.shape[1], recv3.shape[1]]
    step_of_part = []

    def region(part, digits):
        off, n = plan.parts[part]
        base = off
        for digit in range(digits):
            n = n // count[digit]
            base = base + index[digit] * n
        return base, n

    def rows_at(base, n):
        return pl.ds(pl.multiple_of(base, NR), n)

    def received_rows(part, digit, n):
        off, whole = plan.parts[part]
        share = whole // n
        return pl.ds(off // share, n)

    def rs_copy(part, digit, k):
        base, n = region(part, digit)
        other, device = peer(digit, k)
        if digit == 3 and not plan.scatter[part]:
            return remote(
                grads.at[rows_at(base, n)],
                received[digit].at[k - 1, received_rows(part, digit, n)],
                rs_send.at[part, digit, k - 1], rs_recv.at[part, digit, k - 1], device,
            )
        n = n // count[digit]
        return remote(
            grads.at[rows_at(base + other * n, n)],
            received[digit].at[k - 1, received_rows(part, digit, n)],
            rs_send.at[part, digit, k - 1], rs_recv.at[part, digit, k - 1], device,
        )

    def rs_start(part, digit):
        for k in range(1, count[digit]):
            rs_copy(part, digit, k).start()

    def rs_finish(part, digit):
        for k in range(1, count[digit]):
            rs_copy(part, digit, k).wait_recv()
        gather_all = digit == 3 and not plan.scatter[part]
        base, n = region(part, digit if gather_all else digit + 1)
        off, whole = plan.parts[part]
        at = off // (whole // n)
        target = red_ref if digit == 3 else grads
        block = 64 if n % 64 == 0 else NR

        def add(i, carry):
            here = rows_at(base + i * block, block)
            there = pl.ds(pl.multiple_of(at + i * block, NR), block)
            if gather_all:
                acc = jnp.zeros((block, width), F32)
                for s in range(seq):
                    slot = (seq_id - s + seq - 1) % seq
                    theirs = received[digit][jnp.minimum(slot, seq - 2), there].astype(F32)
                    acc = acc + jnp.where(seq_id == s, grads[here].astype(F32), theirs)
            else:
                acc = grads[here].astype(F32)
                for k in range(1, count[digit]):
                    acc = acc + received[digit][k - 1, there].astype(F32)
            target[here] = acc.astype(BF16)
            return carry

        lax.fori_loop(0, n // block, add, 0)

    def ag_copy(part, digit, k):
        base, n = region(part, digit + 1)
        _, device = peer(digit, k)
        return remote(
            red_ref.at[rows_at(base, n)], red_ref.at[rows_at(base, n)],
            ag_send.at[part, digit, k - 1], ag_recv.at[part, digit, k - 1], device,
        )

    def ag_start(part, digit):
        if digit == 3 and not plan.scatter[part]:
            return
        for k in range(1, count[digit]):
            ag_copy(part, digit, k).start()

    def ag_finish(part, digit):
        if digit == 3 and not plan.scatter[part]:
            return
        for k in range(1, count[digit]):
            ag_copy(part, digit, k).wait_recv()

    def part_steps(part):
        steps = [lambda: rs_start(part, 0)]
        for digit in range(1, 4):
            steps.append(
                functools.partial(
                    sequence,
                    functools.partial(rs_finish, part, digit - 1),
                    functools.partial(rs_start, part, digit),
                )
            )
        steps.append(
            functools.partial(
                sequence, functools.partial(rs_finish, part, 3), functools.partial(ag_start, part, 3)
            )
        )
        for digit in (2, 1, 0):
            steps.append(
                functools.partial(
                    sequence,
                    functools.partial(ag_finish, part, digit + 1),
                    functools.partial(ag_start, part, digit),
                )
            )
        steps.append(functools.partial(ag_finish, part, 0))
        return steps

    part_a, part_b, part_c = (part_steps(part) for part in range(3))

    load_o.wait()
    load_up.wait()
    res = tok[...].astype(F32) + dot(att[...], wo[...]) + vec(4)
    mid[...] = res
    center = res - mean(res)
    rstd = lax.rsqrt(mean(center * center) + EPSILON)
    normed = center * rstd
    n2[...] = normed
    stats[1] = jnp.broadcast_to(rstd, (span, LANES))
    second[...] = (normed * vec(5) + vec(6)).astype(BF16)
    racc[...] = jnp.zeros_like(racc)
    dsec[...] = jnp.zeros_like(dsec)
    for copy in load_1:
        copy.wait()
    load_2.wait()
    curve = math.sqrt(2.0 / math.pi)

    def feed(t, carry):
        w2_rows = pl.ds(pl.multiple_of(t * tile, tile), tile)
        pre = dot(second[...], w1[t]) + inb_ref[pl.ds(t, 1), :]
        square = pre * pre
        bend = jnp.tanh(curve * (pre + 0.044715 * (square * pre)))
        half = 0.5 * (1.0 + bend)
        act = (pre * half).astype(BF16)
        slope = half + 0.5 * pre * (1.0 - bend * bend) * (curve * (1.0 + 3 * 0.044715 * square))
        upstream = up[...]
        racc[...] += dot(act, w2[w2_rows])
        d_pre = (dot_nt(upstream, w2[w2_rows]) * slope).astype(BF16)
        base = (t // 2) * 4 * tile + (t % 2) * tile
        grads[rows_at(base, tile)] = dot_tn(act, upstream).astype(BF16)
        grads[rows_at(base + 2 * tile, tile)] = dot_tn(second[...], d_pre).astype(BF16)
        vstage[0, pl.ds(V_INNB + t, 1), :] = total(d_pre.astype(F32))
        dsec[...] += dot_nt(d_pre, w1[t])

        @pl.when(t == 1)
        def _():
            part_a[0]()

        return carry

    lax.fori_loop(0, tiles, feed, 0)
    out_ref[0] = (mid[...] + racc[...] + vec(7)).astype(BF16)

    up_f = up[...].astype(F32)
    vstage[0, V_OUTB : V_OUTB + 1] = total(up_f)
    d_second, normed = dsec[...], n2[...]
    scaled = d_second * vec(5)
    vstage[0, V_MIDG : V_MIDG + 1] = total(d_second * normed)
    vstage[0, V_MIDS : V_MIDS + 1] = total(d_second)
    d_mid = up_f + (scaled - mean(scaled) - normed * mean(scaled * normed)) * stats[1][:, :1]
    mid[...] = d_mid
    d_branch = d_mid.astype(BF16)
    vstage[0, V_OB : V_OB + 1] = total(d_branch.astype(F32))
    grads[2 * hidden : 2 * hidden + width] = dot_tn(att[...], d_branch).astype(BF16)
    part_b[0]()
    d_att = dot_nt(d_branch, wo[...]).astype(BF16)
    for b in range(pairs):
        dah[b] = d_att[:, b * LANES : (b + 1) * LANES]

    schedule = {
        0: [part_a[1]],
        1: [part_b[1]],
        3: [part_a[2]],
        5: [part_b[2], part_a[3]],
        7: [part_a[4], part_b[3]],
    }

    def attend_back(i, carry):
        c, b = i // pairs, i % pairs
        q2 = two_heads(qh[b, chunk_rows(c)])
        g2 = two_heads(dah[b, chunk_rows(c)])
        low = probs[i]
        prob = low.astype(F32)
        d_prob = dot_nt(g2, slots[c, pairs + b])
        weighted = prob * d_prob
        d_score = (weighted - prob * jnp.sum(weighted, axis=1, keepdims=True)).astype(BF16)
        d_query = merge_heads(dot(d_score, slots[c, b])) * (1.0 / math.sqrt(HEAD_DIM))
        dq[chunk_rows(c), pair_lanes(b)] = d_query.astype(BF16)
        dslots[c, b] = dot_tn(d_score, q2)
        dslots[c, pairs + b] = dot_tn(low, g2)
        for when, steps in schedule.items():

            @pl.when(i == when)
            def _():
                sequence(*steps)

        return carry

    lax.fori_loop(0, plan.chunks * pairs, attend_back, 0)

    def fold(b, carry):
        for c in range(plan.chunks):
            for s0, kind, at, n in slot_pieces(c):
                piece = dslots[c, b, s0 : s0 + n]
                if kind == "own":
                    parts_done = own_done[c].get((s0, at))
                    seen = parts_done if parts_done is not None else 0
                    if seen:
                        own[b, at : at + seen] += piece[:seen]
                    if seen < n:
                        own[b, at + seen : at + n] = piece[seen:]
                elif own_done[c].get((s0, kind)):
                    side = 0 if kind == "low" else 1
                    hsend[side, b, at : at + n] = (
                        hsend[side, b, at : at + n].astype(F32) + piece
                    ).astype(BF16)
                else:
                    side = 0 if kind == "low" else 1
                    hsend[side, b, at : at + n] = piece.astype(BF16)
        far = dslots[0, b, plan.far_slot :]
        for c in range(1, plan.chunks):
            far = far + dslots[c, b, plan.far_slot :]
        back = dot_tn(select, far.astype(BF16))
        for s in range(seq):
            fsend[s, b] = back[s * NR : (s + 1) * NR].astype(BF16)
        return carry

    own_done = []
    reached, halo_seen = {}, set()
    for c in range(plan.chunks):
        done = {}
        for s0, kind, at, n in slot_pieces(c):
            if kind == "own":
                lv = max(v for v in range(near + 1) if level_start(v) <= at)
                limit = reached.get(lv, level_start(lv))
                done[(s0, at)] = max(0, min(limit, at + n) - at)
                reached[lv] = max(limit, at + n)
            else:
                done[(s0, kind)] = (kind, at) in halo_seen
                halo_seen.add((kind, at))
        own_done.append(done)

    lax.fori_loop(0, blocks, fold, 0)

    def far_back(k):
        other, device = peer(3, k)
        return remote(
            fsend.at[other], frecv.at[k - 1], fback_send.at[k - 1], fback_recv.at[k - 1], device
        )

    halo_start(hsend, hrecv, back_send, back_recv)
    for k in range(1, seq):
        far_back(k).start()

    d_query = dq[...]
    vstage[0, V_QB : V_QB + 1] = total(d_query.astype(F32))
    off_c = plan.parts[2][0]
    grads[off_c : off_c + width] = dot_tn(first[...], d_query).astype(BF16)
    d_first = dot_nt(d_query, wq[...])
    racc[...] = d_first
    sequence(part_b[4], part_a[5])

    spread = averaging(1)
    halo_wait(hsend, hrecv, back_send, back_recv)
    for k in range(1, seq):
        far_back(k).wait()
    for lv in range(near + 1):
        at, n = level_start(lv), span >> lv
        lo, hi = lv * NR, (lv + 1) * NR
        own[:, at : at + NR] += hrecv[0, :, lo:hi].astype(F32)
        own[:, at + n - NR : at + n] += hrecv[1, :, lo:hi].astype(F32)
    far_sum = fsend[seq_id].astype(F32)
    for k in range(1, seq):
        far_sum = far_sum + frecv[k - 1].astype(F32)
    for b in range(blocks):
        cols = slice(b * LANES, (b + 1) * LANES)
        coarse[:far_at, cols] = own[b, span : span + far_at].astype(BF16)
        coarse[far_at:, cols] = far_sum[b].astype(BF16)
    for half in range(2):
        passed = dot(spread, coarse[:, half * width : (half + 1) * width])
        for b in range(pairs):
            cols = slice((half * pairs + b) * LANES, (half * pairs + b + 1) * LANES)
            dkv[:, cols] = (
                own[half * pairs + b, :span] + passed[:, b * LANES : (b + 1) * LANES]
            ).astype(BF16)
    d_keys, d_values = dkv[:, :width], dkv[:, width:]
    vstage[0, V_VB : V_VB + 1] = total(d_values.astype(F32))
    grads[off_c + width : off_c + 2 * width] = dot_tn(first[...], d_keys).astype(BF16)
    grads[off_c + 2 * width : off_c + 3 * width] = dot_tn(first[...], d_values).astype(BF16)
    part_c[0]()

    d_first = racc[...] + dot_nt(d_keys, wk[...]) + dot_nt(d_values, wv[...])
    normed = n1[...]
    scaled = d_first * vec(0)
    vstage[0, V_PREG : V_PREG + 1] = total(d_first * normed)
    vstage[0, V_PRES : V_PRES + 1] = total(d_first)
    d_in = mid[...] + (scaled - mean(scaled) - normed * mean(scaled * normed)) * stats[0][:, :1]
    gin_ref[0] = d_in.astype(BF16)

    vec_received = [vrecv0, vrecv1, vrecv2, vrecv3]

    def vec_copy(digit, k):
        _, device = peer(digit, k)
        return remote(
            vstage.at[digit], vec_received[digit].at[index[digit]],
            vec_send.at[digit, k - 1], vec_recv.at[digit, k - 1], device,
        )

    def vec_start(digit):
        for k in range(1, count[digit]):
            vec_copy(digit, k).start()

    def vec_finish(digit):
        for k in range(1, count[digit]):
            vec_copy(digit, k).wait_recv()
        acc = jnp.zeros((VEC_ROWS, width), F32)
        for s in range(count[digit]):
            acc = acc + jnp.where(index[digit] == s, vstage[digit], vec_received[digit][s])
        if digit == 3:
            vout_ref[...] = acc
        else:
            vstage[digit + 1] = acc

    vec_start(0)

    part_c[1]()
    part_b[5]()
    vec_finish(0)
    vec_start(1)
    part_a[6]()
    part_c[2]()
    vec_finish(1)
    vec_start(2)
    part_b[6]()
    part_c[3]()
    vec_finish(2)
    vec_start(3)
    part_a[7]()
    part_c[4]()
    part_b[7]()
    part_c[5]()
    part_c[6]()
    vec_finish(3)
    part_a[8]()
    part_c[7]()
    part_b[8]()
    part_c[8]()

    for part in range(3):
        for digit in range(4):
            for k in range(1, count[digit]):
                rs_copy(part, digit, k).wait_send()
                if digit < 3 or plan.scatter[part]:
                    ag_copy(part, digit, k).wait_send()
    for digit in range(4):
        for k in range(1, count[digit]):
            vec_copy(digit, k).wait_send()


def unpack_kernel(
    width, tiles, red_hbm, vec_ref,
    query_ref, key_ref, value_ref, output_ref, inner_ref, outer_ref,
    preg_ref, pres_ref, qb_ref, vb_ref, ob_ref, midg_ref, mids_ref, outb_ref, innb_ref,
    low, wide, in_sem, out_sem,
):
    targets = []
    for t in range(tiles):
        at = (t // 2) * 4 + t % 2
        rows = slice(t * width, (t + 1) * width)
        targets.append((at, outer_ref.at[rows]))
        targets.append((at + 2, inner_ref.at[:, rows]))
    for i, ref in enumerate((output_ref, query_ref, key_ref, value_ref)):
        targets.append((2 * tiles + i, ref))

    def fetch(i):
        at = targets[i][0]
        return pltpu.make_async_copy(
            red_hbm.at[at * width : (at + 1) * width], low.at[i % 4], in_sem.at[i % 4]
        )

    def put(i):
        return pltpu.make_async_copy(wide.at[i % 4], targets[i][1], out_sem.at[i % 4])

    n = len(targets)
    for i in range(min(3, n)):
        fetch(i).start()
    for row, ref in (
        (V_PREG, preg_ref), (V_PRES, pres_ref), (V_QB, qb_ref), (V_VB, vb_ref), (V_OB, ob_ref),
        (V_MIDG, midg_ref), (V_MIDS, mids_ref), (V_OUTB, outb_ref),
    ):
        ref[...] = vec_ref[row]
    for t in range(tiles):
        innb_ref[t * width : (t + 1) * width] = vec_ref[V_INNB + t]
    for i in range(n):
        fetch(i).wait()
        if i >= 4:
            put(i - 4).wait()
        wide[i % 4] = low[i % 4].astype(F32)
        put(i).start()
        if i + 3 < n:
            fetch(i + 3).start()
    for i in range(max(0, n - 4), n):
        put(i).wait()


def shards(
    rows, seq,
    tokens, segment_ids, prenorm_gain, prenorm_shift, query_proj, query_bias, key_proj, value_proj,
    value_bias, output_proj, output_bias, midnorm_gain, midnorm_shift, inner_proj, inner_bias,
    outer_proj, outer_bias, upstream,
):
    _, span, width = tokens.shape
    hidden = inner_proj.shape[1]
    plan = Plan(rows, seq, span, width, hidden)
    tiles = hidden // width
    pairs = width // LANES
    vectors = jnp.concatenate(
        [
            prenorm_gain, prenorm_shift, query_bias, value_bias, output_bias, midnorm_gain,
            midnorm_shift, outer_bias,
        ]
    ).reshape(8, width)
    count = plan.counts
    most = max(count) - 1
    vmem = pl.BlockSpec(memory_space=pltpu.VMEM)
    hbm = pl.BlockSpec(memory_space=pl.ANY)
    grad_rows = plan.grad_rows
    rest = [grad_rows // 2, grad_rows // 4, grad_rows // 4 // count[2]]
    last = rest[2] // seq if all(plan.scatter) else rest[2]
    dma = pltpu.SemaphoreType.DMA
    items = plan.chunks * pairs
    scratch = [
        pltpu.VMEM((span, width), BF16),
        pltpu.VMEM((span, width), BF16),
        pltpu.VMEM((width, width), BF16),
        pltpu.VMEM((width, width), BF16),
        pltpu.VMEM((width, width), BF16),
        pltpu.VMEM((width, width), BF16),
        pltpu.VMEM((tiles, width, width), BF16),
        pltpu.VMEM((hidden, width), BF16),
        pltpu.VMEM((span, width), F32),
        pltpu.VMEM((span, width), F32),
        pltpu.VMEM((span, width), F32),
        pltpu.VMEM((span, width), F32),
        pltpu.VMEM((span, width), F32),
        pltpu.VMEM((span, width), BF16),
        pltpu.VMEM((span, width), BF16),
        pltpu.VMEM((pairs, span, LANES), BF16),
        pltpu.VMEM((span, width), BF16),
        pltpu.VMEM((pairs, span, LANES), BF16),
        pltpu.VMEM((span, width), BF16),
        pltpu.VMEM((2 * pairs, span + plan.far_row, LANES), BF16),
        pltpu.VMEM((2, 2 * pairs, plan.edge, LANES), BF16),
        pltpu.VMEM((2, 2 * pairs, plan.edge, LANES), BF16),
        pltpu.VMEM((seq, NR, 2 * width), BF16),
        pltpu.VMEM((plan.chunks, 2 * pairs, plan.slots, LANES), BF16),
        pltpu.VMEM((seq, 8, span), BF16),
        pltpu.VMEM((plan.chunks, plan.chunk, plan.slots), F32),
        pltpu.VMEM((items, 2 * plan.chunk, plan.slots), BF16),
        pltpu.VMEM((plan.chunks, 2 * pairs, plan.slots, LANES), F32),
        pltpu.VMEM((2 * pairs, span + plan.far_row, LANES), F32),
        pltpu.VMEM((2, 2 * pairs, plan.edge, LANES), BF16),
        pltpu.VMEM((2, 2 * pairs, plan.edge, LANES), BF16),
        pltpu.VMEM((seq, 2 * pairs, NR, LANES), BF16),
        pltpu.VMEM((seq - 1, 2 * pairs, NR, LANES), BF16),
        pltpu.VMEM((plan.coarse_rows, 2 * width), BF16),
        pltpu.VMEM((span, 2 * width), BF16),
        pltpu.VMEM((grad_rows, width), BF16),
        pltpu.VMEM((count[0] - 1, rest[0], width), BF16),
        pltpu.VMEM((count[1] - 1, rest[1], width), BF16),
        pltpu.VMEM((count[2] - 1, rest[2], width), BF16),
        pltpu.VMEM((count[3] - 1, last, width), BF16),
        pltpu.VMEM((4, VEC_ROWS, width), F32),
        pltpu.VMEM((count[0], VEC_ROWS, width), F32),
        pltpu.VMEM((count[1], VEC_ROWS, width), F32),
        pltpu.VMEM((count[2], VEC_ROWS, width), F32),
        pltpu.VMEM((count[3], VEC_ROWS, width), F32),
        pltpu.VMEM((2, span, LANES), F32),
        dma((7 + tiles,)),
        dma((2,)), dma((2,)),
        dma((seq - 1,)), dma((seq - 1,)),
        dma((2,)), dma((2,)),
        dma((seq - 1,)), dma((seq - 1,)),
        dma((3, 4, most)), dma((3, 4, most)),
        dma((3, 4, most)), dma((3, 4, most)),
        dma((4, most)), dma((4, most)),
    ]
    layer_output, input_grad, reduced, vecs = pl.pallas_call(
        functools.partial(layer_kernel, plan),
        out_shape=(
            jax.ShapeDtypeStruct(tokens.shape, BF16),
            jax.ShapeDtypeStruct(tokens.shape, BF16),
            jax.ShapeDtypeStruct((grad_rows, width), BF16),
            jax.ShapeDtypeStruct((VEC_ROWS, width), F32),
        ),
        in_specs=[hbm, vmem, vmem, vmem] + [hbm] * 7,
        out_specs=(vmem, vmem, vmem, vmem),
        scratch_shapes=scratch,
        compiler_params=pltpu.CompilerParams(
            collective_id=0, has_side_effects=True, vmem_limit_bytes=60 * 1024 * 1024
        ),
        name="layer",
    )(
        tokens, segment_ids, vectors, inner_bias.reshape(tiles, width), query_proj, key_proj,
        value_proj, output_proj, inner_proj, outer_proj, upstream,
    )
    matrix = jax.ShapeDtypeStruct((width, width), F32)
    vector = jax.ShapeDtypeStruct((width,), F32)
    grads = pl.pallas_call(
        functools.partial(unpack_kernel, width, tiles),
        out_shape=(
            matrix, matrix, matrix, matrix,
            jax.ShapeDtypeStruct((width, hidden), F32),
            jax.ShapeDtypeStruct((hidden, width), F32),
            vector, vector, vector, vector, vector, vector, vector, vector,
            jax.ShapeDtypeStruct((hidden,), F32),
        ),
        in_specs=[hbm, vmem],
        out_specs=(hbm,) * 6 + (vmem,) * 9,
        scratch_shapes=[
            pltpu.VMEM((4, width, width), BF16),
            pltpu.VMEM((4, width, width), F32),
            dma((4,)), dma((4,)),
        ],
        name="unpack",
    )(reduced, vecs)
    (query_g, key_g, value_g, output_g, inner_g, outer_g,
     preg, pres, qb, vb, ob, midg, mids, outb, innb) = grads
    return (
        layer_output, input_grad, preg, pres, query_g, qb, key_g, value_g, vb, output_g, ob,
        midg, mids, inner_g, innb, outer_g, outb,
    )


def solution(mesh):
    split, ids, whole = P("rows", "seq", None), P("rows", "seq"), P()
    in_specs = (split, ids) + (whole,) * 15 + (split,)
    out_specs = (split, split) + (whole,) * 15
    return jax.shard_map(
        functools.partial(shards, mesh.shape["rows"], mesh.shape["seq"]),
        mesh=mesh, in_specs=in_specs, out_specs=out_specs, check_vma=False,
    )
```

```python
import functools
import math

import jax
import jax.numpy as jnp
from jax import lax
from jax.experimental import pallas as pl
from jax.experimental.pallas import tpu as pltpu
from jax.sharding import PartitionSpec as P

HEADS = 8
HEAD_DIM = 64
NR = 16
LANES = 128
LOG_TWO = math.log(2.0)
EPSILON = 1e-05
MASKED = -1e30
F32 = jnp.float32
BF16 = jnp.bfloat16
MESH = pl.DeviceIdType.MESH

VEC_ROWS = 16
V_PREG, V_PRES, V_QB, V_VB, V_OB, V_MIDG, V_MIDS, V_OUTB, V_INNB = 0, 1, 2, 3, 4, 5, 6, 7, 8


def dot(a, b):
    return jnp.dot(a, b, preferred_element_type=F32)


def dot_nt(a, b):
    return lax.dot_general(a, b, (((1,), (1,)), ((), ())), preferred_element_type=F32)


def dot_tn(a, b):
    return lax.dot_general(a, b, (((0,), (0,)), ((), ())), preferred_element_type=F32)


def iota(shape, dim):
    return lax.broadcasted_iota(jnp.int32, shape, dim)


def mean(x):
    return jnp.mean(x, axis=-1, keepdims=True)


def total(x):
    return jnp.sum(x, axis=0, keepdims=True)


class Plan:
    def __init__(self, rows, seq, span, width, hidden):
        self.rows, self.seq, self.span, self.width, self.hidden = rows, seq, span, width, hidden
        self.near = (span // NR).bit_length() - 1
        self.length = span * seq
        self.top = (self.length // NR).bit_length() - 2
        self.chunk = 128
        self.chunks = span // self.chunk
        self.far = list(range(self.near + 1, self.top + 1))
        self.level_row = [0]
        at = 0
        for level in range(1, self.near + 1):
            self.level_row.append(at)
            at += span >> level
        self.far_row = at
        for level in self.far:
            self.level_row.append(at)
            at += span >> level
        self.coarse_rows = self.far_row + NR
        self.slot, self.slot_len = [], []
        at = 0
        for level in range(self.top + 1):
            n = 2 * NR + max(self.chunk >> level, NR)
            self.slot.append(at)
            self.slot_len.append(n)
            at += n
        self.used = at
        self.slots = -(-at // LANES) * LANES
        self.far_slot = self.slot[self.near + 1]
        self.far_slots = self.slots - self.far_slot
        self.edge = NR * (self.near + 1)
        self.grad_rows = 4 * width + 2 * hidden
        self.parts = [(p * 2 * width, 2 * width) for p in range(self.grad_rows // (2 * width))]
        self.counts = [2, 2, rows // 4, seq]
        self.swap = rows // 4 == 2
        self.scatter = (2 * width // rows) % (NR * seq) == 0


def sequence(*steps):
    for step in steps:
        step()


def layer_kernel(
    plan,
    tok_hbm, ids_ref, preg_ref, pres_ref, wq_hbm, qb_ref, wk_hbm, wv_hbm, vb_ref, wo_hbm, ob_ref,
    midg_ref, mids_ref, w1_hbm, inb_ref, w2_hbm, outb_ref, up_hbm,
    out_ref, gin_ref, red_hbm, vout_ref,
    tok, up, wq, wk, wv, wo, w1, w2, n1, n2, mid, racc, dsec, first, second, qh, att, dah, dq,
    level, edge, halo, farg, slots, bias, probs, dslots, own, hsend, hrecv, fsend, frecv,
    coarse, spread, dkv, grads, recv0, recv1, recv2, recv3, vstage, vrecv0, vrecv1, vrecv2, vrecv3, stats,
    inb, red_ref,
    in_sem, out_sem, halo_send, halo_recv, far_send, far_recv, back_send, back_recv, fback_send, fback_recv,
    rs_send, rs_recv, ag_send, ag_recv, vec_send, vec_recv,
):
    span, width, hidden = plan.span, plan.width, plan.hidden
    seq, near, top = plan.seq, plan.near, plan.top
    tile = hidden // w1.shape[0]
    tiles = w1.shape[0]
    pairs = width // LANES
    blocks = 2 * pairs
    row_id, seq_id = lax.axis_index("rows"), lax.axis_index("seq")
    start = seq_id * span

    core = row_id % 2
    if plan.swap:
        stride_a, stride_b = 2 + 2 * core, 4 - 2 * core
    else:
        stride_a, stride_b = 2, 4
    count = plan.counts
    index = [
        core,
        (row_id // stride_a) % count[1],
        (row_id // stride_b) % count[2],
        seq_id,
    ]

    def peer(digit, k):
        other = (index[digit] + k) % count[digit]
        if digit == 3:
            return other, (row_id, other)
        stride = [1, stride_a, stride_b][digit]
        return other, (row_id + (other - index[digit]) * stride, seq_id)

    def remote(src, dst, send, recv, device):
        return pltpu.make_async_remote_copy(
            src_ref=src, dst_ref=dst, send_sem=send, recv_sem=recv,
            device_id=device, device_id_type=MESH,
        )

    loads = []

    def load(src, dst):
        copy = pltpu.make_async_copy(src, dst, in_sem.at[len(loads)])
        copy.start()
        loads.append(copy)
        return copy

    load_tok = load(tok_hbm.at[0], tok)
    load_q = load(wq_hbm, wq)
    load_k = load(wk_hbm, wk)
    load_v = load(wv_hbm, wv)
    load_up = load(up_hbm.at[0], up)
    load_o = load(wo_hbm, wo)
    load_1 = [load(w1_hbm.at[:, t * tile : (t + 1) * tile], w1.at[t]) for t in range(tiles)]
    load_2 = load(w2_hbm, w2)

    halo[...] = jnp.zeros_like(halo)
    hrecv[...] = jnp.zeros_like(hrecv)
    vstage[0] = jnp.zeros((VEC_ROWS, width), F32)
    for t in range(tiles):
        inb[t : t + 1, :] = inb_ref[t * tile : (t + 1) * tile].reshape(1, tile)

    barrier = pltpu.get_barrier_semaphore()
    greeted = 0
    for digit in range(4):
        for k in range(1, count[digit]):
            _, device = peer(digit, k)
            pl.semaphore_signal(barrier, inc=1, device_id=device, device_id_type=MESH)
            greeted += 1

    vectors = (preg_ref, pres_ref, qb_ref, vb_ref, ob_ref, midg_ref, mids_ref, outb_ref)

    def vec(row):
        return vectors[row][...].reshape(1, width)

    load_tok.wait()
    x = tok[...].astype(F32)
    center = x - mean(x)
    rstd = lax.rsqrt(mean(center * center) + EPSILON)
    normed = center * rstd
    n1[...] = normed
    stats[0] = jnp.broadcast_to(rstd, (span, LANES))
    first[...] = (normed * vec(0) + vec(1)).astype(BF16)
    load_k.wait()
    keys = dot(first[...], wk[...]).astype(BF16)
    load_v.wait()
    values = (dot(first[...], wv[...]) + vec(3)).astype(BF16)
    for b in range(pairs):
        level[b, :span] = keys[:, b * LANES : (b + 1) * LANES]
        level[pairs + b, :span] = values[:, b * LANES : (b + 1) * LANES]

    def averaging(rows_dim):
        shape = (plan.coarse_rows, span) if rows_dim == 0 else (span, plan.coarse_rows)
        r, p = iota(shape, rows_dim), iota(shape, 1 - rows_dim)
        matrix = jnp.zeros(shape, F32)
        for lv in range(1, top + 1):
            at = plan.level_row[lv]
            hit = (r - at == (p >> lv)) & (r >= at) & (r < at + (span >> lv))
            matrix = jnp.where(hit, 0.5**lv, matrix)
        return matrix.astype(BF16)

    matrix = averaging(0)
    far_at = plan.far_row
    feature = (iota((LANES, span), 0) == ids_ref[...]).astype(F32).astype(BF16)
    unit = (iota((span, span), 0) == iota((span, span), 1)).astype(F32).astype(BF16)
    id_hot = dot_nt(unit, feature).astype(BF16)
    level[blocks, :span] = id_hot
    for half, kv in enumerate((keys, values)):
        mixed = dot(matrix, kv).astype(BF16)
        for b in range(pairs):
            level[half * pairs + b, span : span + far_at] = mixed[
                :far_at, b * LANES : (b + 1) * LANES
            ]
        farg[seq_id, :, half * width : (half + 1) * width] = mixed[far_at:]
    alike = dot(matrix, id_hot)
    alike = jnp.where((alike > 0.999) & (iota(alike.shape, 1) > 0), 1.0, 0.0).astype(BF16)
    level[blocks, span : span + far_at] = alike[:far_at]
    farg[seq_id, :, 2 * width :] = alike[far_at:]

    def level_start(lv):
        return 0 if lv == 0 else span + plan.level_row[lv]

    for lv in range(near + 1):
        at, n = level_start(lv), span >> lv
        edge[0, :, lv * NR : (lv + 1) * NR] = level[:, at : at + NR]
        edge[1, :, lv * NR : (lv + 1) * NR] = level[:, at + n - NR : at + n]

    pl.semaphore_wait(barrier, greeted)

    def far_copy(k):
        _, device = peer(3, k)
        return remote(
            farg.at[seq_id], farg.at[seq_id], far_send.at[k - 1], far_recv.at[k - 1], device
        )

    def halo_copy(src, dst, send, recv, side):
        step = 2 * side - 1
        return remote(
            src.at[side], dst.at[1 - side], send.at[side], recv.at[1 - side],
            (row_id, seq_id + step),
        )

    def halo_start(src, dst, send, recv):
        @pl.when(seq_id > 0)
        def _():
            halo_copy(src, dst, send, recv, 0).start()

        @pl.when(seq_id < seq - 1)
        def _():
            halo_copy(src, dst, send, recv, 1).start()

    def halo_wait(src, dst, send, recv):
        @pl.when(seq_id > 0)
        def _():
            remote(
                src.at[0], dst.at[0], send.at[0], recv.at[0], (row_id, seq_id - 1)
            ).wait()

        @pl.when(seq_id < seq - 1)
        def _():
            remote(
                src.at[1], dst.at[1], send.at[1], recv.at[1], (row_id, seq_id + 1)
            ).wait()

    halo_start(edge, halo, halo_send, halo_recv)
    for k in range(1, seq):
        far_copy(k).start()

    load_q.wait()
    query = ((dot(first[...], wq[...]) + vec(2)).astype(BF16) * (1.0 / math.sqrt(HEAD_DIM))).astype(
        BF16
    )
    for b in range(pairs):
        qh[b] = query[:, b * LANES : (b + 1) * LANES]

    def slot_pieces(c):
        pieces = []
        for lv in range(near + 1):
            at, n = level_start(lv), span >> lv
            per = plan.chunk >> lv
            s0 = plan.slot[lv]
            if per >= NR:
                low, high = c * per - NR, c * per + per + NR
            else:
                low, high = -NR, n + NR
            if low < 0:
                pieces.append((s0, "low", lv * NR, NR))
                s0, low = s0 + NR, 0
            inner = min(high, n)
            pieces.append((s0, "own", at + low, inner - low))
            s0 += inner - low
            if high > n:
                pieces.append((s0, "high", lv * NR, NR))
        return pieces

    slot_at = iota((1, plan.slots), 1)
    slot_level = jnp.zeros((1, plan.slots), jnp.int32)
    for lv in range(1, top + 1):
        slot_level = slot_level + (slot_at >= plan.slot[lv]).astype(jnp.int32)
    for c in range(plan.chunks):
        origin = start + c * plan.chunk
        j = slot_at
        for lv in range(top + 1):
            if (plan.chunk >> lv) >= NR:
                base = origin // (1 << lv) - NR
            else:
                base = (origin // (NR << lv) - 1) * NR
            here = slot_at - plan.slot[lv] + base
            j = here if lv == 0 else jnp.where(slot_level == lv, here, j)
        position = origin + iota((plan.chunk, plan.slots), 0)
        off_block = (j >> 4) - (position >> (slot_level + 4))
        off_half = (j >> 3) - (position >> (slot_level + 3))
        reach = jnp.where(slot_level == 0, -1, 1)
        within = (jnp.abs(off_block) <= 1) & (jnp.abs(off_half) > reach)
        bias[c] = jnp.where(within, slot_level.astype(F32) * LOG_TWO, MASKED)

    def far_select():
        pieces = []
        for lv in plan.far:
            per_log = (span >> lv).bit_length() - 1
            first_row = plan.level_row[lv] - plan.far_row
            j = (start // (NR << lv) - 1) * NR + iota((3 * NR, seq * NR), 0)
            column = (j >> per_log) * NR + (j & ((1 << per_log) - 1)) + first_row
            pieces.append((column == iota((3 * NR, seq * NR), 1)).astype(F32))
        rest = plan.far_slots - 3 * NR * len(plan.far)
        if rest:
            pieces.append(jnp.zeros((rest, seq * NR), F32))
        return jnp.concatenate(pieces, axis=0).astype(BF16)

    select = far_select()
    spread[...] = averaging(1)

    halo_wait(edge, halo, halo_send, halo_recv)
    for c in range(plan.chunks):
        for s0, kind, at, n in slot_pieces(c):
            if kind == "own":
                slots[c, :, s0 : s0 + n] = level[:, at : at + n]
            else:
                slots[c, :, s0 : s0 + n] = halo[0 if kind == "low" else 1, :, at : at + n]
    for k in range(1, seq):
        far_copy(k).wait()
    far_values = dot(select, farg[...].reshape(seq * NR, 2 * width + LANES)).astype(BF16)
    for c in range(plan.chunks):
        for b in range(blocks + 1):
            slots[c, b, plan.far_slot :] = far_values[:, b * LANES : (b + 1) * LANES]
    for c in range(plan.chunks):
        same = dot_nt(level[blocks, c * plan.chunk : (c + 1) * plan.chunk], slots[c, blocks])
        bias[c] = jnp.where(same > 0.5, bias[c], MASKED)

    lane = iota((1, LANES), 1)
    low_half = (lane < HEAD_DIM).astype(F32).astype(BF16)
    high_half = (lane >= HEAD_DIM).astype(F32).astype(BF16)
    low_lanes = iota((plan.chunk, LANES), 1) < HEAD_DIM

    def two_heads(block):
        return jnp.concatenate([block * low_half, block * high_half], axis=0)

    def merge_heads(both):
        return jnp.where(low_lanes, both[: plan.chunk], both[plan.chunk :])

    def chunk_rows(c):
        return pl.ds(pl.multiple_of(c * plan.chunk, plan.chunk), plan.chunk)

    def pair_lanes(b):
        return pl.ds(pl.multiple_of(b * LANES, LANES), LANES)

    def attend(i, carry):
        c, b = i // pairs, i % pairs
        q2 = two_heads(qh[b, chunk_rows(c)])
        offset = bias[c]
        score = dot_nt(q2, slots[c, b]) + jnp.concatenate([offset, offset], axis=0)
        peak = jnp.max(score, axis=1, keepdims=True)
        raised = jnp.exp(score - peak)
        prob = raised * (1.0 / jnp.sum(raised, axis=1, keepdims=True))
        low = prob.astype(BF16)
        probs[i] = low
        att[chunk_rows(c), pair_lanes(b)] = merge_heads(dot(low, slots[c, pairs + b])).astype(BF16)
        return carry

    lax.fori_loop(0, plan.chunks * pairs, attend, 0)

    received = [recv0, recv1, recv2, recv3]

    def region(part, digits):
        n = plan.parts[0][1]
        base = part * n
        for digit in range(digits):
            n = n // count[digit]
            base = base + index[digit] * n
        return base, n

    def rows_at(base, n):
        return pl.ds(pl.multiple_of(base, NR), n)

    def received_rows(part, n):
        return rows_at(part * n, n)

    def rs_copy(part, digit, k):
        base, n = region(part, digit)
        other, device = peer(digit, k)
        if digit == 3 and not plan.scatter:
            return remote(
                grads.at[rows_at(base, n)],
                received[digit].at[k - 1, received_rows(part, n)],
                rs_send.at[part, digit, k - 1], rs_recv.at[part, digit, k - 1], device,
            )
        n = n // count[digit]
        return remote(
            grads.at[rows_at(base + other * n, n)],
            received[digit].at[k - 1, received_rows(part, n)],
            rs_send.at[part, digit, k - 1], rs_recv.at[part, digit, k - 1], device,
        )

    def rs_start(part, digit):
        for k in range(1, count[digit]):
            rs_copy(part, digit, k).start()

    def rs_finish(part, digit):
        for k in range(1, count[digit]):
            rs_copy(part, digit, k).wait_recv()
        gather_all = digit == 3 and not plan.scatter
        base, n = region(part, digit if gather_all else digit + 1)
        at = part * n
        target = red_ref if digit == 3 else grads
        block = 64 if n % 64 == 0 else NR

        def add(i, carry):
            here = rows_at(base + i * block, block)
            there = pl.ds(pl.multiple_of(at + i * block, NR), block)
            if gather_all:
                acc = jnp.zeros((block, width), F32)
                for s in range(seq):
                    slot = (seq_id - s + seq - 1) % seq
                    theirs = received[digit][jnp.minimum(slot, seq - 2), there].astype(F32)
                    acc = acc + jnp.where(seq_id == s, grads[here].astype(F32), theirs)
            else:
                acc = grads[here].astype(F32)
                for k in range(1, count[digit]):
                    acc = acc + received[digit][k - 1, there].astype(F32)
            target[here] = acc.astype(BF16)
            return carry

        lax.fori_loop(0, n // block, add, 0)

    def ag_copy(part, digit, k):
        base, n = region(part, digit + 1)
        _, device = peer(digit, k)
        return remote(
            red_ref.at[rows_at(base, n)], red_ref.at[rows_at(base, n)],
            ag_send.at[part, digit, k - 1], ag_recv.at[part, digit, k - 1], device,
        )

    def ag_start(part, digit):
        if digit == 3 and not plan.scatter:
            return
        for k in range(1, count[digit]):
            ag_copy(part, digit, k).start()

    def ag_finish(part, digit):
        if digit == 3 and not plan.scatter:
            return
        for k in range(1, count[digit]):
            ag_copy(part, digit, k).wait_recv()

    def part_steps(part):
        steps = [functools.partial(rs_start, part, 0)]
        for digit in range(1, 4):
            steps.append(
                functools.partial(
                    sequence,
                    functools.partial(rs_finish, part, digit - 1),
                    functools.partial(rs_start, part, digit),
                )
            )
        steps.append(
            functools.partial(
                sequence, functools.partial(rs_finish, part, 3), functools.partial(ag_start, part, 3)
            )
        )
        for digit in (2, 1, 0):
            steps.append(
                functools.partial(
                    sequence,
                    functools.partial(ag_finish, part, digit + 1),
                    functools.partial(ag_start, part, digit),
                )
            )
        steps.append(
            functools.partial(
                sequence, functools.partial(ag_finish, part, 0), lambda: put(part).start()
            )
        )
        return steps

    def put(part):
        off, n = plan.parts[part]
        rows = slice(off, off + n)
        return pltpu.make_async_copy(red_ref.at[rows], red_hbm.at[rows], out_sem.at[part])

    all_steps = [part_steps(part) for part in range(len(plan.parts))]

    def step(part, number):
        all_steps[part][number]()

    load_o.wait()
    load_up.wait()
    res = tok[...].astype(F32) + dot(att[...], wo[...]) + vec(4)
    mid[...] = res
    center = res - mean(res)
    rstd = lax.rsqrt(mean(center * center) + EPSILON)
    normed = center * rstd
    n2[...] = normed
    stats[1] = jnp.broadcast_to(rstd, (span, LANES))
    second[...] = (normed * vec(5) + vec(6)).astype(BF16)
    racc[...] = jnp.zeros_like(racc)
    dsec[...] = jnp.zeros_like(dsec)
    for copy in load_1:
        copy.wait()
    load_2.wait()
    curve = math.sqrt(2.0 / math.pi)

    def feed(t, carry):
        w2_rows = pl.ds(pl.multiple_of(t * tile, tile), tile)
        pre = dot(second[...], w1[t]) + inb[pl.ds(t, 1), :]
        square = pre * pre
        bend = jnp.tanh(curve * (pre + 0.044715 * (square * pre)))
        half = 0.5 * (1.0 + bend)
        act = (pre * half).astype(BF16)
        slope = half + 0.5 * pre * (1.0 - bend * bend) * (curve * (1.0 + 3 * 0.044715 * square))
        upstream = up[...]
        racc[...] += dot(act, w2[w2_rows])
        d_pre = (dot_nt(upstream, w2[w2_rows]) * slope).astype(BF16)
        base = 2 * t * tile
        grads[rows_at(base, tile)] = dot_tn(act, upstream).astype(BF16)
        grads[rows_at(base + tile, tile)] = dot_tn(second[...], d_pre).astype(BF16)
        rs_start(t, 0)
        vstage[0, pl.ds(V_INNB + t, 1), :] = total(d_pre.astype(F32))
        dsec[...] += dot_nt(d_pre, w1[t])

        for when in range(2, tiles):

            @pl.when(t == when)
            def _():
                step(when - 2, 1)

        return carry

    lax.fori_loop(0, tiles, feed, 0)
    out_ref[0] = (mid[...] + racc[...] + vec(7)).astype(BF16)

    up_f = up[...].astype(F32)
    vstage[0, V_OUTB : V_OUTB + 1] = total(up_f)
    d_second, normed = dsec[...], n2[...]
    scaled = d_second * vec(5)
    vstage[0, V_MIDG : V_MIDG + 1] = total(d_second * normed)
    vstage[0, V_MIDS : V_MIDS + 1] = total(d_second)
    d_mid = up_f + (scaled - mean(scaled) - normed * mean(scaled * normed)) * stats[1][:, :1]
    mid[...] = d_mid
    d_branch = d_mid.astype(BF16)
    vstage[0, V_OB : V_OB + 1] = total(d_branch.astype(F32))
    grads[2 * hidden : 2 * hidden + width] = dot_tn(att[...], d_branch).astype(BF16)
    d_att = dot_nt(d_branch, wo[...]).astype(BF16)
    for b in range(pairs):
        dah[b] = d_att[:, b * LANES : (b + 1) * LANES]

    step(tiles - 2, 1)
    schedule = {
        0: [(tiles - 1, 1)],
        2: [(0, 2)],
        4: [(1, 2)],
        6: [(2, 2)],
    }

    def attend_back(i, carry):
        c, b = i // pairs, i % pairs
        q2 = two_heads(qh[b, chunk_rows(c)])
        g2 = two_heads(dah[b, chunk_rows(c)])
        low = probs[i]
        prob = low.astype(F32)
        d_prob = dot_nt(g2, slots[c, pairs + b])
        weighted = prob * d_prob
        d_score = (weighted - prob * jnp.sum(weighted, axis=1, keepdims=True)).astype(BF16)
        d_query = merge_heads(dot(d_score, slots[c, b])) * (1.0 / math.sqrt(HEAD_DIM))
        dq[chunk_rows(c), pair_lanes(b)] = d_query.astype(BF16)
        dslots[c, b] = dot_tn(d_score, q2)
        dslots[c, pairs + b] = dot_tn(low, g2)
        for when, steps in schedule.items():

            @pl.when(i == when)
            def _():
                for item in steps:
                    step(*item)

        return carry

    lax.fori_loop(0, plan.chunks * pairs, attend_back, 0)
    step(3, 2)

    def fold(b, carry):
        for c in range(plan.chunks):
            for s0, kind, at, n in slot_pieces(c):
                piece = dslots[c, b, s0 : s0 + n]
                if kind == "own":
                    parts_done = own_done[c].get((s0, at))
                    seen = parts_done if parts_done is not None else 0
                    if seen:
                        own[b, at : at + seen] += piece[:seen]
                    if seen < n:
                        own[b, at + seen : at + n] = piece[seen:]
                elif own_done[c].get((s0, kind)):
                    side = 0 if kind == "low" else 1
                    hsend[side, b, at : at + n] = (
                        hsend[side, b, at : at + n].astype(F32) + piece
                    ).astype(BF16)
                else:
                    side = 0 if kind == "low" else 1
                    hsend[side, b, at : at + n] = piece.astype(BF16)
        far = dslots[0, b, plan.far_slot :]
        for c in range(1, plan.chunks):
            far = far + dslots[c, b, plan.far_slot :]
        back = dot_tn(select, far.astype(BF16))
        for s in range(seq):
            fsend[s, b] = back[s * NR : (s + 1) * NR].astype(BF16)
        return carry

    own_done = []
    reached, halo_seen = {}, set()
    for c in range(plan.chunks):
        done = {}
        for s0, kind, at, n in slot_pieces(c):
            if kind == "own":
                lv = max(v for v in range(near + 1) if level_start(v) <= at)
                limit = reached.get(lv, level_start(lv))
                done[(s0, at)] = max(0, min(limit, at + n) - at)
                reached[lv] = max(limit, at + n)
            else:
                done[(s0, kind)] = (kind, at) in halo_seen
                halo_seen.add((kind, at))
        own_done.append(done)

    lax.fori_loop(0, blocks, fold, 0)

    def far_back(k):
        other, device = peer(3, k)
        return remote(
            fsend.at[other], frecv.at[k - 1], fback_send.at[k - 1], fback_recv.at[k - 1], device
        )

    halo_start(hsend, hrecv, back_send, back_recv)
    for k in range(1, seq):
        far_back(k).start()

    d_query = dq[...]
    vstage[0, V_QB : V_QB + 1] = total(d_query.astype(F32))
    off_c = 2 * hidden + width
    grads[off_c : off_c + width] = dot_tn(first[...], d_query).astype(BF16)
    d_first = dot_nt(d_query, wq[...])
    racc[...] = d_first
    step(4, 0)
    step(0, 3)

    halo_wait(hsend, hrecv, back_send, back_recv)
    for k in range(1, seq):
        far_back(k).wait()
    for lv in range(near + 1):
        at, n = level_start(lv), span >> lv
        lo, hi = lv * NR, (lv + 1) * NR
        own[:, at : at + NR] += hrecv[0, :, lo:hi].astype(F32)
        own[:, at + n - NR : at + n] += hrecv[1, :, lo:hi].astype(F32)
    far_sum = fsend[seq_id].astype(F32)
    for k in range(1, seq):
        far_sum = far_sum + frecv[k - 1].astype(F32)
    for b in range(blocks):
        cols = slice(b * LANES, (b + 1) * LANES)
        coarse[:far_at, cols] = own[b, span : span + far_at].astype(BF16)
        coarse[far_at:, cols] = far_sum[b].astype(BF16)
    for half in range(2):
        passed = dot(spread[...], coarse[:, half * width : (half + 1) * width])
        for b in range(pairs):
            cols = slice((half * pairs + b) * LANES, (half * pairs + b + 1) * LANES)
            dkv[:, cols] = (
                own[half * pairs + b, :span] + passed[:, b * LANES : (b + 1) * LANES]
            ).astype(BF16)
    d_keys, d_values = dkv[:, :width], dkv[:, width:]
    vstage[0, V_VB : V_VB + 1] = total(d_values.astype(F32))
    grads[off_c + width : off_c + 2 * width] = dot_tn(first[...], d_keys).astype(BF16)
    grads[off_c + 2 * width : off_c + 3 * width] = dot_tn(first[...], d_values).astype(BF16)
    step(5, 0)
    step(1, 3)
    step(4, 1)
    step(2, 3)
    d_first = racc[...] + dot_nt(d_keys, wk[...]) + dot_nt(d_values, wv[...])
    normed = n1[...]
    scaled = d_first * vec(0)
    vstage[0, V_PREG : V_PREG + 1] = total(d_first * normed)
    vstage[0, V_PRES : V_PRES + 1] = total(d_first)
    d_in = mid[...] + (scaled - mean(scaled) - normed * mean(scaled * normed)) * stats[0][:, :1]
    gin_ref[0] = d_in.astype(BF16)

    vec_received = [vrecv0, vrecv1, vrecv2, vrecv3]

    def vec_copy(digit, k):
        _, device = peer(digit, k)
        return remote(
            vstage.at[digit], vec_received[digit].at[index[digit]],
            vec_send.at[digit, k - 1], vec_recv.at[digit, k - 1], device,
        )

    def vec_start(digit):
        for k in range(1, count[digit]):
            vec_copy(digit, k).start()

    def vec_finish(digit):
        for k in range(1, count[digit]):
            vec_copy(digit, k).wait_recv()
        acc = jnp.zeros((VEC_ROWS, width), F32)
        for s in range(count[digit]):
            acc = acc + jnp.where(index[digit] == s, vstage[digit], vec_received[digit][s])
        if digit == 3:
            vout_ref[...] = acc
        else:
            vstage[digit + 1] = acc

    vec_start(0)
    tail = [
        (3, 3), (0, 4), (1, 4), "v0", (4, 2), (5, 1), (2, 4), "v1", (4, 3), (3, 4), (5, 2), (0, 5),
        "v2", (5, 3), (1, 5), (0, 6), (2, 5), "v3", (1, 6), (4, 4), (0, 7), (2, 6), (0, 8), (3, 5),
        (1, 7), (5, 4), (1, 8), (2, 7), (4, 5), (3, 6), (2, 8), (5, 5), (4, 6), (3, 7), (5, 6),
        (3, 8), (4, 7), (5, 7), (4, 8), (5, 8),
    ]
    for item in tail:
        if isinstance(item, str):
            digit = int(item[1])
            vec_finish(digit)
            if digit < 3:
                vec_start(digit + 1)
        else:
            step(*item)

    for part in range(len(plan.parts)):
        for digit in range(4):
            for k in range(1, count[digit]):
                rs_copy(part, digit, k).wait_send()
                if digit < 3 or plan.scatter:
                    ag_copy(part, digit, k).wait_send()
        put(part).wait()
    for digit in range(4):
        for k in range(1, count[digit]):
            vec_copy(digit, k).wait_send()


def unpack_kernel(
    width, tiles, red_hbm, vec_ref, out_hbm, gin_hbm,
    query_ref, key_ref, value_ref, output_ref, inner_ref, outer_ref,
    preg_ref, pres_ref, qb_ref, vb_ref, ob_ref, midg_ref, mids_ref, outb_ref, innb_ref,
    out_ref, gin_ref, low, wide, through, in_sem, out_sem, through_in, through_out,
):
    targets = []
    for t in range(tiles):
        rows = slice(t * width, (t + 1) * width)
        targets.append(outer_ref.at[rows])
        targets.append(inner_ref.at[:, rows])
    targets += [output_ref, query_ref, key_ref, value_ref]

    def fetch(i):
        return pltpu.make_async_copy(
            red_hbm.at[i * width : (i + 1) * width], low.at[i % 4], in_sem.at[i % 4]
        )

    def put(i):
        return pltpu.make_async_copy(wide.at[i % 4], targets[i], out_sem.at[i % 4])

    def take(i):
        return pltpu.make_async_copy((out_hbm, gin_hbm)[i], through.at[i], through_in.at[i])

    def give(i):
        return pltpu.make_async_copy(through.at[i], (out_ref, gin_ref)[i], through_out.at[i])

    n = len(targets)
    for i in range(3):
        fetch(i).start()
    for i in range(2):
        take(i).start()
    for row, ref in (
        (V_PREG, preg_ref), (V_PRES, pres_ref), (V_QB, qb_ref), (V_VB, vb_ref), (V_OB, ob_ref),
        (V_MIDG, midg_ref), (V_MIDS, mids_ref), (V_OUTB, outb_ref),
    ):
        ref[...] = vec_ref[row]
    for t in range(tiles):
        innb_ref[t * width : (t + 1) * width] = vec_ref[V_INNB + t]
    for i in range(n):
        fetch(i).wait()
        if i >= 4:
            put(i - 4).wait()
        wide[i % 4] = low[i % 4].astype(F32)
        put(i).start()
        if i + 3 < n:
            fetch(i + 3).start()
        if 2 <= i < 4:
            take(i - 2).wait()
            give(i - 2).start()
    for i in range(n - 4, n):
        put(i).wait()
    for i in range(2):
        give(i).wait()


def shards(
    rows, seq,
    tokens, segment_ids, prenorm_gain, prenorm_shift, query_proj, query_bias, key_proj, value_proj,
    value_bias, output_proj, output_bias, midnorm_gain, midnorm_shift, inner_proj, inner_bias,
    outer_proj, outer_bias, upstream,
):
    _, span, width = tokens.shape
    hidden = inner_proj.shape[1]
    plan = Plan(rows, seq, span, width, hidden)
    tiles = hidden // width
    pairs = width // LANES
    count = plan.counts
    most = max(count) - 1
    vmem = pl.BlockSpec(memory_space=pltpu.VMEM)
    hbm = pl.BlockSpec(memory_space=pl.ANY)
    grad_rows = plan.grad_rows
    rest = [grad_rows // 2, grad_rows // 4, grad_rows // 4 // count[2]]
    last = rest[2] // seq if plan.scatter else rest[2]
    dma = pltpu.SemaphoreType.DMA
    items = plan.chunks * pairs
    n_parts = len(plan.parts)
    scratch = [
        pltpu.VMEM((span, width), BF16),
        pltpu.VMEM((span, width), BF16),
        pltpu.VMEM((width, width), BF16),
        pltpu.VMEM((width, width), BF16),
        pltpu.VMEM((width, width), BF16),
        pltpu.VMEM((width, width), BF16),
        pltpu.VMEM((tiles, width, width), BF16),
        pltpu.VMEM((hidden, width), BF16),
        pltpu.VMEM((span, width), F32),
        pltpu.VMEM((span, width), F32),
        pltpu.VMEM((span, width), F32),
        pltpu.VMEM((span, width), F32),
        pltpu.VMEM((span, width), F32),
        pltpu.VMEM((span, width), BF16),
        pltpu.VMEM((span, width), BF16),
        pltpu.VMEM((pairs, span, LANES), BF16),
        pltpu.VMEM((span, width), BF16),
        pltpu.VMEM((pairs, span, LANES), BF16),
        pltpu.VMEM((span, width), BF16),
        pltpu.VMEM((2 * pairs + 1, span + plan.far_row, LANES), BF16),
        pltpu.VMEM((2, 2 * pairs + 1, plan.edge, LANES), BF16),
        pltpu.VMEM((2, 2 * pairs + 1, plan.edge, LANES), BF16),
        pltpu.VMEM((seq, NR, 2 * width + LANES), BF16),
        pltpu.VMEM((plan.chunks, 2 * pairs + 1, plan.slots, LANES), BF16),
        pltpu.VMEM((plan.chunks, plan.chunk, plan.slots), F32),
        pltpu.VMEM((items, 2 * plan.chunk, plan.slots), BF16),
        pltpu.VMEM((plan.chunks, 2 * pairs, plan.slots, LANES), F32),
        pltpu.VMEM((2 * pairs, span + plan.far_row, LANES), F32),
        pltpu.VMEM((2, 2 * pairs, plan.edge, LANES), BF16),
        pltpu.VMEM((2, 2 * pairs, plan.edge, LANES), BF16),
        pltpu.VMEM((seq, 2 * pairs, NR, LANES), BF16),
        pltpu.VMEM((seq - 1, 2 * pairs, NR, LANES), BF16),
        pltpu.VMEM((plan.coarse_rows, 2 * width), BF16),
        pltpu.VMEM((span, plan.coarse_rows), BF16),
        pltpu.VMEM((span, 2 * width), BF16),
        pltpu.VMEM((grad_rows, width), BF16),
        pltpu.VMEM((count[0] - 1, rest[0], width), BF16),
        pltpu.VMEM((count[1] - 1, rest[1], width), BF16),
        pltpu.VMEM((count[2] - 1, rest[2], width), BF16),
        pltpu.VMEM((count[3] - 1, last, width), BF16),
        pltpu.VMEM((4, VEC_ROWS, width), F32),
        pltpu.VMEM((count[0], VEC_ROWS, width), F32),
        pltpu.VMEM((count[1], VEC_ROWS, width), F32),
        pltpu.VMEM((count[2], VEC_ROWS, width), F32),
        pltpu.VMEM((count[3], VEC_ROWS, width), F32),
        pltpu.VMEM((2, span, LANES), F32),
        pltpu.VMEM((tiles, width), F32),
        pltpu.VMEM((grad_rows, width), BF16),
        dma((7 + tiles,)),
        dma((n_parts,)),
        dma((2,)), dma((2,)),
        dma((seq - 1,)), dma((seq - 1,)),
        dma((2,)), dma((2,)),
        dma((seq - 1,)), dma((seq - 1,)),
        dma((n_parts, 4, most)), dma((n_parts, 4, most)),
        dma((n_parts, 4, most)), dma((n_parts, 4, most)),
        dma((4, most)), dma((4, most)),
    ]
    layer_output, input_grad, reduced, vecs = pl.pallas_call(
        functools.partial(layer_kernel, plan),
        out_shape=(
            jax.ShapeDtypeStruct(tokens.shape, BF16),
            jax.ShapeDtypeStruct(tokens.shape, BF16),
            jax.ShapeDtypeStruct((grad_rows, width), BF16),
            jax.ShapeDtypeStruct((VEC_ROWS, width), F32),
        ),
        in_specs=[
            hbm, vmem, vmem, vmem, hbm, vmem, hbm, hbm, vmem, hbm, vmem, vmem, vmem, hbm, vmem, hbm,
            vmem, hbm,
        ],
        out_specs=(vmem, vmem, hbm, vmem),
        scratch_shapes=scratch,
        compiler_params=pltpu.CompilerParams(
            collective_id=0, has_side_effects=True, vmem_limit_bytes=60 * 1024 * 1024
        ),
        name="layer",
    )(
        tokens, segment_ids, prenorm_gain, prenorm_shift, query_proj, query_bias, key_proj,
        value_proj, value_bias, output_proj, output_bias, midnorm_gain, midnorm_shift, inner_proj,
        inner_bias, outer_proj, outer_bias, upstream,
    )
    matrix = jax.ShapeDtypeStruct((width, width), F32)
    vector = jax.ShapeDtypeStruct((width,), F32)
    grads = pl.pallas_call(
        functools.partial(unpack_kernel, width, tiles),
        out_shape=(
            matrix, matrix, matrix, matrix,
            jax.ShapeDtypeStruct((width, hidden), F32),
            jax.ShapeDtypeStruct((hidden, width), F32),
            vector, vector, vector, vector, vector, vector, vector, vector,
            jax.ShapeDtypeStruct((hidden,), F32),
            jax.ShapeDtypeStruct(tokens.shape, BF16),
            jax.ShapeDtypeStruct(tokens.shape, BF16),
        ),
        in_specs=[hbm, vmem, hbm, hbm],
        out_specs=(hbm,) * 6 + (vmem,) * 9 + (hbm,) * 2,
        scratch_shapes=[
            pltpu.VMEM((4, width, width), BF16),
            pltpu.VMEM((4, width, width), F32),
            pltpu.VMEM((2, 1, span, width), BF16),
            dma((4,)), dma((4,)), dma((2,)), dma((2,)),
        ],
        name="unpack",
    )(reduced, vecs, layer_output, input_grad)
    (query_g, key_g, value_g, output_g, inner_g, outer_g,
     preg, pres, qb, vb, ob, midg, mids, outb, innb, layer_output, input_grad) = grads
    return (
        layer_output, input_grad, preg, pres, query_g, qb, key_g, value_g, vb, output_g, ob,
        midg, mids, inner_g, innb, outer_g, outb,
    )


def solution(mesh):
    split, ids, whole = P("rows", "seq", None), P("rows", "seq"), P()
    in_specs = (split, ids) + (whole,) * 15 + (split,)
    out_specs = (split, split) + (whole,) * 15
    return jax.shard_map(
        functools.partial(shards, mesh.shape["rows"], mesh.shape["seq"]),
        mesh=mesh, in_specs=in_specs, out_specs=out_specs, check_vma=False,
    )
```

```python
import functools
import math

import jax
import jax.numpy as jnp
from jax import lax
from jax.experimental import pallas as pl
from jax.experimental.pallas import tpu as pltpu
from jax.sharding import PartitionSpec as P

HEADS = 8
HEAD_DIM = 64
NR = 16
LANES = 128
LOG_TWO = math.log(2.0)
EPSILON = 1e-05
MASKED = -1e30
F32 = jnp.float32
BF16 = jnp.bfloat16
MESH = pl.DeviceIdType.MESH

VEC_ROWS = 16
V_PREG, V_PRES, V_QB, V_VB, V_OB, V_MIDG, V_MIDS, V_OUTB, V_INNB = 0, 1, 2, 3, 4, 5, 6, 7, 8


def dot(a, b):
    return jnp.dot(a, b, preferred_element_type=F32)


def dot_nt(a, b):
    return lax.dot_general(a, b, (((1,), (1,)), ((), ())), preferred_element_type=F32)


def dot_tn(a, b):
    return lax.dot_general(a, b, (((0,), (0,)), ((), ())), preferred_element_type=F32)


def iota(shape, dim):
    return lax.broadcasted_iota(jnp.int32, shape, dim)


def mean(x):
    return jnp.mean(x, axis=-1, keepdims=True)


def total(x):
    return jnp.sum(x, axis=0, keepdims=True)


ORDER = {
    "f2": [0, 1],
    "f3": [2, 3],
    "ln2": [4],
    "b0": [5],
    "b1": [0, 6],
    "b2": [1, 7, 8],
    "b4": [2],
    "b6": [0],
    "b7": [3, 1],
    "fold": [2],
    "q": [4, 0, 3, 1, 5, 9, 4, 6, 5, 7],
    "ln1": [
        2, 6, 8, 0, 7, 10, 9, 11, 3, 8, 1, 0, 4, -1, 9, 10, 5, 1, 2, 11, 6, 10, 0, -1,
        7, 2, 3, 0, 11, 1, 8, 4, 1, 2, 3, 9, -1, 4, 5, 2, 6, 3, 10, 5, 3, 7, 4, 6,
        11, -1, 8, 4, 5, 7, 9, 6, 10, 8, 5, 11, 6, 9, 7, 10, 7, 11, 8, 9, 8, 10, 9, 11,
        10, 11,
    ],
}


class Plan:
    def __init__(self, rows, seq, span, width, hidden):
        self.rows, self.seq, self.span, self.width, self.hidden = rows, seq, span, width, hidden
        self.near = (span // NR).bit_length() - 1
        self.length = span * seq
        self.top = (self.length // NR).bit_length() - 2
        self.chunk = 128
        self.chunks = span // self.chunk
        self.far = list(range(self.near + 1, self.top + 1))
        self.level_row = [0]
        at = 0
        for level in range(1, self.near + 1):
            self.level_row.append(at)
            at += span >> level
        self.far_row = at
        for level in self.far:
            self.level_row.append(at)
            at += span >> level
        self.coarse_rows = self.far_row + NR
        self.slot, self.slot_len = [], []
        at = 0
        for level in range(self.top + 1):
            n = 2 * NR + max(self.chunk >> level, NR)
            self.slot.append(at)
            self.slot_len.append(n)
            at += n
        self.used = at
        self.slots = -(-at // LANES) * LANES
        self.far_slot = self.slot[self.near + 1]
        self.far_slots = self.slots - self.far_slot
        self.edge = NR * (self.near + 1)
        self.grad_rows = 4 * width + 2 * hidden
        self.parts = [(p * width, width) for p in range(self.grad_rows // width)]
        self.counts = [2, 2, rows // 4, seq]
        self.swap = rows // 4 == 2
        self.scatter = (width // rows) % (NR * seq) == 0


def sequence(*steps):
    for step in steps:
        step()


def layer_kernel(
    plan,
    tok_hbm, ids_ref, preg_ref, pres_ref, wq_hbm, qb_ref, wk_hbm, wv_hbm, vb_ref, wo_hbm, ob_ref,
    midg_ref, mids_ref, w1_hbm, inb_ref, w2_hbm, outb_ref, up_hbm,
    out_ref, gin_ref, red_hbm, vout_ref,
    tok, up, wq, wk, wv, wo, w1, w2, n1, n2, mid, racc, dsec, first, second, qh, att, dah, dq,
    level, edge, halo, farg, slots, bias, probs, dslots, own, hsend, hrecv, fsend, frecv,
    coarse, spread, dkv, grads, recv0, recv1, recv2, recv3, vstage, vrecv0, vrecv1, vrecv2, vrecv3, stats,
    inb, red_ref,
    in_sem, out_sem, halo_send, halo_recv, far_send, far_recv, back_send, back_recv, fback_send, fback_recv,
    rs_send, rs_recv, ag_send, ag_recv, vec_send, vec_recv,
):
    span, width, hidden = plan.span, plan.width, plan.hidden
    seq, near, top = plan.seq, plan.near, plan.top
    tile = hidden // w1.shape[0]
    tiles = w1.shape[0]
    pairs = width // LANES
    blocks = 2 * pairs
    row_id, seq_id = lax.axis_index("rows"), lax.axis_index("seq")
    start = seq_id * span

    core = row_id % 2
    if plan.swap:
        stride_a, stride_b = 2 + 2 * core, 4 - 2 * core
    else:
        stride_a, stride_b = 2, 4
    count = plan.counts
    index = [
        core,
        (row_id // stride_a) % count[1],
        (row_id // stride_b) % count[2],
        seq_id,
    ]

    def peer(digit, k):
        other = (index[digit] + k) % count[digit]
        if digit == 3:
            return other, (row_id, other)
        stride = [1, stride_a, stride_b][digit]
        return other, (row_id + (other - index[digit]) * stride, seq_id)

    def remote(src, dst, send, recv, device):
        return pltpu.make_async_remote_copy(
            src_ref=src, dst_ref=dst, send_sem=send, recv_sem=recv,
            device_id=device, device_id_type=MESH,
        )

    loads = []

    def load(src, dst):
        copy = pltpu.make_async_copy(src, dst, in_sem.at[len(loads)])
        copy.start()
        loads.append(copy)
        return copy

    load_tok = load(tok_hbm.at[0], tok)
    load_q = load(wq_hbm, wq)
    load_k = load(wk_hbm, wk)
    load_v = load(wv_hbm, wv)
    load_up = load(up_hbm.at[0], up)
    load_o = load(wo_hbm, wo)
    load_1 = [load(w1_hbm.at[:, t * tile : (t + 1) * tile], w1.at[t]) for t in range(tiles)]
    load_2 = load(w2_hbm, w2)

    halo[...] = jnp.zeros_like(halo)
    hrecv[...] = jnp.zeros_like(hrecv)
    vstage[0] = jnp.zeros((VEC_ROWS, width), F32)
    for t in range(tiles):
        inb[t : t + 1, :] = inb_ref[t * tile : (t + 1) * tile].reshape(1, tile)

    barrier = pltpu.get_barrier_semaphore()
    greeted = 0
    for digit in range(4):
        for k in range(1, count[digit]):
            _, device = peer(digit, k)
            pl.semaphore_signal(barrier, inc=1, device_id=device, device_id_type=MESH)
            greeted += 1

    vectors = (preg_ref, pres_ref, qb_ref, vb_ref, ob_ref, midg_ref, mids_ref, outb_ref)

    def vec(row):
        return vectors[row][...].reshape(1, width)

    load_tok.wait()
    x = tok[...].astype(F32)
    center = x - mean(x)
    rstd = lax.rsqrt(mean(center * center) + EPSILON)
    normed = center * rstd
    n1[...] = normed
    stats[0] = jnp.broadcast_to(rstd, (span, LANES))
    first[...] = (normed * vec(0) + vec(1)).astype(BF16)
    load_k.wait()
    keys = dot(first[...], wk[...]).astype(BF16)
    load_v.wait()
    values = (dot(first[...], wv[...]) + vec(3)).astype(BF16)
    for b in range(pairs):
        level[b, :span] = keys[:, b * LANES : (b + 1) * LANES]
        level[pairs + b, :span] = values[:, b * LANES : (b + 1) * LANES]

    def averaging(rows_dim):
        shape = (plan.coarse_rows, span) if rows_dim == 0 else (span, plan.coarse_rows)
        r, p = iota(shape, rows_dim), iota(shape, 1 - rows_dim)
        matrix = jnp.zeros(shape, F32)
        for lv in range(1, top + 1):
            at = plan.level_row[lv]
            hit = (r - at == (p >> lv)) & (r >= at) & (r < at + (span >> lv))
            matrix = jnp.where(hit, 0.5**lv, matrix)
        return matrix.astype(BF16)

    matrix = averaging(0)
    far_at = plan.far_row
    feature = (iota((LANES, span), 0) == ids_ref[...]).astype(F32).astype(BF16)
    unit = (iota((span, span), 0) == iota((span, span), 1)).astype(F32).astype(BF16)
    id_hot = dot_nt(unit, feature).astype(BF16)
    level[blocks, :span] = id_hot
    for half, kv in enumerate((keys, values)):
        mixed = dot(matrix, kv).astype(BF16)
        for b in range(pairs):
            level[half * pairs + b, span : span + far_at] = mixed[
                :far_at, b * LANES : (b + 1) * LANES
            ]
        farg[seq_id, :, half * width : (half + 1) * width] = mixed[far_at:]
    alike = dot(matrix, id_hot)
    alike = jnp.where((alike > 0.999) & (iota(alike.shape, 1) > 0), 1.0, 0.0).astype(BF16)
    level[blocks, span : span + far_at] = alike[:far_at]
    farg[seq_id, :, 2 * width :] = alike[far_at:]

    def level_start(lv):
        return 0 if lv == 0 else span + plan.level_row[lv]

    for lv in range(near + 1):
        at, n = level_start(lv), span >> lv
        edge[0, :, lv * NR : (lv + 1) * NR] = level[:, at : at + NR]
        edge[1, :, lv * NR : (lv + 1) * NR] = level[:, at + n - NR : at + n]

    pl.semaphore_wait(barrier, greeted)

    def far_copy(k):
        _, device = peer(3, k)
        return remote(
            farg.at[seq_id], farg.at[seq_id], far_send.at[k - 1], far_recv.at[k - 1], device
        )

    def halo_copy(src, dst, send, recv, side):
        step = 2 * side - 1
        return remote(
            src.at[side], dst.at[1 - side], send.at[side], recv.at[1 - side],
            (row_id, seq_id + step),
        )

    def halo_start(src, dst, send, recv):
        @pl.when(seq_id > 0)
        def _():
            halo_copy(src, dst, send, recv, 0).start()

        @pl.when(seq_id < seq - 1)
        def _():
            halo_copy(src, dst, send, recv, 1).start()

    def halo_wait(src, dst, send, recv):
        @pl.when(seq_id > 0)
        def _():
            remote(
                src.at[0], dst.at[0], send.at[0], recv.at[0], (row_id, seq_id - 1)
            ).wait()

        @pl.when(seq_id < seq - 1)
        def _():
            remote(
                src.at[1], dst.at[1], send.at[1], recv.at[1], (row_id, seq_id + 1)
            ).wait()

    halo_start(edge, halo, halo_send, halo_recv)
    for k in range(1, seq):
        far_copy(k).start()

    load_q.wait()
    query = ((dot(first[...], wq[...]) + vec(2)).astype(BF16) * (1.0 / math.sqrt(HEAD_DIM))).astype(
        BF16
    )
    for b in range(pairs):
        qh[b] = query[:, b * LANES : (b + 1) * LANES]

    def slot_pieces(c):
        pieces = []
        for lv in range(near + 1):
            at, n = level_start(lv), span >> lv
            per = plan.chunk >> lv
            s0 = plan.slot[lv]
            if per >= NR:
                low, high = c * per - NR, c * per + per + NR
            else:
                low, high = -NR, n + NR
            if low < 0:
                pieces.append((s0, "low", lv * NR, NR))
                s0, low = s0 + NR, 0
            inner = min(high, n)
            pieces.append((s0, "own", at + low, inner - low))
            s0 += inner - low
            if high > n:
                pieces.append((s0, "high", lv * NR, NR))
        return pieces

    slot_at = iota((1, plan.slots), 1)
    slot_level = jnp.zeros((1, plan.slots), jnp.int32)
    for lv in range(1, top + 1):
        slot_level = slot_level + (slot_at >= plan.slot[lv]).astype(jnp.int32)
    for c in range(plan.chunks):
        origin = start + c * plan.chunk
        j = slot_at
        for lv in range(top + 1):
            if (plan.chunk >> lv) >= NR:
                base = origin // (1 << lv) - NR
            else:
                base = (origin // (NR << lv) - 1) * NR
            here = slot_at - plan.slot[lv] + base
            j = here if lv == 0 else jnp.where(slot_level == lv, here, j)
        position = origin + iota((plan.chunk, plan.slots), 0)
        off_block = (j >> 4) - (position >> (slot_level + 4))
        off_half = (j >> 3) - (position >> (slot_level + 3))
        reach = jnp.where(slot_level == 0, -1, 1)
        within = (jnp.abs(off_block) <= 1) & (jnp.abs(off_half) > reach)
        bias[c] = jnp.where(within, slot_level.astype(F32) * LOG_TWO, MASKED)

    def far_select():
        pieces = []
        for lv in plan.far:
            per_log = (span >> lv).bit_length() - 1
            first_row = plan.level_row[lv] - plan.far_row
            j = (start // (NR << lv) - 1) * NR + iota((3 * NR, seq * NR), 0)
            column = (j >> per_log) * NR + (j & ((1 << per_log) - 1)) + first_row
            pieces.append((column == iota((3 * NR, seq * NR), 1)).astype(F32))
        rest = plan.far_slots - 3 * NR * len(plan.far)
        if rest:
            pieces.append(jnp.zeros((rest, seq * NR), F32))
        return jnp.concatenate(pieces, axis=0).astype(BF16)

    select = far_select()
    spread[...] = averaging(1)

    halo_wait(edge, halo, halo_send, halo_recv)
    for c in range(plan.chunks):
        for s0, kind, at, n in slot_pieces(c):
            if kind == "own":
                slots[c, :, s0 : s0 + n] = level[:, at : at + n]
            else:
                slots[c, :, s0 : s0 + n] = halo[0 if kind == "low" else 1, :, at : at + n]
    for k in range(1, seq):
        far_copy(k).wait()
    far_values = dot(select, farg[...].reshape(seq * NR, 2 * width + LANES)).astype(BF16)
    for c in range(plan.chunks):
        for b in range(blocks + 1):
            slots[c, b, plan.far_slot :] = far_values[:, b * LANES : (b + 1) * LANES]
    for c in range(plan.chunks):
        same = dot_nt(level[blocks, c * plan.chunk : (c + 1) * plan.chunk], slots[c, blocks])
        bias[c] = jnp.where(same > 0.5, bias[c], MASKED)

    lane = iota((1, LANES), 1)
    low_half = (lane < HEAD_DIM).astype(F32).astype(BF16)
    high_half = (lane >= HEAD_DIM).astype(F32).astype(BF16)
    low_lanes = iota((plan.chunk, LANES), 1) < HEAD_DIM

    def two_heads(block):
        return jnp.concatenate([block * low_half, block * high_half], axis=0)

    def merge_heads(both):
        return jnp.where(low_lanes, both[: plan.chunk], both[plan.chunk :])

    def chunk_rows(c):
        return pl.ds(pl.multiple_of(c * plan.chunk, plan.chunk), plan.chunk)

    def pair_lanes(b):
        return pl.ds(pl.multiple_of(b * LANES, LANES), LANES)

    def attend(i, carry):
        c, b = i // pairs, i % pairs
        q2 = two_heads(qh[b, chunk_rows(c)])
        offset = bias[c]
        score = dot_nt(q2, slots[c, b]) + jnp.concatenate([offset, offset], axis=0)
        peak = jnp.max(score, axis=1, keepdims=True)
        raised = jnp.exp(score - peak)
        prob = raised * (1.0 / jnp.sum(raised, axis=1, keepdims=True))
        low = prob.astype(BF16)
        probs[i] = low
        att[chunk_rows(c), pair_lanes(b)] = merge_heads(dot(low, slots[c, pairs + b])).astype(BF16)
        return carry

    lax.fori_loop(0, plan.chunks * pairs, attend, 0)

    received = [recv0, recv1, recv2, recv3]

    def region(part, digits):
        n = plan.parts[0][1]
        base = part * n
        for digit in range(digits):
            n = n // count[digit]
            base = base + index[digit] * n
        return base, n

    def rows_at(base, n):
        return pl.ds(pl.multiple_of(base, NR), n)

    def received_rows(part, n):
        return rows_at(part * n, n)

    def rs_copy(part, digit, k):
        base, n = region(part, digit)
        other, device = peer(digit, k)
        if digit == 3 and not plan.scatter:
            return remote(
                grads.at[rows_at(base, n)],
                received[digit].at[k - 1, received_rows(part, n)],
                rs_send.at[part, digit, k - 1], rs_recv.at[part, digit, k - 1], device,
            )
        n = n // count[digit]
        return remote(
            grads.at[rows_at(base + other * n, n)],
            received[digit].at[k - 1, received_rows(part, n)],
            rs_send.at[part, digit, k - 1], rs_recv.at[part, digit, k - 1], device,
        )

    def rs_start(part, digit):
        for k in range(1, count[digit]):
            rs_copy(part, digit, k).start()

    def rs_finish(part, digit):
        for k in range(1, count[digit]):
            rs_copy(part, digit, k).wait_recv()
        gather_all = digit == 3 and not plan.scatter
        base, n = region(part, digit if gather_all else digit + 1)
        at = part * n
        target = red_ref if digit == 3 else grads
        block = 64 if n % 64 == 0 else NR

        def add(i, carry):
            here = rows_at(base + i * block, block)
            there = pl.ds(pl.multiple_of(at + i * block, NR), block)
            if gather_all:
                acc = jnp.zeros((block, width), F32)
                for s in range(seq):
                    slot = (seq_id - s + seq - 1) % seq
                    theirs = received[digit][jnp.minimum(slot, seq - 2), there].astype(F32)
                    acc = acc + jnp.where(seq_id == s, grads[here].astype(F32), theirs)
            else:
                acc = grads[here].astype(F32)
                for k in range(1, count[digit]):
                    acc = acc + received[digit][k - 1, there].astype(F32)
            target[here] = acc.astype(BF16)
            return carry

        lax.fori_loop(0, n // block, add, 0)

    def ag_copy(part, digit, k):
        base, n = region(part, digit + 1)
        _, device = peer(digit, k)
        return remote(
            red_ref.at[rows_at(base, n)], red_ref.at[rows_at(base, n)],
            ag_send.at[part, digit, k - 1], ag_recv.at[part, digit, k - 1], device,
        )

    def ag_start(part, digit):
        if digit == 3 and not plan.scatter:
            return
        for k in range(1, count[digit]):
            ag_copy(part, digit, k).start()

    def ag_finish(part, digit):
        if digit == 3 and not plan.scatter:
            return
        for k in range(1, count[digit]):
            ag_copy(part, digit, k).wait_recv()

    def part_steps(part):
        steps = [functools.partial(rs_start, part, 0)]
        for digit in range(1, 4):
            steps.append(
                functools.partial(
                    sequence,
                    functools.partial(rs_finish, part, digit - 1),
                    functools.partial(rs_start, part, digit),
                )
            )
        steps.append(
            functools.partial(
                sequence, functools.partial(rs_finish, part, 3), functools.partial(ag_start, part, 3)
            )
        )
        for digit in (2, 1, 0):
            steps.append(
                functools.partial(
                    sequence,
                    functools.partial(ag_finish, part, digit + 1),
                    functools.partial(ag_start, part, digit),
                )
            )
        steps.append(
            functools.partial(
                sequence, functools.partial(ag_finish, part, 0), lambda: put(part).start()
            )
        )
        return steps

    def put(part):
        off, n = plan.parts[part]
        rows = slice(off, off + n)
        return pltpu.make_async_copy(red_ref.at[rows], red_hbm.at[rows], out_sem.at[part])

    all_steps = [part_steps(part) for part in range(len(plan.parts))]

    def step(part, number):
        all_steps[part][number]()

    at_place = {}
    reached_step = [0] * (len(plan.parts) + 1)
    for place, parts_here in ORDER.items():
        at_place[place] = []
        for part in parts_here:
            reached_step[part] += 1
            at_place[place].append((part, reached_step[part]))

    def advance(place):
        for part, number in at_place.get(place, ()):
            if part < 0:
                vec_finish(number - 1)
                if number < 4:
                    vec_start(number)
            else:
                step(part, number)

    load_o.wait()
    load_up.wait()
    res = tok[...].astype(F32) + dot(att[...], wo[...]) + vec(4)
    mid[...] = res
    center = res - mean(res)
    rstd = lax.rsqrt(mean(center * center) + EPSILON)
    normed = center * rstd
    n2[...] = normed
    stats[1] = jnp.broadcast_to(rstd, (span, LANES))
    second[...] = (normed * vec(5) + vec(6)).astype(BF16)
    racc[...] = jnp.zeros_like(racc)
    dsec[...] = jnp.zeros_like(dsec)
    for copy in load_1:
        copy.wait()
    load_2.wait()
    curve = math.sqrt(2.0 / math.pi)

    def feed(t, carry):
        w2_rows = pl.ds(pl.multiple_of(t * tile, tile), tile)
        pre = dot(second[...], w1[t]) + inb[pl.ds(t, 1), :]
        square = pre * pre
        bend = jnp.tanh(curve * (pre + 0.044715 * (square * pre)))
        half = 0.5 * (1.0 + bend)
        act = (pre * half).astype(BF16)
        slope = half + 0.5 * pre * (1.0 - bend * bend) * (curve * (1.0 + 3 * 0.044715 * square))
        upstream = up[...]
        racc[...] += dot(act, w2[w2_rows])
        d_pre = (dot_nt(upstream, w2[w2_rows]) * slope).astype(BF16)
        base = 2 * t * tile
        grads[rows_at(base, tile)] = dot_tn(act, upstream).astype(BF16)
        grads[rows_at(base + tile, tile)] = dot_tn(second[...], d_pre).astype(BF16)
        rs_start(2 * t, 0)
        rs_start(2 * t + 1, 0)
        vstage[0, pl.ds(V_INNB + t, 1), :] = total(d_pre.astype(F32))
        dsec[...] += dot_nt(d_pre, w1[t])

        for when in range(tiles):
            if f"f{when}" in ORDER:
                pl.when(t == when)(functools.partial(advance, f"f{when}"))

        return carry

    lax.fori_loop(0, tiles, feed, 0)
    out_ref[0] = (mid[...] + racc[...] + vec(7)).astype(BF16)

    up_f = up[...].astype(F32)
    vstage[0, V_OUTB : V_OUTB + 1] = total(up_f)
    d_second, normed = dsec[...], n2[...]
    scaled = d_second * vec(5)
    vstage[0, V_MIDG : V_MIDG + 1] = total(d_second * normed)
    vstage[0, V_MIDS : V_MIDS + 1] = total(d_second)
    d_mid = up_f + (scaled - mean(scaled) - normed * mean(scaled * normed)) * stats[1][:, :1]
    mid[...] = d_mid
    d_branch = d_mid.astype(BF16)
    vstage[0, V_OB : V_OB + 1] = total(d_branch.astype(F32))
    grads[2 * hidden : 2 * hidden + width] = dot_tn(att[...], d_branch).astype(BF16)
    rs_start(2 * tiles, 0)
    advance("ln2")
    d_att = dot_nt(d_branch, wo[...]).astype(BF16)
    for b in range(pairs):
        dah[b] = d_att[:, b * LANES : (b + 1) * LANES]

    def attend_back(i, carry):
        c, b = i // pairs, i % pairs
        q2 = two_heads(qh[b, chunk_rows(c)])
        g2 = two_heads(dah[b, chunk_rows(c)])
        low = probs[i]
        prob = low.astype(F32)
        d_prob = dot_nt(g2, slots[c, pairs + b])
        weighted = prob * d_prob
        d_score = (weighted - prob * jnp.sum(weighted, axis=1, keepdims=True)).astype(BF16)
        d_query = merge_heads(dot(d_score, slots[c, b])) * (1.0 / math.sqrt(HEAD_DIM))
        dq[chunk_rows(c), pair_lanes(b)] = d_query.astype(BF16)
        dslots[c, b] = dot_tn(d_score, q2)
        dslots[c, pairs + b] = dot_tn(low, g2)
        for when in range(plan.chunks * pairs):
            if f"b{when}" in ORDER:
                pl.when(i == when)(functools.partial(advance, f"b{when}"))

        return carry

    lax.fori_loop(0, plan.chunks * pairs, attend_back, 0)

    def fold(b, carry):
        for c in range(plan.chunks):
            for s0, kind, at, n in slot_pieces(c):
                piece = dslots[c, b, s0 : s0 + n]
                if kind == "own":
                    parts_done = own_done[c].get((s0, at))
                    seen = parts_done if parts_done is not None else 0
                    if seen:
                        own[b, at : at + seen] += piece[:seen]
                    if seen < n:
                        own[b, at + seen : at + n] = piece[seen:]
                elif own_done[c].get((s0, kind)):
                    side = 0 if kind == "low" else 1
                    hsend[side, b, at : at + n] = (
                        hsend[side, b, at : at + n].astype(F32) + piece
                    ).astype(BF16)
                else:
                    side = 0 if kind == "low" else 1
                    hsend[side, b, at : at + n] = piece.astype(BF16)
        far = dslots[0, b, plan.far_slot :]
        for c in range(1, plan.chunks):
            far = far + dslots[c, b, plan.far_slot :]
        back = dot_tn(select, far.astype(BF16))
        for s in range(seq):
            fsend[s, b] = back[s * NR : (s + 1) * NR].astype(BF16)
        return carry

    own_done = []
    reached, halo_seen = {}, set()
    for c in range(plan.chunks):
        done = {}
        for s0, kind, at, n in slot_pieces(c):
            if kind == "own":
                lv = max(v for v in range(near + 1) if level_start(v) <= at)
                limit = reached.get(lv, level_start(lv))
                done[(s0, at)] = max(0, min(limit, at + n) - at)
                reached[lv] = max(limit, at + n)
            else:
                done[(s0, kind)] = (kind, at) in halo_seen
                halo_seen.add((kind, at))
        own_done.append(done)

    lax.fori_loop(0, blocks, fold, 0)

    def far_back(k):
        other, device = peer(3, k)
        return remote(
            fsend.at[other], frecv.at[k - 1], fback_send.at[k - 1], fback_recv.at[k - 1], device
        )

    halo_start(hsend, hrecv, back_send, back_recv)
    for k in range(1, seq):
        far_back(k).start()

    advance("fold")

    d_query = dq[...]
    vstage[0, V_QB : V_QB + 1] = total(d_query.astype(F32))
    off_c = 2 * hidden + width
    grads[off_c : off_c + width] = dot_tn(first[...], d_query).astype(BF16)
    d_first = dot_nt(d_query, wq[...])
    racc[...] = d_first
    rs_start(2 * tiles + 1, 0)
    advance("q")

    halo_wait(hsend, hrecv, back_send, back_recv)
    for k in range(1, seq):
        far_back(k).wait()
    for lv in range(near + 1):
        at, n = level_start(lv), span >> lv
        lo, hi = lv * NR, (lv + 1) * NR
        own[:, at : at + NR] += hrecv[0, :, lo:hi].astype(F32)
        own[:, at + n - NR : at + n] += hrecv[1, :, lo:hi].astype(F32)
    far_sum = fsend[seq_id].astype(F32)
    for k in range(1, seq):
        far_sum = far_sum + frecv[k - 1].astype(F32)
    for b in range(blocks):
        cols = slice(b * LANES, (b + 1) * LANES)
        coarse[:far_at, cols] = own[b, span : span + far_at].astype(BF16)
        coarse[far_at:, cols] = far_sum[b].astype(BF16)
    for half in range(2):
        passed = dot(spread[...], coarse[:, half * width : (half + 1) * width])
        for b in range(pairs):
            cols = slice((half * pairs + b) * LANES, (half * pairs + b + 1) * LANES)
            dkv[:, cols] = (
                own[half * pairs + b, :span] + passed[:, b * LANES : (b + 1) * LANES]
            ).astype(BF16)
    d_keys, d_values = dkv[:, :width], dkv[:, width:]
    vstage[0, V_VB : V_VB + 1] = total(d_values.astype(F32))
    grads[off_c + width : off_c + 2 * width] = dot_tn(first[...], d_keys).astype(BF16)
    grads[off_c + 2 * width : off_c + 3 * width] = dot_tn(first[...], d_values).astype(BF16)
    rs_start(2 * tiles + 2, 0)
    rs_start(2 * tiles + 3, 0)
    advance("dkv")
    d_first = racc[...] + dot_nt(d_keys, wk[...]) + dot_nt(d_values, wv[...])
    normed = n1[...]
    scaled = d_first * vec(0)
    vstage[0, V_PREG : V_PREG + 1] = total(d_first * normed)
    vstage[0, V_PRES : V_PRES + 1] = total(d_first)
    d_in = mid[...] + (scaled - mean(scaled) - normed * mean(scaled * normed)) * stats[0][:, :1]
    gin_ref[0] = d_in.astype(BF16)

    vec_received = [vrecv0, vrecv1, vrecv2, vrecv3]

    def vec_copy(digit, k):
        _, device = peer(digit, k)
        return remote(
            vstage.at[digit], vec_received[digit].at[index[digit]],
            vec_send.at[digit, k - 1], vec_recv.at[digit, k - 1], device,
        )

    def vec_start(digit):
        for k in range(1, count[digit]):
            vec_copy(digit, k).start()

    def vec_finish(digit):
        for k in range(1, count[digit]):
            vec_copy(digit, k).wait_recv()
        acc = jnp.zeros((VEC_ROWS, width), F32)
        for s in range(count[digit]):
            acc = acc + jnp.where(index[digit] == s, vstage[digit], vec_received[digit][s])
        if digit == 3:
            vout_ref[...] = acc
        else:
            vstage[digit + 1] = acc

    vec_start(0)
    advance("ln1")

    for part in range(len(plan.parts)):
        for digit in range(4):
            for k in range(1, count[digit]):
                rs_copy(part, digit, k).wait_send()
                if digit < 3 or plan.scatter:
                    ag_copy(part, digit, k).wait_send()
        put(part).wait()
    for digit in range(4):
        for k in range(1, count[digit]):
            vec_copy(digit, k).wait_send()


def unpack_kernel(
    width, tiles, red_hbm, vec_ref, out_hbm, gin_hbm,
    query_ref, key_ref, value_ref, output_ref, inner_ref, outer_ref,
    preg_ref, pres_ref, qb_ref, vb_ref, ob_ref, midg_ref, mids_ref, outb_ref, innb_ref,
    out_ref, gin_ref, low, wide, through, in_sem, out_sem, through_in, through_out,
):
    targets = []
    for t in range(tiles):
        rows = slice(t * width, (t + 1) * width)
        targets.append(outer_ref.at[rows])
        targets.append(inner_ref.at[:, rows])
    targets += [output_ref, query_ref, key_ref, value_ref]

    def fetch(i):
        return pltpu.make_async_copy(
            red_hbm.at[i * width : (i + 1) * width], low.at[i % 4], in_sem.at[i % 4]
        )

    def put(i):
        return pltpu.make_async_copy(wide.at[i % 4], targets[i], out_sem.at[i % 4])

    def take(i):
        return pltpu.make_async_copy((out_hbm, gin_hbm)[i], through.at[i], through_in.at[i])

    def give(i):
        return pltpu.make_async_copy(through.at[i], (out_ref, gin_ref)[i], through_out.at[i])

    n = len(targets)
    for i in range(3):
        fetch(i).start()
    for i in range(2):
        take(i).start()
    for row, ref in (
        (V_PREG, preg_ref), (V_PRES, pres_ref), (V_QB, qb_ref), (V_VB, vb_ref), (V_OB, ob_ref),
        (V_MIDG, midg_ref), (V_MIDS, mids_ref), (V_OUTB, outb_ref),
    ):
        ref[...] = vec_ref[row]
    for t in range(tiles):
        innb_ref[t * width : (t + 1) * width] = vec_ref[V_INNB + t]
    for i in range(n):
        fetch(i).wait()
        if i >= 4:
            put(i - 4).wait()
        wide[i % 4] = low[i % 4].astype(F32)
        put(i).start()
        if i + 3 < n:
            fetch(i + 3).start()
        if 2 <= i < 4:
            take(i - 2).wait()
            give(i - 2).start()
    for i in range(n - 4, n):
        put(i).wait()
    for i in range(2):
        give(i).wait()


def shards(
    rows, seq,
    tokens, segment_ids, prenorm_gain, prenorm_shift, query_proj, query_bias, key_proj, value_proj,
    value_bias, output_proj, output_bias, midnorm_gain, midnorm_shift, inner_proj, inner_bias,
    outer_proj, outer_bias, upstream,
):
    _, span, width = tokens.shape
    hidden = inner_proj.shape[1]
    plan = Plan(rows, seq, span, width, hidden)
    tiles = hidden // width
    pairs = width // LANES
    count = plan.counts
    most = max(count) - 1
    vmem = pl.BlockSpec(memory_space=pltpu.VMEM)
    hbm = pl.BlockSpec(memory_space=pl.ANY)
    grad_rows = plan.grad_rows
    rest = [grad_rows // 2, grad_rows // 4, grad_rows // 4 // count[2]]
    last = rest[2] // seq if plan.scatter else rest[2]
    dma = pltpu.SemaphoreType.DMA
    items = plan.chunks * pairs
    n_parts = len(plan.parts)
    scratch = [
        pltpu.VMEM((span, width), BF16),
        pltpu.VMEM((span, width), BF16),
        pltpu.VMEM((width, width), BF16),
        pltpu.VMEM((width, width), BF16),
        pltpu.VMEM((width, width), BF16),
        pltpu.VMEM((width, width), BF16),
        pltpu.VMEM((tiles, width, width), BF16),
        pltpu.VMEM((hidden, width), BF16),
        pltpu.VMEM((span, width), F32),
        pltpu.VMEM((span, width), F32),
        pltpu.VMEM((span, width), F32),
        pltpu.VMEM((span, width), F32),
        pltpu.VMEM((span, width), F32),
        pltpu.VMEM((span, width), BF16),
        pltpu.VMEM((span, width), BF16),
        pltpu.VMEM((pairs, span, LANES), BF16),
        pltpu.VMEM((span, width), BF16),
        pltpu.VMEM((pairs, span, LANES), BF16),
        pltpu.VMEM((span, width), BF16),
        pltpu.VMEM((2 * pairs + 1, span + plan.far_row, LANES), BF16),
        pltpu.VMEM((2, 2 * pairs + 1, plan.edge, LANES), BF16),
        pltpu.VMEM((2, 2 * pairs + 1, plan.edge, LANES), BF16),
        pltpu.VMEM((seq, NR, 2 * width + LANES), BF16),
        pltpu.VMEM((plan.chunks, 2 * pairs + 1, plan.slots, LANES), BF16),
        pltpu.VMEM((plan.chunks, plan.chunk, plan.slots), F32),
        pltpu.VMEM((items, 2 * plan.chunk, plan.slots), BF16),
        pltpu.VMEM((plan.chunks, 2 * pairs, plan.slots, LANES), F32),
        pltpu.VMEM((2 * pairs, span + plan.far_row, LANES), F32),
        pltpu.VMEM((2, 2 * pairs, plan.edge, LANES), BF16),
        pltpu.VMEM((2, 2 * pairs, plan.edge, LANES), BF16),
        pltpu.VMEM((seq, 2 * pairs, NR, LANES), BF16),
        pltpu.VMEM((seq - 1, 2 * pairs, NR, LANES), BF16),
        pltpu.VMEM((plan.coarse_rows, 2 * width), BF16),
        pltpu.VMEM((span, plan.coarse_rows), BF16),
        pltpu.VMEM((span, 2 * width), BF16),
        pltpu.VMEM((grad_rows, width), BF16),
        pltpu.VMEM((count[0] - 1, rest[0], width), BF16),
        pltpu.VMEM((count[1] - 1, rest[1], width), BF16),
        pltpu.VMEM((count[2] - 1, rest[2], width), BF16),
        pltpu.VMEM((count[3] - 1, last, width), BF16),
        pltpu.VMEM((4, VEC_ROWS, width), F32),
        pltpu.VMEM((count[0], VEC_ROWS, width), F32),
        pltpu.VMEM((count[1], VEC_ROWS, width), F32),
        pltpu.VMEM((count[2], VEC_ROWS, width), F32),
        pltpu.VMEM((count[3], VEC_ROWS, width), F32),
        pltpu.VMEM((2, span, LANES), F32),
        pltpu.VMEM((tiles, width), F32),
        pltpu.VMEM((grad_rows, width), BF16),
        dma((7 + tiles,)),
        dma((n_parts,)),
        dma((2,)), dma((2,)),
        dma((seq - 1,)), dma((seq - 1,)),
        dma((2,)), dma((2,)),
        dma((seq - 1,)), dma((seq - 1,)),
        dma((n_parts, 4, most)), dma((n_parts, 4, most)),
        dma((n_parts, 4, most)), dma((n_parts, 4, most)),
        dma((4, most)), dma((4, most)),
    ]
    layer_output, input_grad, reduced, vecs = pl.pallas_call(
        functools.partial(layer_kernel, plan),
        out_shape=(
            jax.ShapeDtypeStruct(tokens.shape, BF16),
            jax.ShapeDtypeStruct(tokens.shape, BF16),
            jax.ShapeDtypeStruct((grad_rows, width), BF16),
            jax.ShapeDtypeStruct((VEC_ROWS, width), F32),
        ),
        in_specs=[
            hbm, vmem, vmem, vmem, hbm, vmem, hbm, hbm, vmem, hbm, vmem, vmem, vmem, hbm, vmem, hbm,
            vmem, hbm,
        ],
        out_specs=(vmem, vmem, hbm, vmem),
        scratch_shapes=scratch,
        compiler_params=pltpu.CompilerParams(
            collective_id=0, has_side_effects=True, vmem_limit_bytes=60 * 1024 * 1024
        ),
        name="layer",
    )(
        tokens, segment_ids, prenorm_gain, prenorm_shift, query_proj, query_bias, key_proj,
        value_proj, value_bias, output_proj, output_bias, midnorm_gain, midnorm_shift, inner_proj,
        inner_bias, outer_proj, outer_bias, upstream,
    )
    matrix = jax.ShapeDtypeStruct((width, width), F32)
    vector = jax.ShapeDtypeStruct((width,), F32)
    grads = pl.pallas_call(
        functools.partial(unpack_kernel, width, tiles),
        out_shape=(
            matrix, matrix, matrix, matrix,
            jax.ShapeDtypeStruct((width, hidden), F32),
            jax.ShapeDtypeStruct((hidden, width), F32),
            vector, vector, vector, vector, vector, vector, vector, vector,
            jax.ShapeDtypeStruct((hidden,), F32),
            jax.ShapeDtypeStruct(tokens.shape, BF16),
            jax.ShapeDtypeStruct(tokens.shape, BF16),
        ),
        in_specs=[hbm, vmem, hbm, hbm],
        out_specs=(hbm,) * 6 + (vmem,) * 9 + (hbm,) * 2,
        scratch_shapes=[
            pltpu.VMEM((4, width, width), BF16),
            pltpu.VMEM((4, width, width), F32),
            pltpu.VMEM((2, 1, span, width), BF16),
            dma((4,)), dma((4,)), dma((2,)), dma((2,)),
        ],
        name="unpack",
    )(reduced, vecs, layer_output, input_grad)
    (query_g, key_g, value_g, output_g, inner_g, outer_g,
     preg, pres, qb, vb, ob, midg, mids, outb, innb, layer_output, input_grad) = grads
    return (
        layer_output, input_grad, preg, pres, query_g, qb, key_g, value_g, vb, output_g, ob,
        midg, mids, inner_g, innb, outer_g, outb,
    )


def solution(mesh):
    split, ids, whole = P("rows", "seq", None), P("rows", "seq"), P()
    in_specs = (split, ids) + (whole,) * 15 + (split,)
    out_specs = (split, split) + (whole,) * 15
    return jax.shard_map(
        functools.partial(shards, mesh.shape["rows"], mesh.shape["seq"]),
        mesh=mesh, in_specs=in_specs, out_specs=out_specs, check_vma=False,
    )
```

```python
import functools
import math

import jax
import jax.numpy as jnp
from jax import lax
from jax.experimental import pallas as pl
from jax.experimental.pallas import tpu as pltpu
from jax.sharding import PartitionSpec as P

HEADS = 8
HEAD_DIM = 64
NR = 16
LANES = 128
LOG_TWO = math.log(2.0)
EPSILON = 1e-05
MASKED = -1e30
F32 = jnp.float32
BF16 = jnp.bfloat16
MESH = pl.DeviceIdType.MESH

VEC_ROWS = 16
V_PREG, V_PRES, V_QB, V_VB, V_OB, V_MIDG, V_MIDS, V_OUTB, V_INNB = 0, 1, 2, 3, 4, 5, 6, 7, 8


def dot(a, b):
    return jnp.dot(a, b, preferred_element_type=F32)


def dot_nt(a, b):
    return lax.dot_general(a, b, (((1,), (1,)), ((), ())), preferred_element_type=F32)


def dot_tn(a, b):
    return lax.dot_general(a, b, (((0,), (0,)), ((), ())), preferred_element_type=F32)


def iota(shape, dim):
    return lax.broadcasted_iota(jnp.int32, shape, dim)


def mean(x):
    return jnp.mean(x, axis=-1, keepdims=True)


def total(x):
    return jnp.sum(x, axis=0, keepdims=True)


ORDER = {
    "f2": [0, 1],
    "f3": [2, 3],
    "ln2": [4],
    "b0": [5],
    "b1": [0, 6],
    "b2": [1, 7, 8],
    "b4": [2],
    "b6": [0],
    "b7": [3, 1],
    "fold": [2],
    "q": [4, 0, 3, 1, 5, 9, 4, 6, 5, 7],
    "ln1": [
        2, 6, 8, 0, 7, 10, 9, 11, 3, 8, 1, 0, 4, -1, 9, 10, 5, 1, 2, 11, 6, 10, 0, -1,
        7, 2, 3, 0, 11, 1, 8, 4, 1, 2, 3, 9, -1, 4, 5, 2, 6, 3, 10, 5, 3, 7, 4, 6,
        11, -1, 8, 4, 5, 7, 9, 6, 10, 8, 5, 11, 6, 9, 7, 10, 7, 11, 8, 9, 8, 10, 9, 11,
        10, 11,
    ],
}


class Plan:
    def __init__(self, rows, seq, span, width, hidden):
        self.rows, self.seq, self.span, self.width, self.hidden = rows, seq, span, width, hidden
        self.near = (span // NR).bit_length() - 1
        self.length = span * seq
        self.top = (self.length // NR).bit_length() - 2
        self.chunk = 128
        self.chunks = span // self.chunk
        self.far = list(range(self.near + 1, self.top + 1))
        self.level_row = [0]
        at = 0
        for level in range(1, self.near + 1):
            self.level_row.append(at)
            at += span >> level
        self.far_row = at
        for level in self.far:
            self.level_row.append(at)
            at += span >> level
        self.coarse_rows = self.far_row + NR
        self.slot, self.slot_len = [], []
        at = 0
        for level in range(self.top + 1):
            n = 2 * NR + max(self.chunk >> level, NR)
            self.slot.append(at)
            self.slot_len.append(n)
            at += n
        self.used = at
        self.slots = -(-at // LANES) * LANES
        self.far_slot = self.slot[self.near + 1]
        self.far_slots = self.slots - self.far_slot
        self.edge = NR * (self.near + 1)
        self.grad_rows = 4 * width + 2 * hidden
        self.parts = [(p * width, width) for p in range(self.grad_rows // width)]
        self.counts = [2, 2, rows // 4, seq]
        self.swap = rows // 4 == 2
        self.scatter = (width // rows) % (NR * seq) == 0


def sequence(*steps):
    for step in steps:
        step()


def layer_kernel(
    plan,
    tok_hbm, ids_ref, preg_ref, pres_ref, wq_hbm, qb_ref, wk_hbm, wv_hbm, vb_ref, wo_hbm, ob_ref,
    midg_ref, mids_ref, w1_hbm, inb_ref, w2_hbm, outb_ref, up_hbm,
    out_ref, gin_ref, red_ref, vout_ref,
    tok, up, wq, wk, wv, wo, w1, w2, n1, n2, mid, racc, dsec, first, second, qh, att, dah, dq,
    level, edge, halo, farg, slots, bias, probs, dslots, own, hsend, hrecv, fsend, frecv,
    coarse, spread, dkv, grads, recv0, recv1, recv2, recv3, vstage, vrecv0, vrecv1, vrecv2, vrecv3, stats,
    inb,
    in_sem, halo_send, halo_recv, far_send, far_recv, back_send, back_recv, fback_send, fback_recv,
    rs_send, rs_recv, ag_send, ag_recv, vec_send, vec_recv,
):
    span, width, hidden = plan.span, plan.width, plan.hidden
    seq, near, top = plan.seq, plan.near, plan.top
    tile = hidden // w1.shape[0]
    tiles = w1.shape[0]
    pairs = width // LANES
    blocks = 2 * pairs
    row_id, seq_id = lax.axis_index("rows"), lax.axis_index("seq")
    start = seq_id * span

    core = row_id % 2
    if plan.swap:
        stride_a, stride_b = 2 + 2 * core, 4 - 2 * core
    else:
        stride_a, stride_b = 2, 4
    count = plan.counts
    index = [
        core,
        (row_id // stride_a) % count[1],
        (row_id // stride_b) % count[2],
        seq_id,
    ]

    def peer(digit, k):
        other = (index[digit] + k) % count[digit]
        if digit == 3:
            return other, (row_id, other)
        stride = [1, stride_a, stride_b][digit]
        return other, (row_id + (other - index[digit]) * stride, seq_id)

    def remote(src, dst, send, recv, device):
        return pltpu.make_async_remote_copy(
            src_ref=src, dst_ref=dst, send_sem=send, recv_sem=recv,
            device_id=device, device_id_type=MESH,
        )

    loads = []

    def load(src, dst):
        copy = pltpu.make_async_copy(src, dst, in_sem.at[len(loads)])
        copy.start()
        loads.append(copy)
        return copy

    load_tok = load(tok_hbm.at[0], tok)
    load_q = load(wq_hbm, wq)
    load_k = load(wk_hbm, wk)
    load_v = load(wv_hbm, wv)
    load_up = load(up_hbm.at[0], up)
    load_o = load(wo_hbm, wo)
    load_1 = [load(w1_hbm.at[:, t * tile : (t + 1) * tile], w1.at[t]) for t in range(tiles)]
    load_2 = load(w2_hbm, w2)

    halo[...] = jnp.zeros_like(halo)
    hrecv[...] = jnp.zeros_like(hrecv)
    vstage[0] = jnp.zeros((VEC_ROWS, width), F32)
    for t in range(tiles):
        inb[t : t + 1, :] = inb_ref[t * tile : (t + 1) * tile].reshape(1, tile)

    barrier = pltpu.get_barrier_semaphore()
    greeted = 0
    for digit in range(4):
        for k in range(1, count[digit]):
            _, device = peer(digit, k)
            pl.semaphore_signal(barrier, inc=1, device_id=device, device_id_type=MESH)
            greeted += 1

    vectors = (preg_ref, pres_ref, qb_ref, vb_ref, ob_ref, midg_ref, mids_ref, outb_ref)

    def vec(row):
        return vectors[row][...].reshape(1, width)

    load_tok.wait()
    x = tok[...].astype(F32)
    center = x - mean(x)
    rstd = lax.rsqrt(mean(center * center) + EPSILON)
    normed = center * rstd
    n1[...] = normed
    stats[0] = jnp.broadcast_to(rstd, (span, LANES))
    first[...] = (normed * vec(0) + vec(1)).astype(BF16)
    load_k.wait()
    keys = dot(first[...], wk[...]).astype(BF16)
    load_v.wait()
    values = (dot(first[...], wv[...]) + vec(3)).astype(BF16)
    for b in range(pairs):
        level[b, :span] = keys[:, b * LANES : (b + 1) * LANES]
        level[pairs + b, :span] = values[:, b * LANES : (b + 1) * LANES]

    def averaging(rows_dim):
        shape = (plan.coarse_rows, span) if rows_dim == 0 else (span, plan.coarse_rows)
        r, p = iota(shape, rows_dim), iota(shape, 1 - rows_dim)
        matrix = jnp.zeros(shape, F32)
        for lv in range(1, top + 1):
            at = plan.level_row[lv]
            hit = (r - at == (p >> lv)) & (r >= at) & (r < at + (span >> lv))
            matrix = jnp.where(hit, 0.5**lv, matrix)
        return matrix.astype(BF16)

    matrix = averaging(0)
    far_at = plan.far_row
    feature = (iota((LANES, span), 0) == ids_ref[...]).astype(F32).astype(BF16)
    unit = (iota((span, span), 0) == iota((span, span), 1)).astype(F32).astype(BF16)
    id_hot = dot_nt(unit, feature).astype(BF16)
    level[blocks, :span] = id_hot
    for half, kv in enumerate((keys, values)):
        mixed = dot(matrix, kv).astype(BF16)
        for b in range(pairs):
            level[half * pairs + b, span : span + far_at] = mixed[
                :far_at, b * LANES : (b + 1) * LANES
            ]
        farg[seq_id, :, half * width : (half + 1) * width] = mixed[far_at:]
    alike = dot(matrix, id_hot)
    alike = jnp.where((alike > 0.999) & (iota(alike.shape, 1) > 0), 1.0, 0.0).astype(BF16)
    level[blocks, span : span + far_at] = alike[:far_at]
    farg[seq_id, :, 2 * width :] = alike[far_at:]

    def level_start(lv):
        return 0 if lv == 0 else span + plan.level_row[lv]

    for lv in range(near + 1):
        at, n = level_start(lv), span >> lv
        edge[0, :, lv * NR : (lv + 1) * NR] = level[:, at : at + NR]
        edge[1, :, lv * NR : (lv + 1) * NR] = level[:, at + n - NR : at + n]

    pl.semaphore_wait(barrier, greeted)

    def far_copy(k):
        _, device = peer(3, k)
        return remote(
            farg.at[seq_id], farg.at[seq_id], far_send.at[k - 1], far_recv.at[k - 1], device
        )

    def halo_copy(src, dst, send, recv, side):
        step = 2 * side - 1
        return remote(
            src.at[side], dst.at[1 - side], send.at[side], recv.at[1 - side],
            (row_id, seq_id + step),
        )

    def halo_start(src, dst, send, recv):
        @pl.when(seq_id > 0)
        def _():
            halo_copy(src, dst, send, recv, 0).start()

        @pl.when(seq_id < seq - 1)
        def _():
            halo_copy(src, dst, send, recv, 1).start()

    def halo_wait(src, dst, send, recv):
        @pl.when(seq_id > 0)
        def _():
            remote(
                src.at[0], dst.at[0], send.at[0], recv.at[0], (row_id, seq_id - 1)
            ).wait()

        @pl.when(seq_id < seq - 1)
        def _():
            remote(
                src.at[1], dst.at[1], send.at[1], recv.at[1], (row_id, seq_id + 1)
            ).wait()

    halo_start(edge, halo, halo_send, halo_recv)
    for k in range(1, seq):
        far_copy(k).start()

    load_q.wait()
    query = ((dot(first[...], wq[...]) + vec(2)).astype(BF16) * (1.0 / math.sqrt(HEAD_DIM))).astype(
        BF16
    )
    for b in range(pairs):
        qh[b] = query[:, b * LANES : (b + 1) * LANES]

    def slot_pieces(c):
        pieces = []
        for lv in range(near + 1):
            at, n = level_start(lv), span >> lv
            per = plan.chunk >> lv
            s0 = plan.slot[lv]
            if per >= NR:
                low, high = c * per - NR, c * per + per + NR
            else:
                low, high = -NR, n + NR
            if low < 0:
                pieces.append((s0, "low", lv * NR, NR))
                s0, low = s0 + NR, 0
            inner = min(high, n)
            pieces.append((s0, "own", at + low, inner - low))
            s0 += inner - low
            if high > n:
                pieces.append((s0, "high", lv * NR, NR))
        return pieces

    slot_at = iota((1, plan.slots), 1)
    slot_level = jnp.zeros((1, plan.slots), jnp.int32)
    for lv in range(1, top + 1):
        slot_level = slot_level + (slot_at >= plan.slot[lv]).astype(jnp.int32)
    for c in range(plan.chunks):
        origin = start + c * plan.chunk
        j = slot_at
        for lv in range(top + 1):
            if (plan.chunk >> lv) >= NR:
                base = origin // (1 << lv) - NR
            else:
                base = (origin // (NR << lv) - 1) * NR
            here = slot_at - plan.slot[lv] + base
            j = here if lv == 0 else jnp.where(slot_level == lv, here, j)
        position = origin + iota((plan.chunk, plan.slots), 0)
        off_block = (j >> 4) - (position >> (slot_level + 4))
        off_half = (j >> 3) - (position >> (slot_level + 3))
        reach = jnp.where(slot_level == 0, -1, 1)
        within = (jnp.abs(off_block) <= 1) & (jnp.abs(off_half) > reach)
        bias[c] = jnp.where(within, slot_level.astype(F32) * LOG_TWO, MASKED)

    def far_select():
        pieces = []
        for lv in plan.far:
            per_log = (span >> lv).bit_length() - 1
            first_row = plan.level_row[lv] - plan.far_row
            j = (start // (NR << lv) - 1) * NR + iota((3 * NR, seq * NR), 0)
            column = (j >> per_log) * NR + (j & ((1 << per_log) - 1)) + first_row
            pieces.append((column == iota((3 * NR, seq * NR), 1)).astype(F32))
        rest = plan.far_slots - 3 * NR * len(plan.far)
        if rest:
            pieces.append(jnp.zeros((rest, seq * NR), F32))
        return jnp.concatenate(pieces, axis=0).astype(BF16)

    select = far_select()
    spread[...] = averaging(1)

    halo_wait(edge, halo, halo_send, halo_recv)
    for c in range(plan.chunks):
        for s0, kind, at, n in slot_pieces(c):
            if kind == "own":
                slots[c, :, s0 : s0 + n] = level[:, at : at + n]
            else:
                slots[c, :, s0 : s0 + n] = halo[0 if kind == "low" else 1, :, at : at + n]
    for k in range(1, seq):
        far_copy(k).wait()
    far_values = dot(select, farg[...].reshape(seq * NR, 2 * width + LANES)).astype(BF16)
    for c in range(plan.chunks):
        for b in range(blocks + 1):
            slots[c, b, plan.far_slot :] = far_values[:, b * LANES : (b + 1) * LANES]
    for c in range(plan.chunks):
        same = dot_nt(level[blocks, c * plan.chunk : (c + 1) * plan.chunk], slots[c, blocks])
        bias[c] = jnp.where(same > 0.5, bias[c], MASKED)

    lane = iota((1, LANES), 1)
    low_half = (lane < HEAD_DIM).astype(F32).astype(BF16)
    high_half = (lane >= HEAD_DIM).astype(F32).astype(BF16)
    low_lanes = iota((plan.chunk, LANES), 1) < HEAD_DIM

    def two_heads(block):
        return jnp.concatenate([block * low_half, block * high_half], axis=0)

    def merge_heads(both):
        return jnp.where(low_lanes, both[: plan.chunk], both[plan.chunk :])

    def chunk_rows(c):
        return pl.ds(pl.multiple_of(c * plan.chunk, plan.chunk), plan.chunk)

    def pair_lanes(b):
        return pl.ds(pl.multiple_of(b * LANES, LANES), LANES)

    def attend(i, carry):
        c, b = i // pairs, i % pairs
        q2 = two_heads(qh[b, chunk_rows(c)])
        offset = bias[c]
        score = dot_nt(q2, slots[c, b]) + jnp.concatenate([offset, offset], axis=0)
        peak = jnp.max(score, axis=1, keepdims=True)
        raised = jnp.exp(score - peak)
        prob = raised * (1.0 / jnp.sum(raised, axis=1, keepdims=True))
        low = prob.astype(BF16)
        probs[i] = low
        att[chunk_rows(c), pair_lanes(b)] = merge_heads(dot(low, slots[c, pairs + b])).astype(BF16)
        return carry

    lax.fori_loop(0, plan.chunks * pairs, attend, 0)

    received = [recv0, recv1, recv2, recv3]

    def region(part, digits):
        n = plan.parts[0][1]
        base = part * n
        for digit in range(digits):
            n = n // count[digit]
            base = base + index[digit] * n
        return base, n

    def rows_at(base, n):
        return pl.ds(pl.multiple_of(base, NR), n)

    def received_rows(part, n):
        return rows_at(part * n, n)

    def rs_copy(part, digit, k):
        base, n = region(part, digit)
        other, device = peer(digit, k)
        if digit == 3 and not plan.scatter:
            return remote(
                grads.at[rows_at(base, n)],
                received[digit].at[k - 1, received_rows(part, n)],
                rs_send.at[part, digit, k - 1], rs_recv.at[part, digit, k - 1], device,
            )
        n = n // count[digit]
        return remote(
            grads.at[rows_at(base + other * n, n)],
            received[digit].at[k - 1, received_rows(part, n)],
            rs_send.at[part, digit, k - 1], rs_recv.at[part, digit, k - 1], device,
        )

    def rs_start(part, digit):
        for k in range(1, count[digit]):
            rs_copy(part, digit, k).start()

    def rs_finish(part, digit):
        for k in range(1, count[digit]):
            rs_copy(part, digit, k).wait_recv()
        gather_all = digit == 3 and not plan.scatter
        base, n = region(part, digit if gather_all else digit + 1)
        at = part * n
        target = red_ref if digit == 3 else grads
        block = 64 if n % 64 == 0 else NR

        def add(i, carry):
            here = rows_at(base + i * block, block)
            there = pl.ds(pl.multiple_of(at + i * block, NR), block)
            if gather_all:
                acc = jnp.zeros((block, width), F32)
                for s in range(seq):
                    slot = (seq_id - s + seq - 1) % seq
                    theirs = received[digit][jnp.minimum(slot, seq - 2), there].astype(F32)
                    acc = acc + jnp.where(seq_id == s, grads[here].astype(F32), theirs)
            else:
                acc = grads[here].astype(F32)
                for k in range(1, count[digit]):
                    acc = acc + received[digit][k - 1, there].astype(F32)
            target[here] = acc.astype(BF16)
            return carry

        lax.fori_loop(0, n // block, add, 0)

    def ag_copy(part, digit, k):
        base, n = region(part, digit + 1)
        _, device = peer(digit, k)
        return remote(
            red_ref.at[rows_at(base, n)], red_ref.at[rows_at(base, n)],
            ag_send.at[part, digit, k - 1], ag_recv.at[part, digit, k - 1], device,
        )

    def ag_start(part, digit):
        if digit == 3 and not plan.scatter:
            return
        for k in range(1, count[digit]):
            ag_copy(part, digit, k).start()

    def ag_finish(part, digit):
        if digit == 3 and not plan.scatter:
            return
        for k in range(1, count[digit]):
            ag_copy(part, digit, k).wait_recv()

    def part_steps(part):
        steps = [functools.partial(rs_start, part, 0)]
        for digit in range(1, 4):
            steps.append(
                functools.partial(
                    sequence,
                    functools.partial(rs_finish, part, digit - 1),
                    functools.partial(rs_start, part, digit),
                )
            )
        steps.append(
            functools.partial(
                sequence, functools.partial(rs_finish, part, 3), functools.partial(ag_start, part, 3)
            )
        )
        for digit in (2, 1, 0):
            steps.append(
                functools.partial(
                    sequence,
                    functools.partial(ag_finish, part, digit + 1),
                    functools.partial(ag_start, part, digit),
                )
            )
        steps.append(functools.partial(ag_finish, part, 0))
        return steps

    all_steps = [part_steps(part) for part in range(len(plan.parts))]

    def step(part, number):
        all_steps[part][number]()

    at_place = {}
    reached_step = [0] * (len(plan.parts) + 1)
    for place, parts_here in ORDER.items():
        at_place[place] = []
        for part in parts_here:
            reached_step[part] += 1
            at_place[place].append((part, reached_step[part]))

    def advance(place):
        for part, number in at_place.get(place, ()):
            if part < 0:
                vec_finish(number - 1)
                if number < 4:
                    vec_start(number)
            else:
                step(part, number)

    load_o.wait()
    load_up.wait()
    res = tok[...].astype(F32) + dot(att[...], wo[...]) + vec(4)
    mid[...] = res
    center = res - mean(res)
    rstd = lax.rsqrt(mean(center * center) + EPSILON)
    normed = center * rstd
    n2[...] = normed
    stats[1] = jnp.broadcast_to(rstd, (span, LANES))
    second[...] = (normed * vec(5) + vec(6)).astype(BF16)
    racc[...] = jnp.zeros_like(racc)
    dsec[...] = jnp.zeros_like(dsec)
    for copy in load_1:
        copy.wait()
    load_2.wait()
    curve = math.sqrt(2.0 / math.pi)

    def feed(t, carry):
        w2_rows = pl.ds(pl.multiple_of(t * tile, tile), tile)
        pre = dot(second[...], w1[t]) + inb[pl.ds(t, 1), :]
        square = pre * pre
        bend = jnp.tanh(curve * (pre + 0.044715 * (square * pre)))
        half = 0.5 * (1.0 + bend)
        act = (pre * half).astype(BF16)
        slope = half + 0.5 * pre * (1.0 - bend * bend) * (curve * (1.0 + 3 * 0.044715 * square))
        upstream = up[...]
        racc[...] += dot(act, w2[w2_rows])
        d_pre = (dot_nt(upstream, w2[w2_rows]) * slope).astype(BF16)
        base = 2 * t * tile
        grads[rows_at(base, tile)] = dot_tn(act, upstream).astype(BF16)
        grads[rows_at(base + tile, tile)] = dot_tn(second[...], d_pre).astype(BF16)
        rs_start(2 * t, 0)
        rs_start(2 * t + 1, 0)
        vstage[0, pl.ds(V_INNB + t, 1), :] = total(d_pre.astype(F32))
        dsec[...] += dot_nt(d_pre, w1[t])

        for when in range(tiles):
            if f"f{when}" in ORDER:
                pl.when(t == when)(functools.partial(advance, f"f{when}"))

        return carry

    lax.fori_loop(0, tiles, feed, 0)
    out_ref[0] = (mid[...] + racc[...] + vec(7)).astype(BF16)

    up_f = up[...].astype(F32)
    vstage[0, V_OUTB : V_OUTB + 1] = total(up_f)
    d_second, normed = dsec[...], n2[...]
    scaled = d_second * vec(5)
    vstage[0, V_MIDG : V_MIDG + 1] = total(d_second * normed)
    vstage[0, V_MIDS : V_MIDS + 1] = total(d_second)
    d_mid = up_f + (scaled - mean(scaled) - normed * mean(scaled * normed)) * stats[1][:, :1]
    mid[...] = d_mid
    d_branch = d_mid.astype(BF16)
    vstage[0, V_OB : V_OB + 1] = total(d_branch.astype(F32))
    grads[2 * hidden : 2 * hidden + width] = dot_tn(att[...], d_branch).astype(BF16)
    rs_start(2 * tiles, 0)
    advance("ln2")
    d_att = dot_nt(d_branch, wo[...]).astype(BF16)
    for b in range(pairs):
        dah[b] = d_att[:, b * LANES : (b + 1) * LANES]

    def attend_back(i, carry):
        c, b = i // pairs, i % pairs
        q2 = two_heads(qh[b, chunk_rows(c)])
        g2 = two_heads(dah[b, chunk_rows(c)])
        low = probs[i]
        prob = low.astype(F32)
        d_prob = dot_nt(g2, slots[c, pairs + b])
        weighted = prob * d_prob
        d_score = (weighted - prob * jnp.sum(weighted, axis=1, keepdims=True)).astype(BF16)
        d_query = merge_heads(dot(d_score, slots[c, b])) * (1.0 / math.sqrt(HEAD_DIM))
        dq[chunk_rows(c), pair_lanes(b)] = d_query.astype(BF16)
        dslots[c, b] = dot_tn(d_score, q2)
        dslots[c, pairs + b] = dot_tn(low, g2)
        for when in range(plan.chunks * pairs):
            if f"b{when}" in ORDER:
                pl.when(i == when)(functools.partial(advance, f"b{when}"))

        return carry

    lax.fori_loop(0, plan.chunks * pairs, attend_back, 0)

    def fold(b, carry):
        for c in range(plan.chunks):
            for s0, kind, at, n in slot_pieces(c):
                piece = dslots[c, b, s0 : s0 + n]
                if kind == "own":
                    parts_done = own_done[c].get((s0, at))
                    seen = parts_done if parts_done is not None else 0
                    if seen:
                        own[b, at : at + seen] += piece[:seen]
                    if seen < n:
                        own[b, at + seen : at + n] = piece[seen:]
                elif own_done[c].get((s0, kind)):
                    side = 0 if kind == "low" else 1
                    hsend[side, b, at : at + n] = (
                        hsend[side, b, at : at + n].astype(F32) + piece
                    ).astype(BF16)
                else:
                    side = 0 if kind == "low" else 1
                    hsend[side, b, at : at + n] = piece.astype(BF16)
        far = dslots[0, b, plan.far_slot :]
        for c in range(1, plan.chunks):
            far = far + dslots[c, b, plan.far_slot :]
        back = dot_tn(select, far.astype(BF16))
        for s in range(seq):
            fsend[s, b] = back[s * NR : (s + 1) * NR].astype(BF16)
        return carry

    own_done = []
    reached, halo_seen = {}, set()
    for c in range(plan.chunks):
        done = {}
        for s0, kind, at, n in slot_pieces(c):
            if kind == "own":
                lv = max(v for v in range(near + 1) if level_start(v) <= at)
                limit = reached.get(lv, level_start(lv))
                done[(s0, at)] = max(0, min(limit, at + n) - at)
                reached[lv] = max(limit, at + n)
            else:
                done[(s0, kind)] = (kind, at) in halo_seen
                halo_seen.add((kind, at))
        own_done.append(done)

    lax.fori_loop(0, blocks, fold, 0)

    def far_back(k):
        other, device = peer(3, k)
        return remote(
            fsend.at[other], frecv.at[k - 1], fback_send.at[k - 1], fback_recv.at[k - 1], device
        )

    halo_start(hsend, hrecv, back_send, back_recv)
    for k in range(1, seq):
        far_back(k).start()

    advance("fold")

    d_query = dq[...]
    vstage[0, V_QB : V_QB + 1] = total(d_query.astype(F32))
    off_c = 2 * hidden + width
    grads[off_c : off_c + width] = dot_tn(first[...], d_query).astype(BF16)
    d_first = dot_nt(d_query, wq[...])
    racc[...] = d_first
    rs_start(2 * tiles + 1, 0)
    advance("q")

    halo_wait(hsend, hrecv, back_send, back_recv)
    for k in range(1, seq):
        far_back(k).wait()
    for lv in range(near + 1):
        at, n = level_start(lv), span >> lv
        lo, hi = lv * NR, (lv + 1) * NR
        own[:, at : at + NR] += hrecv[0, :, lo:hi].astype(F32)
        own[:, at + n - NR : at + n] += hrecv[1, :, lo:hi].astype(F32)
    far_sum = fsend[seq_id].astype(F32)
    for k in range(1, seq):
        far_sum = far_sum + frecv[k - 1].astype(F32)
    for b in range(blocks):
        cols = slice(b * LANES, (b + 1) * LANES)
        coarse[:far_at, cols] = own[b, span : span + far_at].astype(BF16)
        coarse[far_at:, cols] = far_sum[b].astype(BF16)
    for half in range(2):
        passed = dot(spread[...], coarse[:, half * width : (half + 1) * width])
        for b in range(pairs):
            cols = slice((half * pairs + b) * LANES, (half * pairs + b + 1) * LANES)
            dkv[:, cols] = (
                own[half * pairs + b, :span] + passed[:, b * LANES : (b + 1) * LANES]
            ).astype(BF16)
    d_keys, d_values = dkv[:, :width], dkv[:, width:]
    vstage[0, V_VB : V_VB + 1] = total(d_values.astype(F32))
    grads[off_c + width : off_c + 2 * width] = dot_tn(first[...], d_keys).astype(BF16)
    grads[off_c + 2 * width : off_c + 3 * width] = dot_tn(first[...], d_values).astype(BF16)
    rs_start(2 * tiles + 2, 0)
    rs_start(2 * tiles + 3, 0)
    advance("dkv")
    d_first = racc[...] + dot_nt(d_keys, wk[...]) + dot_nt(d_values, wv[...])
    normed = n1[...]
    scaled = d_first * vec(0)
    vstage[0, V_PREG : V_PREG + 1] = total(d_first * normed)
    vstage[0, V_PRES : V_PRES + 1] = total(d_first)
    d_in = mid[...] + (scaled - mean(scaled) - normed * mean(scaled * normed)) * stats[0][:, :1]
    gin_ref[0] = d_in.astype(BF16)

    vec_received = [vrecv0, vrecv1, vrecv2, vrecv3]

    def vec_copy(digit, k):
        _, device = peer(digit, k)
        return remote(
            vstage.at[digit], vec_received[digit].at[index[digit]],
            vec_send.at[digit, k - 1], vec_recv.at[digit, k - 1], device,
        )

    def vec_start(digit):
        for k in range(1, count[digit]):
            vec_copy(digit, k).start()

    def vec_finish(digit):
        for k in range(1, count[digit]):
            vec_copy(digit, k).wait_recv()
        acc = jnp.zeros((VEC_ROWS, width), F32)
        for s in range(count[digit]):
            acc = acc + jnp.where(index[digit] == s, vstage[digit], vec_received[digit][s])
        if digit == 3:
            vout_ref[...] = acc
        else:
            vstage[digit + 1] = acc

    vec_start(0)
    advance("ln1")

    for part in range(len(plan.parts)):
        for digit in range(4):
            for k in range(1, count[digit]):
                rs_copy(part, digit, k).wait_send()
                if digit < 3 or plan.scatter:
                    ag_copy(part, digit, k).wait_send()
    for digit in range(4):
        for k in range(1, count[digit]):
            vec_copy(digit, k).wait_send()


def unpack_kernel(
    width, tiles, red_ref, vec_ref, out_in, gin_in,
    query_ref, key_ref, value_ref, output_ref, inner_ref, outer_ref,
    preg_ref, pres_ref, qb_ref, vb_ref, ob_ref, midg_ref, mids_ref, outb_ref, innb_ref,
    out_ref, gin_ref, wide, out_sem, through_sem,
):
    targets = []
    for t in range(tiles):
        rows = slice(t * width, (t + 1) * width)
        targets.append(outer_ref.at[rows])
        targets.append(inner_ref.at[:, rows])
    targets += [output_ref, query_ref, key_ref, value_ref]

    def put(i):
        return pltpu.make_async_copy(wide.at[i], targets[i], out_sem.at[i])

    def give(i):
        return pltpu.make_async_copy(
            (out_in, gin_in)[i], (out_ref, gin_ref)[i], through_sem.at[i]
        )

    for i in range(2):
        give(i).start()
    for i in range(len(targets)):
        wide[i] = red_ref[i * width : (i + 1) * width].astype(F32)
        put(i).start()
    for row, ref in (
        (V_PREG, preg_ref), (V_PRES, pres_ref), (V_QB, qb_ref), (V_VB, vb_ref), (V_OB, ob_ref),
        (V_MIDG, midg_ref), (V_MIDS, mids_ref), (V_OUTB, outb_ref),
    ):
        ref[...] = vec_ref[row]
    for t in range(tiles):
        innb_ref[t * width : (t + 1) * width] = vec_ref[V_INNB + t]
    for i in range(len(targets)):
        put(i).wait()
    for i in range(2):
        give(i).wait()


def shards(
    rows, seq,
    tokens, segment_ids, prenorm_gain, prenorm_shift, query_proj, query_bias, key_proj, value_proj,
    value_bias, output_proj, output_bias, midnorm_gain, midnorm_shift, inner_proj, inner_bias,
    outer_proj, outer_bias, upstream,
):
    _, span, width = tokens.shape
    hidden = inner_proj.shape[1]
    plan = Plan(rows, seq, span, width, hidden)
    tiles = hidden // width
    pairs = width // LANES
    count = plan.counts
    most = max(count) - 1
    vmem = pl.BlockSpec(memory_space=pltpu.VMEM)
    hbm = pl.BlockSpec(memory_space=pl.ANY)
    grad_rows = plan.grad_rows
    rest = [grad_rows // 2, grad_rows // 4, grad_rows // 4 // count[2]]
    last = rest[2] // seq if plan.scatter else rest[2]
    dma = pltpu.SemaphoreType.DMA
    items = plan.chunks * pairs
    n_parts = len(plan.parts)
    scratch = [
        pltpu.VMEM((span, width), BF16),
        pltpu.VMEM((span, width), BF16),
        pltpu.VMEM((width, width), BF16),
        pltpu.VMEM((width, width), BF16),
        pltpu.VMEM((width, width), BF16),
        pltpu.VMEM((width, width), BF16),
        pltpu.VMEM((tiles, width, width), BF16),
        pltpu.VMEM((hidden, width), BF16),
        pltpu.VMEM((span, width), F32),
        pltpu.VMEM((span, width), F32),
        pltpu.VMEM((span, width), F32),
        pltpu.VMEM((span, width), F32),
        pltpu.VMEM((span, width), F32),
        pltpu.VMEM((span, width), BF16),
        pltpu.VMEM((span, width), BF16),
        pltpu.VMEM((pairs, span, LANES), BF16),
        pltpu.VMEM((span, width), BF16),
        pltpu.VMEM((pairs, span, LANES), BF16),
        pltpu.VMEM((span, width), BF16),
        pltpu.VMEM((2 * pairs + 1, span + plan.far_row, LANES), BF16),
        pltpu.VMEM((2, 2 * pairs + 1, plan.edge, LANES), BF16),
        pltpu.VMEM((2, 2 * pairs + 1, plan.edge, LANES), BF16),
        pltpu.VMEM((seq, NR, 2 * width + LANES), BF16),
        pltpu.VMEM((plan.chunks, 2 * pairs + 1, plan.slots, LANES), BF16),
        pltpu.VMEM((plan.chunks, plan.chunk, plan.slots), F32),
        pltpu.VMEM((items, 2 * plan.chunk, plan.slots), BF16),
        pltpu.VMEM((plan.chunks, 2 * pairs, plan.slots, LANES), F32),
        pltpu.VMEM((2 * pairs, span + plan.far_row, LANES), F32),
        pltpu.VMEM((2, 2 * pairs, plan.edge, LANES), BF16),
        pltpu.VMEM((2, 2 * pairs, plan.edge, LANES), BF16),
        pltpu.VMEM((seq, 2 * pairs, NR, LANES), BF16),
        pltpu.VMEM((seq - 1, 2 * pairs, NR, LANES), BF16),
        pltpu.VMEM((plan.coarse_rows, 2 * width), BF16),
        pltpu.VMEM((span, plan.coarse_rows), BF16),
        pltpu.VMEM((span, 2 * width), BF16),
        pltpu.VMEM((grad_rows, width), BF16),
        pltpu.VMEM((count[0] - 1, rest[0], width), BF16),
        pltpu.VMEM((count[1] - 1, rest[1], width), BF16),
        pltpu.VMEM((count[2] - 1, rest[2], width), BF16),
        pltpu.VMEM((count[3] - 1, last, width), BF16),
        pltpu.VMEM((4, VEC_ROWS, width), F32),
        pltpu.VMEM((count[0], VEC_ROWS, width), F32),
        pltpu.VMEM((count[1], VEC_ROWS, width), F32),
        pltpu.VMEM((count[2], VEC_ROWS, width), F32),
        pltpu.VMEM((count[3], VEC_ROWS, width), F32),
        pltpu.VMEM((2, span, LANES), F32),
        pltpu.VMEM((tiles, width), F32),
        dma((7 + tiles,)),
        dma((2,)), dma((2,)),
        dma((seq - 1,)), dma((seq - 1,)),
        dma((2,)), dma((2,)),
        dma((seq - 1,)), dma((seq - 1,)),
        dma((n_parts, 4, most)), dma((n_parts, 4, most)),
        dma((n_parts, 4, most)), dma((n_parts, 4, most)),
        dma((4, most)), dma((4, most)),
    ]
    layer_output, input_grad, reduced, vecs = pl.pallas_call(
        functools.partial(layer_kernel, plan),
        out_shape=(
            pltpu.VMEM(tokens.shape, BF16),
            pltpu.VMEM(tokens.shape, BF16),
            pltpu.VMEM((grad_rows, width), BF16),
            pltpu.VMEM((VEC_ROWS, width), F32),
        ),
        in_specs=[
            hbm, vmem, vmem, vmem, hbm, vmem, hbm, hbm, vmem, hbm, vmem, vmem, vmem, hbm, vmem, hbm,
            vmem, hbm,
        ],
        out_specs=(vmem, vmem, vmem, vmem),
        scratch_shapes=scratch,
        compiler_params=pltpu.CompilerParams(
            collective_id=0, has_side_effects=True, vmem_limit_bytes=50 * 1024 * 1024
        ),
        name="layer",
    )(
        tokens, segment_ids, prenorm_gain, prenorm_shift, query_proj, query_bias, key_proj,
        value_proj, value_bias, output_proj, output_bias, midnorm_gain, midnorm_shift, inner_proj,
        inner_bias, outer_proj, outer_bias, upstream,
    )
    matrix = jax.ShapeDtypeStruct((width, width), F32)
    vector = jax.ShapeDtypeStruct((width,), F32)
    grads = pl.pallas_call(
        functools.partial(unpack_kernel, width, tiles),
        out_shape=(
            matrix, matrix, matrix, matrix,
            jax.ShapeDtypeStruct((width, hidden), F32),
            jax.ShapeDtypeStruct((hidden, width), F32),
            vector, vector, vector, vector, vector, vector, vector, vector,
            jax.ShapeDtypeStruct((hidden,), F32),
            jax.ShapeDtypeStruct(tokens.shape, BF16),
            jax.ShapeDtypeStruct(tokens.shape, BF16),
        ),
        in_specs=[vmem] * 4,
        out_specs=(hbm,) * 6 + (vmem,) * 9 + (hbm,) * 2,
        scratch_shapes=[
            pltpu.VMEM((n_parts, width, width), F32),
            dma((n_parts,)), dma((2,)),
        ],
        compiler_params=pltpu.CompilerParams(vmem_limit_bytes=24 * 1024 * 1024),
        name="unpack",
    )(reduced, vecs, layer_output, input_grad)
    (query_g, key_g, value_g, output_g, inner_g, outer_g,
     preg, pres, qb, vb, ob, midg, mids, outb, innb, layer_output, input_grad) = grads
    return (
        layer_output, input_grad, preg, pres, query_g, qb, key_g, value_g, vb, output_g, ob,
        midg, mids, inner_g, innb, outer_g, outb,
    )


def solution(mesh):
    split, ids, whole = P("rows", "seq", None), P("rows", "seq"), P()
    in_specs = (split, ids) + (whole,) * 15 + (split,)
    out_specs = (split, split) + (whole,) * 15
    return jax.shard_map(
        functools.partial(shards, mesh.shape["rows"], mesh.shape["seq"]),
        mesh=mesh, in_specs=in_specs, out_specs=out_specs, check_vma=False,
    )
```

```python
import functools
import math

import jax
import jax.numpy as jnp
from jax import lax
from jax.experimental import pallas as pl
from jax.experimental.pallas import tpu as pltpu
from jax.sharding import PartitionSpec as P

HEADS = 8
HEAD_DIM = 64
NR = 16
LANES = 128
LOG_TWO = math.log(2.0)
EPSILON = 1e-05
MASKED = -1e30
F32 = jnp.float32
BF16 = jnp.bfloat16
MESH = pl.DeviceIdType.MESH

VEC_ROWS = 16
V_PREG, V_PRES, V_QB, V_VB, V_OB, V_MIDG, V_MIDS, V_OUTB, V_INNB = 0, 1, 2, 3, 4, 5, 6, 7, 8


def dot(a, b):
    return jnp.dot(a, b, preferred_element_type=F32)


def dot_nt(a, b):
    return lax.dot_general(a, b, (((1,), (1,)), ((), ())), preferred_element_type=F32)


def dot_tn(a, b):
    return lax.dot_general(a, b, (((0,), (0,)), ((), ())), preferred_element_type=F32)


def iota(shape, dim):
    return lax.broadcasted_iota(jnp.int32, shape, dim)


def mean(x):
    return jnp.mean(x, axis=-1, keepdims=True)


def total(x):
    return jnp.sum(x, axis=0, keepdims=True)


ORDER = {
    "f2": [0, 1],
    "f3": [2, 3],
    "ln2": [4],
    "b0": [5],
    "b1": [0, 6],
    "b2": [1, 7, 8],
    "b4": [2],
    "b6": [0],
    "b7": [3, 1],
    "fold": [2],
    "q": [4, 0, 3, 1, 5, 9, 4, 6, 5, 7],
    "ln1": [
        2, 6, 8, 0, 7, 10, 9, 11, 3, 8, 1, 0, 4, -1, 9, 10, 5, 1, 2, 11, 6, 10, 0, -1,
        7, 2, 3, 0, 11, 1, 8, 4, 1, 2, 3, 9, -1, 4, 5, 2, 6, 3, 10, 5, 3, 7, 4, 6,
        11, -1, 8, 4, 5, 7, 9, 6, 10, 8, 5, 11, 6, 9, 7, 10, 7, 11, 8, 9, 8, 10, 9, 11,
        10, 11,
    ],
}


class Plan:
    def __init__(self, rows, seq, span, width, hidden):
        self.rows, self.seq, self.span, self.width, self.hidden = rows, seq, span, width, hidden
        self.near = (span // NR).bit_length() - 1
        self.length = span * seq
        self.top = (self.length // NR).bit_length() - 2
        self.chunk = 128
        self.chunks = span // self.chunk
        self.far = list(range(self.near + 1, self.top + 1))
        self.level_row = [0]
        at = 0
        for level in range(1, self.near + 1):
            self.level_row.append(at)
            at += span >> level
        self.far_row = at
        for level in self.far:
            self.level_row.append(at)
            at += span >> level
        self.far_rows = -(-(at - self.far_row) // 8) * 8
        self.coarse_rows = self.far_row + NR
        self.slot, self.slot_len = [], []
        at = 0
        for level in range(self.top + 1):
            n = 2 * NR + max(self.chunk >> level, NR)
            self.slot.append(at)
            self.slot_len.append(n)
            at += n
        self.used = at
        self.slots = -(-at // LANES) * LANES
        self.far_slot = self.slot[self.near + 1]
        self.far_slots = self.slots - self.far_slot
        self.edge = NR * (self.near + 1)
        self.grad_rows = 4 * width + 2 * hidden
        self.parts = [(p * width, width) for p in range(self.grad_rows // width)]
        self.counts = [2, 2, rows // 4, seq]
        self.swap = rows // 4 == 2
        self.scatter = (width // rows) % (NR * seq) == 0


def sequence(*steps):
    for step in steps:
        step()


def layer_kernel(
    plan,
    tok_hbm, ids_ref, preg_ref, pres_ref, wq_hbm, qb_ref, wk_hbm, wv_hbm, vb_ref, wo_hbm, ob_ref,
    midg_ref, mids_ref, w1_hbm, inb_ref, w2_hbm, outb_ref, up_hbm,
    out_ref, gin_ref, red_ref, vout_ref,
    tok, up, wq, wk, wv, wo, w1, w2, n1, n2, mid, racc, dsec, first, second, qh, att, dah, dq,
    level, edge, halo, far_k, far_v, slots, bias, probs, dslots, own, hsend, hrecv, fsend, frecv,
    coarse, spread, dkv, grads, recv0, recv1, recv2, recv3, vstage, vrecv0, vrecv1, vrecv2, vrecv3, stats,
    inb,
    in_sem, halo_send, halo_recv, far_send, far_recv, back_send, back_recv, fback_send, fback_recv,
    rs_send, rs_recv, ag_send, ag_recv, vec_send, vec_recv,
):
    span, width, hidden = plan.span, plan.width, plan.hidden
    seq, near, top = plan.seq, plan.near, plan.top
    tile = hidden // w1.shape[0]
    tiles = w1.shape[0]
    pairs = width // LANES
    blocks = 2 * pairs
    id_at, value_at = pairs, pairs + 1
    far_rows = plan.far_rows
    row_id, seq_id = lax.axis_index("rows"), lax.axis_index("seq")
    start = seq_id * span

    core = row_id % 2
    if plan.swap:
        stride_a, stride_b = 2 + 2 * core, 4 - 2 * core
    else:
        stride_a, stride_b = 2, 4
    count = plan.counts
    index = [
        core,
        (row_id // stride_a) % count[1],
        (row_id // stride_b) % count[2],
        seq_id,
    ]

    def peer(digit, k):
        other = (index[digit] + k) % count[digit]
        if digit == 3:
            return other, (row_id, other)
        stride = [1, stride_a, stride_b][digit]
        return other, (row_id + (other - index[digit]) * stride, seq_id)

    def remote(src, dst, send, recv, device):
        return pltpu.make_async_remote_copy(
            src_ref=src, dst_ref=dst, send_sem=send, recv_sem=recv,
            device_id=device, device_id_type=MESH,
        )

    loads = []

    def load(src, dst):
        copy = pltpu.make_async_copy(src, dst, in_sem.at[len(loads)])
        copy.start()
        loads.append(copy)
        return copy

    load_tok = load(tok_hbm.at[0], tok)
    load_q = load(wq_hbm, wq)
    load_k = load(wk_hbm, wk)
    load_v = load(wv_hbm, wv)
    load_up = load(up_hbm.at[0], up)
    load_o = load(wo_hbm, wo)
    load_1 = [load(w1_hbm.at[:, t * tile : (t + 1) * tile], w1.at[t]) for t in range(tiles)]
    load_2 = load(w2_hbm, w2)

    halo[...] = jnp.zeros_like(halo)
    hrecv[...] = jnp.zeros_like(hrecv)
    far_k[...] = jnp.zeros_like(far_k)
    far_v[...] = jnp.zeros_like(far_v)
    frecv[...] = jnp.zeros_like(frecv)
    vstage[0] = jnp.zeros((VEC_ROWS, width), F32)
    for t in range(tiles):
        inb[t : t + 1, :] = inb_ref[t * tile : (t + 1) * tile].reshape(1, tile)

    barrier = pltpu.get_barrier_semaphore()
    greeted = 0
    for digit in range(4):
        for k in range(1, count[digit]):
            _, device = peer(digit, k)
            pl.semaphore_signal(barrier, inc=1, device_id=device, device_id_type=MESH)
            greeted += 1

    vectors = (preg_ref, pres_ref, qb_ref, vb_ref, ob_ref, midg_ref, mids_ref, outb_ref)

    def vec(row):
        return vectors[row][...].reshape(1, width)

    load_tok.wait()
    x = tok[...].astype(F32)
    center = x - mean(x)
    rstd = lax.rsqrt(mean(center * center) + EPSILON)
    normed = center * rstd
    n1[...] = normed
    stats[0] = jnp.broadcast_to(rstd, (span, LANES))
    first[...] = (normed * vec(0) + vec(1)).astype(BF16)
    def averaging(rows_dim):
        shape = (plan.coarse_rows, span) if rows_dim == 0 else (span, plan.coarse_rows)
        r, p = iota(shape, rows_dim), iota(shape, 1 - rows_dim)
        matrix = jnp.zeros(shape, F32)
        for lv in range(1, top + 1):
            at = plan.level_row[lv]
            hit = (r - at == (p >> lv)) & (r >= at) & (r < at + (span >> lv))
            matrix = jnp.where(hit, 0.5**lv, matrix)
        return matrix.astype(BF16)

    def level_start(lv):
        return 0 if lv == 0 else span + plan.level_row[lv]

    far_at = plan.far_row

    def fill(at, fresh, coarser):
        for b in range(fresh.shape[1] // LANES):
            cols = slice(b * LANES, (b + 1) * LANES)
            level[at + b, :span] = fresh[:, cols]
            level[at + b, span : span + far_at] = coarser[:far_at, cols]

    def cut_edges(first_block, last_block):
        for lv in range(near + 1):
            at, n = level_start(lv), span >> lv
            to = slice(lv * NR, (lv + 1) * NR)
            edge[0, first_block:last_block, to] = level[first_block:last_block, at : at + NR]
            edge[1, first_block:last_block, to] = level[first_block:last_block, at + n - NR : at + n]

    def apart(other):
        return (other - seq_id > 1) | (other - seq_id < -1)

    class Halo:
        def __init__(self, src, dst, send, recv, blocks_sent=None):
            self.sems = send, recv
            self.src, self.dst, self.sent = src, dst, blocks_sent

        def copy(self, from_side, to_side, recv_side, step):
            send, recv = self.sems
            src, dst = self.src.at[from_side], self.dst.at[to_side]
            if self.sent is not None:
                src, dst = (
                    self.src.at[from_side, pl.ds(*self.sent)],
                    self.dst.at[to_side, pl.ds(*self.sent)],
                )
            return remote(
                src, dst, send.at[from_side], recv.at[recv_side], (row_id, seq_id + step)
            )

        def start(self):
            @pl.when(seq_id > 0)
            def _():
                self.copy(0, 1, 1, -1).start()

            @pl.when(seq_id < seq - 1)
            def _():
                self.copy(1, 0, 0, 1).start()

        def wait(self):
            @pl.when(seq_id > 0)
            def _():
                self.copy(0, 0, 0, -1).wait()

            @pl.when(seq_id < seq - 1)
            def _():
                self.copy(1, 1, 1, 1).wait()

    class Far:
        def __init__(self, src, dst, send, recv):
            self.src, self.dst, self.send, self.recv = src, dst, send, recv

        def copy(self, k):
            other, device = peer(3, k)
            return remote(
                self.src(other), self.dst(k), self.send.at[k - 1], self.recv.at[k - 1], device
            )

        def start(self):
            for k in range(1, seq):
                pl.when(apart(peer(3, k)[0]))(lambda: self.copy(k).start())

        def wait(self):
            for k in range(1, seq):
                pl.when(apart(peer(3, seq - k)[0]))(lambda: self.copy(k).wait_recv())
                pl.when(apart(peer(3, k)[0]))(lambda: self.copy(k).wait_send())

    key_halo = Halo(edge, halo, halo_send.at[0], halo_recv.at[0], (0, value_at))
    value_halo = Halo(edge, halo, halo_send.at[1], halo_recv.at[1], (value_at, pairs))
    key_far = Far(
        lambda other: far_k.at[seq_id], lambda k: far_k.at[seq_id], far_send.at[0], far_recv.at[0]
    )
    value_far = Far(
        lambda other: far_v.at[seq_id], lambda k: far_v.at[seq_id], far_send.at[1], far_recv.at[1]
    )

    matrix = averaging(0)
    load_k.wait()
    keys = dot(first[...], wk[...]).astype(BF16)
    mixed = dot(matrix, keys).astype(BF16)
    fill(0, keys, mixed)
    far_k[seq_id, :, :width] = mixed[far_at : far_at + far_rows]
    feature = (iota((LANES, span), 0) == ids_ref[...]).astype(F32).astype(BF16)
    unit = (iota((span, span), 0) == iota((span, span), 1)).astype(F32).astype(BF16)
    id_hot = dot_nt(unit, feature).astype(BF16)
    alike = dot(matrix, id_hot)
    alike = jnp.where((alike > 0.999) & (iota(alike.shape, 1) > 0), 1.0, 0.0).astype(BF16)
    fill(id_at, id_hot, alike)
    far_k[seq_id, :, width:] = alike[far_at : far_at + far_rows]
    cut_edges(0, value_at)

    pl.semaphore_wait(barrier, greeted)
    key_far.start()
    key_halo.start()

    load_v.wait()
    values = (dot(first[...], wv[...]) + vec(3)).astype(BF16)
    mixed = dot(matrix, values).astype(BF16)
    fill(value_at, values, mixed)
    far_v[seq_id] = mixed[far_at : far_at + far_rows]
    cut_edges(value_at, value_at + pairs)
    value_far.start()
    value_halo.start()

    load_q.wait()
    query = ((dot(first[...], wq[...]) + vec(2)).astype(BF16) * (1.0 / math.sqrt(HEAD_DIM))).astype(
        BF16
    )
    for b in range(pairs):
        qh[b] = query[:, b * LANES : (b + 1) * LANES]

    def slot_pieces(c):
        pieces = []
        for lv in range(near + 1):
            at, n = level_start(lv), span >> lv
            per = plan.chunk >> lv
            s0 = plan.slot[lv]
            if per >= NR:
                low, high = c * per - NR, c * per + per + NR
            else:
                low, high = -NR, n + NR
            if low < 0:
                pieces.append((s0, "low", lv * NR, NR))
                s0, low = s0 + NR, 0
            inner = min(high, n)
            pieces.append((s0, "own", at + low, inner - low))
            s0 += inner - low
            if high > n:
                pieces.append((s0, "high", lv * NR, NR))
        return pieces

    slot_at = iota((1, plan.slots), 1)
    slot_level = jnp.zeros((1, plan.slots), jnp.int32)
    for lv in range(1, top + 1):
        slot_level = slot_level + (slot_at >= plan.slot[lv]).astype(jnp.int32)
    for c in range(plan.chunks):
        origin = start + c * plan.chunk
        j = slot_at
        for lv in range(top + 1):
            if (plan.chunk >> lv) >= NR:
                base = origin // (1 << lv) - NR
            else:
                base = (origin // (NR << lv) - 1) * NR
            here = slot_at - plan.slot[lv] + base
            j = here if lv == 0 else jnp.where(slot_level == lv, here, j)
        position = origin + iota((plan.chunk, plan.slots), 0)
        off_block = (j >> 4) - (position >> (slot_level + 4))
        off_half = (j >> 3) - (position >> (slot_level + 3))
        reach = jnp.where(slot_level == 0, -1, 1)
        within = (jnp.abs(off_block) <= 1) & (jnp.abs(off_half) > reach)
        bias[c] = jnp.where(within, slot_level.astype(F32) * LOG_TWO, MASKED)

    def far_select():
        pieces = []
        for lv in plan.far:
            per_log = (span >> lv).bit_length() - 1
            first_row = plan.level_row[lv] - plan.far_row
            j = (start // (NR << lv) - 1) * NR + iota((3 * NR, seq * far_rows), 0)
            column = (j >> per_log) * far_rows + (j & ((1 << per_log) - 1)) + first_row
            pieces.append((column == iota((3 * NR, seq * far_rows), 1)).astype(F32))
        rest = plan.far_slots - 3 * NR * len(plan.far)
        if rest:
            pieces.append(jnp.zeros((rest, seq * far_rows), F32))
        return jnp.concatenate(pieces, axis=0).astype(BF16)

    select = far_select()
    spread[...] = averaging(1)

    def fill_slots(first_block, n_blocks, far_values):
        those = slice(first_block, first_block + n_blocks)
        for c in range(plan.chunks):
            for s0, kind, at, n in slot_pieces(c):
                if kind == "own":
                    slots[c, those, s0 : s0 + n] = level[those, at : at + n]
                else:
                    slots[c, those, s0 : s0 + n] = halo[
                        0 if kind == "low" else 1, those, at : at + n
                    ]
            for b in range(n_blocks):
                slots[c, first_block + b, plan.far_slot :] = far_values[
                    :, b * LANES : (b + 1) * LANES
                ]

    key_halo.wait()
    key_far.wait()
    fill_slots(
        0, value_at, dot(select, far_k[...].reshape(seq * far_rows, width + LANES)).astype(BF16)
    )
    for c in range(plan.chunks):
        same = dot_nt(level[id_at, c * plan.chunk : (c + 1) * plan.chunk], slots[c, id_at])
        bias[c] = jnp.where(same > 0.5, bias[c], MASKED)

    lane = iota((1, LANES), 1)
    low_half = (lane < HEAD_DIM).astype(F32).astype(BF16)
    high_half = (lane >= HEAD_DIM).astype(F32).astype(BF16)
    low_lanes = iota((plan.chunk, LANES), 1) < HEAD_DIM

    def two_heads(block):
        return jnp.concatenate([block * low_half, block * high_half], axis=0)

    def merge_heads(both):
        return jnp.where(low_lanes, both[: plan.chunk], both[plan.chunk :])

    def chunk_rows(c):
        return pl.ds(pl.multiple_of(c * plan.chunk, plan.chunk), plan.chunk)

    def pair_lanes(b):
        return pl.ds(pl.multiple_of(b * LANES, LANES), LANES)

    def attend(i, carry):
        c, b = i // pairs, i % pairs
        q2 = two_heads(qh[b, chunk_rows(c)])
        offset = bias[c]
        score = dot_nt(q2, slots[c, b]) + jnp.concatenate([offset, offset], axis=0)
        peak = jnp.max(score, axis=1, keepdims=True)
        raised = jnp.exp(score - peak)
        prob = raised * (1.0 / jnp.sum(raised, axis=1, keepdims=True))
        probs[i] = prob.astype(BF16)
        return carry

    lax.fori_loop(0, plan.chunks * pairs, attend, 0, unroll=2)

    value_halo.wait()
    value_far.wait()
    fill_slots(
        value_at, pairs, dot(select, far_v[...].reshape(seq * far_rows, width)).astype(BF16)
    )

    def mix(i, carry):
        c, b = i // pairs, i % pairs
        both = dot(probs[i], slots[c, value_at + b])
        att[chunk_rows(c), pair_lanes(b)] = merge_heads(both).astype(BF16)
        return carry

    lax.fori_loop(0, plan.chunks * pairs, mix, 0, unroll=2)

    received = [recv0, recv1, recv2, recv3]

    def region(part, digits):
        n = plan.parts[0][1]
        base = part * n
        for digit in range(digits):
            n = n // count[digit]
            base = base + index[digit] * n
        return base, n

    def rows_at(base, n):
        return pl.ds(pl.multiple_of(base, NR), n)

    def received_rows(part, n):
        return rows_at(part * n, n)

    def rs_copy(part, digit, k):
        base, n = region(part, digit)
        other, device = peer(digit, k)
        if digit == 3 and not plan.scatter:
            return remote(
                grads.at[rows_at(base, n)],
                received[digit].at[k - 1, received_rows(part, n)],
                rs_send.at[part, digit, k - 1], rs_recv.at[part, digit, k - 1], device,
            )
        n = n // count[digit]
        return remote(
            grads.at[rows_at(base + other * n, n)],
            received[digit].at[k - 1, received_rows(part, n)],
            rs_send.at[part, digit, k - 1], rs_recv.at[part, digit, k - 1], device,
        )

    def rs_start(part, digit):
        for k in range(1, count[digit]):
            rs_copy(part, digit, k).start()

    def rs_finish(part, digit):
        for k in range(1, count[digit]):
            rs_copy(part, digit, k).wait()
        gather_all = digit == 3 and not plan.scatter
        base, n = region(part, digit if gather_all else digit + 1)
        at = part * n
        target = red_ref if digit == 3 else grads
        block = 64 if n % 64 == 0 else NR

        def add(i, carry):
            here = rows_at(base + i * block, block)
            there = pl.ds(pl.multiple_of(at + i * block, NR), block)
            if gather_all:
                acc = jnp.zeros((block, width), F32)
                for s in range(seq):
                    slot = (seq_id - s + seq - 1) % seq
                    theirs = received[digit][jnp.minimum(slot, seq - 2), there].astype(F32)
                    acc = acc + jnp.where(seq_id == s, grads[here].astype(F32), theirs)
            else:
                acc = grads[here].astype(F32)
                for k in range(1, count[digit]):
                    acc = acc + received[digit][k - 1, there].astype(F32)
            target[here] = acc.astype(BF16)
            return carry

        lax.fori_loop(0, n // block, add, 0)

    def ag_copy(part, digit, k):
        base, n = region(part, digit + 1)
        _, device = peer(digit, k)
        return remote(
            red_ref.at[rows_at(base, n)], red_ref.at[rows_at(base, n)],
            ag_send.at[part, digit, k - 1], ag_recv.at[part, digit, k - 1], device,
        )

    def ag_start(part, digit):
        if digit == 3 and not plan.scatter:
            return
        for k in range(1, count[digit]):
            ag_copy(part, digit, k).start()

    def ag_finish(part, digit):
        if digit == 3 and not plan.scatter:
            return
        for k in range(1, count[digit]):
            ag_copy(part, digit, k).wait()

    def part_steps(part):
        steps = [functools.partial(rs_start, part, 0)]
        for digit in range(1, 4):
            steps.append(
                functools.partial(
                    sequence,
                    functools.partial(rs_finish, part, digit - 1),
                    functools.partial(rs_start, part, digit),
                )
            )
        steps.append(
            functools.partial(
                sequence, functools.partial(rs_finish, part, 3), functools.partial(ag_start, part, 3)
            )
        )
        for digit in (2, 1, 0):
            steps.append(
                functools.partial(
                    sequence,
                    functools.partial(ag_finish, part, digit + 1),
                    functools.partial(ag_start, part, digit),
                )
            )
        steps.append(functools.partial(ag_finish, part, 0))
        return steps

    all_steps = [part_steps(part) for part in range(len(plan.parts))]

    def step(part, number):
        all_steps[part][number]()

    at_place = {}
    reached_step = [0] * (len(plan.parts) + 1)
    for place, parts_here in ORDER.items():
        at_place[place] = []
        for part in parts_here:
            reached_step[part] += 1
            at_place[place].append((part, reached_step[part]))

    def advance(place):
        for part, number in at_place.get(place, ()):
            if part < 0:
                vec_finish(number - 1)
                if number < 4:
                    vec_start(number)
            else:
                step(part, number)

    load_o.wait()
    load_up.wait()
    res = tok[...].astype(F32) + dot(att[...], wo[...]) + vec(4)
    mid[...] = res
    center = res - mean(res)
    rstd = lax.rsqrt(mean(center * center) + EPSILON)
    normed = center * rstd
    n2[...] = normed
    stats[1] = jnp.broadcast_to(rstd, (span, LANES))
    second[...] = (normed * vec(5) + vec(6)).astype(BF16)
    racc[...] = jnp.zeros_like(racc)
    dsec[...] = jnp.zeros_like(dsec)
    for copy in load_1:
        copy.wait()
    load_2.wait()
    curve = math.sqrt(2.0 / math.pi)

    def feed(t, carry):
        w2_rows = pl.ds(pl.multiple_of(t * tile, tile), tile)
        pre = dot(second[...], w1[t]) + inb[pl.ds(t, 1), :]
        square = pre * pre
        bend = jnp.tanh(curve * (pre + 0.044715 * (square * pre)))
        half = 0.5 * (1.0 + bend)
        act = (pre * half).astype(BF16)
        slope = half + 0.5 * pre * (1.0 - bend * bend) * (curve * (1.0 + 3 * 0.044715 * square))
        upstream = up[...]
        racc[...] += dot(act, w2[w2_rows])
        d_pre = (dot_nt(upstream, w2[w2_rows]) * slope).astype(BF16)
        base = 2 * t * tile
        grads[rows_at(base, tile)] = dot_tn(act, upstream).astype(BF16)
        grads[rows_at(base + tile, tile)] = dot_tn(second[...], d_pre).astype(BF16)
        rs_start(2 * t, 0)
        rs_start(2 * t + 1, 0)
        vstage[0, pl.ds(V_INNB + t, 1), :] = total(d_pre.astype(F32))
        dsec[...] += dot_nt(d_pre, w1[t])

        for when in range(tiles):
            if f"f{when}" in ORDER:
                pl.when(t == when)(functools.partial(advance, f"f{when}"))

        return carry

    lax.fori_loop(0, tiles, feed, 0)
    out_ref[0] = (mid[...] + racc[...] + vec(7)).astype(BF16)

    up_f = up[...].astype(F32)
    vstage[0, V_OUTB : V_OUTB + 1] = total(up_f)
    d_second, normed = dsec[...], n2[...]
    scaled = d_second * vec(5)
    vstage[0, V_MIDG : V_MIDG + 1] = total(d_second * normed)
    vstage[0, V_MIDS : V_MIDS + 1] = total(d_second)
    d_mid = up_f + (scaled - mean(scaled) - normed * mean(scaled * normed)) * stats[1][:, :1]
    mid[...] = d_mid
    d_branch = d_mid.astype(BF16)
    vstage[0, V_OB : V_OB + 1] = total(d_branch.astype(F32))
    grads[2 * hidden : 2 * hidden + width] = dot_tn(att[...], d_branch).astype(BF16)
    rs_start(2 * tiles, 0)
    advance("ln2")
    d_att = dot_nt(d_branch, wo[...]).astype(BF16)
    for b in range(pairs):
        dah[b] = d_att[:, b * LANES : (b + 1) * LANES]

    def attend_back(i, carry):
        c, b = i // pairs, i % pairs
        q2 = two_heads(qh[b, chunk_rows(c)])
        g2 = two_heads(dah[b, chunk_rows(c)])
        low = probs[i]
        prob = low.astype(F32)
        d_prob = dot_nt(g2, slots[c, value_at + b])
        weighted = prob * d_prob
        d_score = (weighted - prob * jnp.sum(weighted, axis=1, keepdims=True)).astype(BF16)
        d_query = merge_heads(dot(d_score, slots[c, b])) * (1.0 / math.sqrt(HEAD_DIM))
        dq[chunk_rows(c), pair_lanes(b)] = d_query.astype(BF16)
        dslots[c, b] = dot_tn(d_score, q2)
        dslots[c, pairs + b] = dot_tn(low, g2)
        for when in range(plan.chunks * pairs):
            if f"b{when}" in ORDER:
                pl.when(i == when)(functools.partial(advance, f"b{when}"))

        return carry

    lax.fori_loop(0, plan.chunks * pairs, attend_back, 0)

    def fold(b, carry):
        for c in range(plan.chunks):
            for s0, kind, at, n in slot_pieces(c):
                piece = dslots[c, b, s0 : s0 + n]
                if kind == "own":
                    parts_done = own_done[c].get((s0, at))
                    seen = parts_done if parts_done is not None else 0
                    if seen:
                        own[b, at : at + seen] += piece[:seen]
                    if seen < n:
                        own[b, at + seen : at + n] = piece[seen:]
                elif own_done[c].get((s0, kind)):
                    side = 0 if kind == "low" else 1
                    hsend[side, b, at : at + n] = (
                        hsend[side, b, at : at + n].astype(F32) + piece
                    ).astype(BF16)
                else:
                    side = 0 if kind == "low" else 1
                    hsend[side, b, at : at + n] = piece.astype(BF16)
        far = dslots[0, b, plan.far_slot :]
        for c in range(1, plan.chunks):
            far = far + dslots[c, b, plan.far_slot :]
        back = dot_tn(select, far.astype(BF16))
        for s in range(seq):
            fsend[s, b] = back[s * far_rows : (s + 1) * far_rows].astype(BF16)
        return carry

    own_done = []
    reached, halo_seen = {}, set()
    for c in range(plan.chunks):
        done = {}
        for s0, kind, at, n in slot_pieces(c):
            if kind == "own":
                lv = max(v for v in range(near + 1) if level_start(v) <= at)
                limit = reached.get(lv, level_start(lv))
                done[(s0, at)] = max(0, min(limit, at + n) - at)
                reached[lv] = max(limit, at + n)
            else:
                done[(s0, kind)] = (kind, at) in halo_seen
                halo_seen.add((kind, at))
        own_done.append(done)

    lax.fori_loop(0, blocks, fold, 0)

    back_halo = Halo(hsend, hrecv, back_send, back_recv)
    back_far = Far(
        lambda other: fsend.at[other], lambda k: frecv.at[k - 1], fback_send, fback_recv
    )
    back_far.start()
    back_halo.start()
    advance("fold")

    d_query = dq[...]
    vstage[0, V_QB : V_QB + 1] = total(d_query.astype(F32))
    off_c = 2 * hidden + width
    grads[off_c : off_c + width] = dot_tn(first[...], d_query).astype(BF16)
    d_first = dot_nt(d_query, wq[...])
    racc[...] = d_first
    rs_start(2 * tiles + 1, 0)
    advance("q")

    back_halo.wait()
    back_far.wait()
    for lv in range(near + 1):
        at, n = level_start(lv), span >> lv
        lo, hi = lv * NR, (lv + 1) * NR
        own[:, at : at + NR] += hrecv[0, :, lo:hi].astype(F32)
        own[:, at + n - NR : at + n] += hrecv[1, :, lo:hi].astype(F32)
    far_sum = fsend[seq_id].astype(F32)
    for k in range(1, seq):
        far_sum = far_sum + frecv[k - 1].astype(F32)
    coarse[far_at:] = jnp.zeros((plan.coarse_rows - far_at, 2 * width), BF16)
    for b in range(blocks):
        cols = slice(b * LANES, (b + 1) * LANES)
        coarse[:far_at, cols] = own[b, span : span + far_at].astype(BF16)
        coarse[far_at : far_at + far_rows, cols] = far_sum[b].astype(BF16)
    for half in range(2):
        passed = dot(spread[...], coarse[:, half * width : (half + 1) * width])
        for b in range(pairs):
            cols = slice((half * pairs + b) * LANES, (half * pairs + b + 1) * LANES)
            dkv[:, cols] = (
                own[half * pairs + b, :span] + passed[:, b * LANES : (b + 1) * LANES]
            ).astype(BF16)
    d_keys, d_values = dkv[:, :width], dkv[:, width:]
    vstage[0, V_VB : V_VB + 1] = total(d_values.astype(F32))
    grads[off_c + width : off_c + 2 * width] = dot_tn(first[...], d_keys).astype(BF16)
    grads[off_c + 2 * width : off_c + 3 * width] = dot_tn(first[...], d_values).astype(BF16)
    rs_start(2 * tiles + 2, 0)
    rs_start(2 * tiles + 3, 0)
    advance("dkv")
    d_first = racc[...] + dot_nt(d_keys, wk[...]) + dot_nt(d_values, wv[...])
    normed = n1[...]
    scaled = d_first * vec(0)
    vstage[0, V_PREG : V_PREG + 1] = total(d_first * normed)
    vstage[0, V_PRES : V_PRES + 1] = total(d_first)
    d_in = mid[...] + (scaled - mean(scaled) - normed * mean(scaled * normed)) * stats[0][:, :1]
    gin_ref[0] = d_in.astype(BF16)

    vec_received = [vrecv0, vrecv1, vrecv2, vrecv3]

    def vec_copy(digit, k):
        _, device = peer(digit, k)
        return remote(
            vstage.at[digit], vec_received[digit].at[index[digit]],
            vec_send.at[digit, k - 1], vec_recv.at[digit, k - 1], device,
        )

    def vec_start(digit):
        for k in range(1, count[digit]):
            vec_copy(digit, k).start()

    def vec_finish(digit):
        for k in range(1, count[digit]):
            vec_copy(digit, k).wait()
        acc = jnp.zeros((VEC_ROWS, width), F32)
        for s in range(count[digit]):
            acc = acc + jnp.where(index[digit] == s, vstage[digit], vec_received[digit][s])
        if digit == 3:
            vout_ref[...] = acc
        else:
            vstage[digit + 1] = acc

    vec_start(0)
    advance("ln1")


def unpack_kernel(
    width, tiles, red_ref, vec_ref, out_in, gin_in,
    query_ref, key_ref, value_ref, output_ref, inner_ref, outer_ref,
    preg_ref, pres_ref, qb_ref, vb_ref, ob_ref, midg_ref, mids_ref, outb_ref, innb_ref,
    out_ref, gin_ref, wide, out_sem, through_sem,
):
    targets = []
    for t in range(tiles):
        rows = slice(t * width, (t + 1) * width)
        targets.append(outer_ref.at[rows])
        targets.append(inner_ref.at[:, rows])
    targets += [output_ref, query_ref, key_ref, value_ref]

    def put(i):
        return pltpu.make_async_copy(wide.at[i], targets[i], out_sem.at[i])

    def give(i):
        return pltpu.make_async_copy(
            (out_in, gin_in)[i], (out_ref, gin_ref)[i], through_sem.at[i]
        )

    for i in range(2):
        give(i).start()
    for i in range(len(targets)):
        wide[i] = red_ref[i * width : (i + 1) * width].astype(F32)
        put(i).start()
    for row, ref in (
        (V_PREG, preg_ref), (V_PRES, pres_ref), (V_QB, qb_ref), (V_VB, vb_ref), (V_OB, ob_ref),
        (V_MIDG, midg_ref), (V_MIDS, mids_ref), (V_OUTB, outb_ref),
    ):
        ref[...] = vec_ref[row]
    for t in range(tiles):
        innb_ref[t * width : (t + 1) * width] = vec_ref[V_INNB + t]
    for i in range(len(targets)):
        put(i).wait()
    for i in range(2):
        give(i).wait()


def shards(
    rows, seq,
    tokens, segment_ids, prenorm_gain, prenorm_shift, query_proj, query_bias, key_proj, value_proj,
    value_bias, output_proj, output_bias, midnorm_gain, midnorm_shift, inner_proj, inner_bias,
    outer_proj, outer_bias, upstream,
):
    _, span, width = tokens.shape
    hidden = inner_proj.shape[1]
    plan = Plan(rows, seq, span, width, hidden)
    tiles = hidden // width
    pairs = width // LANES
    count = plan.counts
    most = max(count) - 1
    vmem = pl.BlockSpec(memory_space=pltpu.VMEM)
    hbm = pl.BlockSpec(memory_space=pl.ANY)
    grad_rows = plan.grad_rows
    rest = [grad_rows // 2, grad_rows // 4, grad_rows // 4 // count[2]]
    last = rest[2] // seq if plan.scatter else rest[2]
    dma = pltpu.SemaphoreType.DMA
    items = plan.chunks * pairs
    n_parts = len(plan.parts)
    scratch = [
        pltpu.VMEM((span, width), BF16),
        pltpu.VMEM((span, width), BF16),
        pltpu.VMEM((width, width), BF16),
        pltpu.VMEM((width, width), BF16),
        pltpu.VMEM((width, width), BF16),
        pltpu.VMEM((width, width), BF16),
        pltpu.VMEM((tiles, width, width), BF16),
        pltpu.VMEM((hidden, width), BF16),
        pltpu.VMEM((span, width), F32),
        pltpu.VMEM((span, width), F32),
        pltpu.VMEM((span, width), F32),
        pltpu.VMEM((span, width), F32),
        pltpu.VMEM((span, width), F32),
        pltpu.VMEM((span, width), BF16),
        pltpu.VMEM((span, width), BF16),
        pltpu.VMEM((pairs, span, LANES), BF16),
        pltpu.VMEM((span, width), BF16),
        pltpu.VMEM((pairs, span, LANES), BF16),
        pltpu.VMEM((span, width), BF16),
        pltpu.VMEM((2 * pairs + 1, span + plan.far_row, LANES), BF16),
        pltpu.VMEM((2, 2 * pairs + 1, plan.edge, LANES), BF16),
        pltpu.VMEM((2, 2 * pairs + 1, plan.edge, LANES), BF16),
        pltpu.VMEM((seq, plan.far_rows, width + LANES), BF16),
        pltpu.VMEM((seq, plan.far_rows, width), BF16),
        pltpu.VMEM((plan.chunks, 2 * pairs + 1, plan.slots, LANES), BF16),
        pltpu.VMEM((plan.chunks, plan.chunk, plan.slots), F32),
        pltpu.VMEM((items, 2 * plan.chunk, plan.slots), BF16),
        pltpu.VMEM((plan.chunks, 2 * pairs, plan.slots, LANES), F32),
        pltpu.VMEM((2 * pairs, span + plan.far_row, LANES), F32),
        pltpu.VMEM((2, 2 * pairs, plan.edge, LANES), BF16),
        pltpu.VMEM((2, 2 * pairs, plan.edge, LANES), BF16),
        pltpu.VMEM((seq, 2 * pairs, plan.far_rows, LANES), BF16),
        pltpu.VMEM((seq - 1, 2 * pairs, plan.far_rows, LANES), BF16),
        pltpu.VMEM((plan.coarse_rows, 2 * width), BF16),
        pltpu.VMEM((span, plan.coarse_rows), BF16),
        pltpu.VMEM((span, 2 * width), BF16),
        pltpu.VMEM((grad_rows, width), BF16),
        pltpu.VMEM((count[0] - 1, rest[0], width), BF16),
        pltpu.VMEM((count[1] - 1, rest[1], width), BF16),
        pltpu.VMEM((count[2] - 1, rest[2], width), BF16),
        pltpu.VMEM((count[3] - 1, last, width), BF16),
        pltpu.VMEM((4, VEC_ROWS, width), F32),
        pltpu.VMEM((count[0], VEC_ROWS, width), F32),
        pltpu.VMEM((count[1], VEC_ROWS, width), F32),
        pltpu.VMEM((count[2], VEC_ROWS, width), F32),
        pltpu.VMEM((count[3], VEC_ROWS, width), F32),
        pltpu.VMEM((2, span, LANES), F32),
        pltpu.VMEM((tiles, width), F32),
        dma((7 + tiles,)),
        dma((2, 2)), dma((2, 2)),
        dma((2, seq - 1)), dma((2, seq - 1)),
        dma((2,)), dma((2,)),
        dma((seq - 1,)), dma((seq - 1,)),
        dma((n_parts, 4, most)), dma((n_parts, 4, most)),
        dma((n_parts, 4, most)), dma((n_parts, 4, most)),
        dma((4, most)), dma((4, most)),
    ]
    layer_output, input_grad, reduced, vecs = pl.pallas_call(
        functools.partial(layer_kernel, plan),
        out_shape=(
            pltpu.VMEM(tokens.shape, BF16),
            pltpu.VMEM(tokens.shape, BF16),
            pltpu.VMEM((grad_rows, width), BF16),
            pltpu.VMEM((VEC_ROWS, width), F32),
        ),
        in_specs=[
            hbm, vmem, vmem, vmem, hbm, vmem, hbm, hbm, vmem, hbm, vmem, vmem, vmem, hbm, vmem, hbm,
            vmem, hbm,
        ],
        out_specs=(vmem, vmem, vmem, vmem),
        scratch_shapes=scratch,
        compiler_params=pltpu.CompilerParams(
            collective_id=0, has_side_effects=True, vmem_limit_bytes=50 * 1024 * 1024
        ),
        name="layer",
    )(
        tokens, segment_ids, prenorm_gain, prenorm_shift, query_proj, query_bias, key_proj,
        value_proj, value_bias, output_proj, output_bias, midnorm_gain, midnorm_shift, inner_proj,
        inner_bias, outer_proj, outer_bias, upstream,
    )
    matrix = jax.ShapeDtypeStruct((width, width), F32)
    vector = jax.ShapeDtypeStruct((width,), F32)
    grads = pl.pallas_call(
        functools.partial(unpack_kernel, width, tiles),
        out_shape=(
            matrix, matrix, matrix, matrix,
            jax.ShapeDtypeStruct((width, hidden), F32),
            jax.ShapeDtypeStruct((hidden, width), F32),
            vector, vector, vector, vector, vector, vector, vector, vector,
            jax.ShapeDtypeStruct((hidden,), F32),
            jax.ShapeDtypeStruct(tokens.shape, BF16),
            jax.ShapeDtypeStruct(tokens.shape, BF16),
        ),
        in_specs=[vmem] * 4,
        out_specs=(hbm,) * 6 + (vmem,) * 9 + (hbm,) * 2,
        scratch_shapes=[
            pltpu.VMEM((n_parts, width, width), F32),
            dma((n_parts,)), dma((2,)),
        ],
        compiler_params=pltpu.CompilerParams(vmem_limit_bytes=24 * 1024 * 1024),
        name="unpack",
    )(reduced, vecs, layer_output, input_grad)
    (query_g, key_g, value_g, output_g, inner_g, outer_g,
     preg, pres, qb, vb, ob, midg, mids, outb, innb, layer_output, input_grad) = grads
    return (
        layer_output, input_grad, preg, pres, query_g, qb, key_g, value_g, vb, output_g, ob,
        midg, mids, inner_g, innb, outer_g, outb,
    )


def solution(mesh):
    split, ids, whole = P("rows", "seq", None), P("rows", "seq"), P()
    in_specs = (split, ids) + (whole,) * 15 + (split,)
    out_specs = (split, split) + (whole,) * 15
    return jax.shard_map(
        functools.partial(shards, mesh.shape["rows"], mesh.shape["seq"]),
        mesh=mesh, in_specs=in_specs, out_specs=out_specs, check_vma=False,
    )
```

```python
import functools
import math

import jax
import jax.numpy as jnp
from jax import lax
from jax.experimental import pallas as pl
from jax.experimental.pallas import tpu as pltpu
from jax.sharding import PartitionSpec as P

HEADS = 8
HEAD_DIM = 64
NR = 16
LANES = 128
LOG_TWO = math.log(2.0)
EPSILON = 1e-05
MASKED = -1e30
F32 = jnp.float32
BF16 = jnp.bfloat16
MESH = pl.DeviceIdType.MESH

VEC_ROWS = 16
V_PREG, V_PRES, V_QB, V_VB, V_OB, V_MIDG, V_MIDS, V_OUTB, V_INNB = 0, 1, 2, 3, 4, 5, 6, 7, 8


def dot(a, b):
    return jnp.dot(a, b, preferred_element_type=F32)


def dot_nt(a, b):
    return lax.dot_general(a, b, (((1,), (1,)), ((), ())), preferred_element_type=F32)


def dot_tn(a, b):
    return lax.dot_general(a, b, (((0,), (0,)), ((), ())), preferred_element_type=F32)


def iota(shape, dim):
    return lax.broadcasted_iota(jnp.int32, shape, dim)


def mean(x):
    return jnp.mean(x, axis=-1, keepdims=True)


def total(x):
    return jnp.sum(x, axis=0, keepdims=True)


ORDER = {
    "f1": [0],
    "f2": [1, 2],
    "f3": [3, 4, 5],
    "ln2": [0],
    "b0": [6, 7],
    "b1": [1, 8],
    "b3": [2],
    "b5": [0],
    "b6": [3],
    "b7": [1],
    "fold": [2, 4],
    "q": [3, 5, 9, 0, 6, 1, 4, 7, 5, 6, 8],
    "ln1": [
        2, 7, 9, 10, 3, 11, 8, 0, 9, 1, 4, 10, -1, 5, 0, 11, 6, 1, 10, 2, -1, 7, 0, 11,
        3, 0, 8, 2, 1, 9, 1, 3, -1, 4, 5, 2, 6, 2, 10, 4, 3, 5, 7, 3, 6, 11, -1, 8,
        4, 9, 7, 4, 5, 10, 5, 8, 11, 6, 9, 6, 10, 7, 11, 7, 8, 9, 8, 10, 9, 11, 10, 11,
    ],
}


class Plan:
    def __init__(self, rows, seq, span, width, hidden):
        self.rows, self.seq, self.span, self.width, self.hidden = rows, seq, span, width, hidden
        self.near = (span // NR).bit_length() - 1
        self.length = span * seq
        self.top = (self.length // NR).bit_length() - 2
        self.chunk = 128
        self.chunks = span // self.chunk
        self.far = list(range(self.near + 1, self.top + 1))
        self.level_row = [0]
        at = 0
        for level in range(1, self.near + 1):
            self.level_row.append(at)
            at += span >> level
        self.far_row = at
        for level in self.far:
            self.level_row.append(at)
            at += span >> level
        self.far_rows = -(-(at - self.far_row) // 8) * 8
        self.coarse_rows = self.far_row + NR
        self.slot, self.slot_len = [], []
        at = 0
        for level in range(self.top + 1):
            n = 2 * NR + max(self.chunk >> level, NR)
            self.slot.append(at)
            self.slot_len.append(n)
            at += n
        self.used = at
        self.slots = -(-at // LANES) * LANES
        self.far_slot = self.slot[self.near + 1]
        self.far_slots = self.slots - self.far_slot
        self.edge = NR * (self.near + 1)
        self.grad_rows = 4 * width + 2 * hidden
        self.parts = [(p * width, width) for p in range(self.grad_rows // width)]
        self.counts = [2, 2, rows // 4, seq]
        self.swap = rows // 4 == 2
        self.scatter = (width // rows) % (NR * seq) == 0


def sequence(*steps):
    for step in steps:
        step()


def layer_kernel(
    plan,
    tok_hbm, ids_ref, preg_ref, pres_ref, wq_hbm, qb_ref, wk_hbm, wv_hbm, vb_ref, wo_hbm, ob_ref,
    midg_ref, mids_ref, w1_hbm, inb_ref, w2_hbm, outb_ref, up_hbm,
    out_ref, gin_ref, red_ref, vout_ref,
    tok, up, wq, wk, wv, wo, w1, w2, n1, n2, mid, racc, dsec, first, second, qh, att, dah, dq,
    level, edge, halo, far_k, far_v, slots, bias, probs, dslots, own, hsend, hrecv, fsend, frecv,
    coarse, spread, dkv, grads, recv0, recv1, recv2, recv3, vstage, vrecv0, vrecv1, vrecv2, vrecv3, stats,
    inb,
    in_sem, halo_send, halo_recv, far_send, far_recv, back_send, back_recv, fback_send, fback_recv,
    rs_send, rs_recv, ag_send, ag_recv, vec_send, vec_recv,
):
    span, width, hidden = plan.span, plan.width, plan.hidden
    seq, near, top = plan.seq, plan.near, plan.top
    tile = hidden // w1.shape[0]
    tiles = w1.shape[0]
    pairs = width // LANES
    blocks = 2 * pairs
    id_at, value_at = pairs, pairs + 1
    far_rows = plan.far_rows
    row_id, seq_id = lax.axis_index("rows"), lax.axis_index("seq")
    start = seq_id * span

    core = row_id % 2
    if plan.swap:
        stride_a, stride_b = 2 + 2 * core, 4 - 2 * core
    else:
        stride_a, stride_b = 2, 4
    count = plan.counts
    index = [
        core,
        (row_id // stride_a) % count[1],
        (row_id // stride_b) % count[2],
        seq_id,
    ]

    def peer(digit, k):
        other = (index[digit] + k) % count[digit]
        if digit == 3:
            return other, (row_id, other)
        stride = [1, stride_a, stride_b][digit]
        return other, (row_id + (other - index[digit]) * stride, seq_id)

    def remote(src, dst, send, recv, device):
        return pltpu.make_async_remote_copy(
            src_ref=src, dst_ref=dst, send_sem=send, recv_sem=recv,
            device_id=device, device_id_type=MESH,
        )

    loads = []

    def load(src, dst):
        copy = pltpu.make_async_copy(src, dst, in_sem.at[len(loads)])
        copy.start()
        loads.append(copy)
        return copy

    load_tok = load(tok_hbm.at[0], tok)
    load_q = load(wq_hbm, wq)
    load_k = load(wk_hbm, wk)
    load_v = load(wv_hbm, wv)
    load_up = load(up_hbm.at[0], up)
    load_o = load(wo_hbm, wo)
    load_1 = [load(w1_hbm.at[:, t * tile : (t + 1) * tile], w1.at[t]) for t in range(tiles)]
    load_2 = load(w2_hbm, w2)

    halo[...] = jnp.zeros_like(halo)
    hrecv[...] = jnp.zeros_like(hrecv)
    far_k[...] = jnp.zeros_like(far_k)
    far_v[...] = jnp.zeros_like(far_v)
    frecv[...] = jnp.zeros_like(frecv)
    vstage[0] = jnp.zeros((VEC_ROWS, width), F32)
    for t in range(tiles):
        inb[t : t + 1, :] = inb_ref[t * tile : (t + 1) * tile].reshape(1, tile)

    barrier = pltpu.get_barrier_semaphore()
    greeted = 0
    for digit in range(4):
        for k in range(1, count[digit]):
            _, device = peer(digit, k)
            pl.semaphore_signal(barrier, inc=1, device_id=device, device_id_type=MESH)
            greeted += 1

    vectors = (preg_ref, pres_ref, qb_ref, vb_ref, ob_ref, midg_ref, mids_ref, outb_ref)

    def vec(row):
        return vectors[row][...].reshape(1, width)

    load_tok.wait()
    x = tok[...].astype(F32)
    center = x - mean(x)
    rstd = lax.rsqrt(mean(center * center) + EPSILON)
    normed = center * rstd
    n1[...] = normed
    stats[0] = jnp.broadcast_to(rstd, (span, LANES))
    first[...] = (normed * vec(0) + vec(1)).astype(BF16)
    def averaging(rows_dim):
        shape = (plan.coarse_rows, span) if rows_dim == 0 else (span, plan.coarse_rows)
        r, p = iota(shape, rows_dim), iota(shape, 1 - rows_dim)
        matrix = jnp.zeros(shape, F32)
        for lv in range(1, top + 1):
            at = plan.level_row[lv]
            hit = (r - at == (p >> lv)) & (r >= at) & (r < at + (span >> lv))
            matrix = jnp.where(hit, 0.5**lv, matrix)
        return matrix.astype(BF16)

    def level_start(lv):
        return 0 if lv == 0 else span + plan.level_row[lv]

    far_at = plan.far_row

    def fill(at, fresh, coarser):
        for b in range(fresh.shape[1] // LANES):
            cols = slice(b * LANES, (b + 1) * LANES)
            level[at + b, :span] = fresh[:, cols]
            level[at + b, span : span + far_at] = coarser[:far_at, cols]

    def cut_edges(first_block, last_block):
        for lv in range(near + 1):
            at, n = level_start(lv), span >> lv
            to = slice(lv * NR, (lv + 1) * NR)
            edge[0, first_block:last_block, to] = level[first_block:last_block, at : at + NR]
            edge[1, first_block:last_block, to] = level[first_block:last_block, at + n - NR : at + n]

    def apart(other):
        return (other - seq_id > 1) | (other - seq_id < -1)

    class Halo:
        def __init__(self, src, dst, send, recv, blocks_sent=None):
            self.sems = send, recv
            self.src, self.dst, self.sent = src, dst, blocks_sent

        def copy(self, from_side, to_side, recv_side, step):
            send, recv = self.sems
            src, dst = self.src.at[from_side], self.dst.at[to_side]
            if self.sent is not None:
                src, dst = (
                    self.src.at[from_side, pl.ds(*self.sent)],
                    self.dst.at[to_side, pl.ds(*self.sent)],
                )
            return remote(
                src, dst, send.at[from_side], recv.at[recv_side], (row_id, seq_id + step)
            )

        def start(self):
            @pl.when(seq_id > 0)
            def _():
                self.copy(0, 1, 1, -1).start()

            @pl.when(seq_id < seq - 1)
            def _():
                self.copy(1, 0, 0, 1).start()

        def wait(self):
            @pl.when(seq_id > 0)
            def _():
                self.copy(0, 0, 0, -1).wait()

            @pl.when(seq_id < seq - 1)
            def _():
                self.copy(1, 1, 1, 1).wait()

    class Far:
        def __init__(self, src, dst, send, recv):
            self.src, self.dst, self.send, self.recv = src, dst, send, recv

        def copy(self, k):
            other, device = peer(3, k)
            return remote(
                self.src(other), self.dst(k), self.send.at[k - 1], self.recv.at[k - 1], device
            )

        def start(self):
            for k in range(1, seq):
                pl.when(apart(peer(3, k)[0]))(lambda: self.copy(k).start())

        def wait(self):
            for k in range(1, seq):
                pl.when(apart(peer(3, seq - k)[0]))(lambda: self.copy(k).wait_recv())
                pl.when(apart(peer(3, k)[0]))(lambda: self.copy(k).wait_send())

    key_halo = Halo(edge, halo, halo_send.at[0], halo_recv.at[0], (0, value_at))
    value_halo = Halo(edge, halo, halo_send.at[1], halo_recv.at[1], (value_at, pairs))
    key_far = Far(
        lambda other: far_k.at[seq_id], lambda k: far_k.at[seq_id], far_send.at[0], far_recv.at[0]
    )
    value_far = Far(
        lambda other: far_v.at[seq_id], lambda k: far_v.at[seq_id], far_send.at[1], far_recv.at[1]
    )

    matrix = averaging(0)
    load_k.wait()
    keys = dot(first[...], wk[...]).astype(BF16)
    mixed = dot(matrix, keys).astype(BF16)
    fill(0, keys, mixed)
    far_k[seq_id, :, :width] = mixed[far_at : far_at + far_rows]
    feature = (iota((LANES, span), 0) == ids_ref[...]).astype(F32).astype(BF16)
    unit = (iota((span, span), 0) == iota((span, span), 1)).astype(F32).astype(BF16)
    id_hot = dot_nt(unit, feature).astype(BF16)
    alike = dot(matrix, id_hot)
    alike = jnp.where((alike > 0.999) & (iota(alike.shape, 1) > 0), 1.0, 0.0).astype(BF16)
    fill(id_at, id_hot, alike)
    far_k[seq_id, :, width:] = alike[far_at : far_at + far_rows]
    cut_edges(0, value_at)

    pl.semaphore_wait(barrier, greeted)
    key_far.start()
    key_halo.start()

    load_v.wait()
    values = (dot(first[...], wv[...]) + vec(3)).astype(BF16)
    mixed = dot(matrix, values).astype(BF16)
    fill(value_at, values, mixed)
    far_v[seq_id] = mixed[far_at : far_at + far_rows]
    cut_edges(value_at, value_at + pairs)
    value_far.start()
    value_halo.start()

    load_q.wait()
    query = ((dot(first[...], wq[...]) + vec(2)).astype(BF16) * (1.0 / math.sqrt(HEAD_DIM))).astype(
        BF16
    )
    for b in range(pairs):
        qh[b] = query[:, b * LANES : (b + 1) * LANES]

    def slot_pieces(c):
        pieces = []
        for lv in range(near + 1):
            at, n = level_start(lv), span >> lv
            per = plan.chunk >> lv
            s0 = plan.slot[lv]
            if per >= NR:
                low, high = c * per - NR, c * per + per + NR
            else:
                low, high = -NR, n + NR
            if low < 0:
                pieces.append((s0, "low", lv * NR, NR))
                s0, low = s0 + NR, 0
            inner = min(high, n)
            pieces.append((s0, "own", at + low, inner - low))
            s0 += inner - low
            if high > n:
                pieces.append((s0, "high", lv * NR, NR))
        return pieces

    slot_at = iota((1, plan.slots), 1)
    slot_level = jnp.zeros((1, plan.slots), jnp.int32)
    for lv in range(1, top + 1):
        slot_level = slot_level + (slot_at >= plan.slot[lv]).astype(jnp.int32)
    for c in range(plan.chunks):
        origin = start + c * plan.chunk
        j = slot_at
        for lv in range(top + 1):
            if (plan.chunk >> lv) >= NR:
                base = origin // (1 << lv) - NR
            else:
                base = (origin // (NR << lv) - 1) * NR
            here = slot_at - plan.slot[lv] + base
            j = here if lv == 0 else jnp.where(slot_level == lv, here, j)
        position = origin + iota((plan.chunk, plan.slots), 0)
        off_block = (j >> 4) - (position >> (slot_level + 4))
        off_half = (j >> 3) - (position >> (slot_level + 3))
        reach = jnp.where(slot_level == 0, -1, 1)
        within = (jnp.abs(off_block) <= 1) & (jnp.abs(off_half) > reach)
        bias[c] = jnp.where(within, slot_level.astype(F32) * LOG_TWO, MASKED)

    def far_select():
        pieces = []
        for lv in plan.far:
            per_log = (span >> lv).bit_length() - 1
            first_row = plan.level_row[lv] - plan.far_row
            j = (start // (NR << lv) - 1) * NR + iota((3 * NR, seq * far_rows), 0)
            column = (j >> per_log) * far_rows + (j & ((1 << per_log) - 1)) + first_row
            pieces.append((column == iota((3 * NR, seq * far_rows), 1)).astype(F32))
        rest = plan.far_slots - 3 * NR * len(plan.far)
        if rest:
            pieces.append(jnp.zeros((rest, seq * far_rows), F32))
        return jnp.concatenate(pieces, axis=0).astype(BF16)

    select = far_select()
    spread[...] = averaging(1)

    def fill_slots(first_block, n_blocks, far_values):
        those = slice(first_block, first_block + n_blocks)
        for c in range(plan.chunks):
            for s0, kind, at, n in slot_pieces(c):
                if kind == "own":
                    slots[c, those, s0 : s0 + n] = level[those, at : at + n]
                else:
                    slots[c, those, s0 : s0 + n] = halo[
                        0 if kind == "low" else 1, those, at : at + n
                    ]
            for b in range(n_blocks):
                slots[c, first_block + b, plan.far_slot :] = far_values[
                    :, b * LANES : (b + 1) * LANES
                ]

    key_halo.wait()
    key_far.wait()
    fill_slots(
        0, value_at, dot(select, far_k[...].reshape(seq * far_rows, width + LANES)).astype(BF16)
    )
    for c in range(plan.chunks):
        same = dot_nt(level[id_at, c * plan.chunk : (c + 1) * plan.chunk], slots[c, id_at])
        bias[c] = jnp.where(same > 0.5, bias[c], MASKED)

    lane = iota((1, LANES), 1)
    low_half = (lane < HEAD_DIM).astype(F32).astype(BF16)
    high_half = (lane >= HEAD_DIM).astype(F32).astype(BF16)
    low_lanes = iota((plan.chunk, LANES), 1) < HEAD_DIM

    def two_heads(block):
        return jnp.concatenate([block * low_half, block * high_half], axis=0)

    def merge_heads(both):
        return jnp.where(low_lanes, both[: plan.chunk], both[plan.chunk :])

    def chunk_rows(c):
        return pl.ds(pl.multiple_of(c * plan.chunk, plan.chunk), plan.chunk)

    def pair_lanes(b):
        return pl.ds(pl.multiple_of(b * LANES, LANES), LANES)

    def attend(i, carry):
        c, b = i // pairs, i % pairs
        q2 = two_heads(qh[b, chunk_rows(c)])
        offset = bias[c]
        score = dot_nt(q2, slots[c, b]) + jnp.concatenate([offset, offset], axis=0)
        peak = jnp.max(score, axis=1, keepdims=True)
        raised = jnp.exp(score - peak)
        prob = raised * (1.0 / jnp.sum(raised, axis=1, keepdims=True))
        probs[i] = prob.astype(BF16)
        return carry

    lax.fori_loop(0, plan.chunks * pairs, attend, 0, unroll=2)

    value_halo.wait()
    value_far.wait()
    fill_slots(
        value_at, pairs, dot(select, far_v[...].reshape(seq * far_rows, width)).astype(BF16)
    )

    def mix(i, carry):
        c, b = i // pairs, i % pairs
        both = dot(probs[i], slots[c, value_at + b])
        att[chunk_rows(c), pair_lanes(b)] = merge_heads(both).astype(BF16)
        return carry

    lax.fori_loop(0, plan.chunks * pairs, mix, 0, unroll=2)

    received = [recv0, recv1, recv2, recv3]

    def region(part, digits):
        n = plan.parts[0][1]
        base = part * n
        for digit in range(digits):
            n = n // count[digit]
            base = base + index[digit] * n
        return base, n

    def rows_at(base, n):
        return pl.ds(pl.multiple_of(base, NR), n)

    def received_rows(part, n):
        return rows_at(part * n, n)

    def rs_copy(part, digit, k):
        base, n = region(part, digit)
        other, device = peer(digit, k)
        if digit == 3 and not plan.scatter:
            return remote(
                grads.at[rows_at(base, n)],
                received[digit].at[k - 1, received_rows(part, n)],
                rs_send.at[part, digit, k - 1], rs_recv.at[part, digit, k - 1], device,
            )
        n = n // count[digit]
        return remote(
            grads.at[rows_at(base + other * n, n)],
            received[digit].at[k - 1, received_rows(part, n)],
            rs_send.at[part, digit, k - 1], rs_recv.at[part, digit, k - 1], device,
        )

    def rs_start(part, digit):
        for k in range(1, count[digit]):
            rs_copy(part, digit, k).start()

    def rs_finish(part, digit):
        for k in range(1, count[digit]):
            rs_copy(part, digit, k).wait()
        gather_all = digit == 3 and not plan.scatter
        base, n = region(part, digit if gather_all else digit + 1)
        at = part * n
        target = red_ref if digit == 3 else grads
        block = 64 if n % 64 == 0 else NR

        def add(i, carry):
            here = rows_at(base + i * block, block)
            there = pl.ds(pl.multiple_of(at + i * block, NR), block)
            if gather_all:
                acc = jnp.zeros((block, width), F32)
                for s in range(seq):
                    slot = (seq_id - s + seq - 1) % seq
                    theirs = received[digit][jnp.minimum(slot, seq - 2), there].astype(F32)
                    acc = acc + jnp.where(seq_id == s, grads[here].astype(F32), theirs)
            else:
                acc = grads[here].astype(F32)
                for k in range(1, count[digit]):
                    acc = acc + received[digit][k - 1, there].astype(F32)
            target[here] = acc.astype(BF16)
            return carry

        lax.fori_loop(0, n // block, add, 0)

    def ag_copy(part, digit, k):
        base, n = region(part, digit + 1)
        _, device = peer(digit, k)
        return remote(
            red_ref.at[rows_at(base, n)], red_ref.at[rows_at(base, n)],
            ag_send.at[part, digit, k - 1], ag_recv.at[part, digit, k - 1], device,
        )

    def ag_start(part, digit):
        if digit == 3 and not plan.scatter:
            return
        for k in range(1, count[digit]):
            ag_copy(part, digit, k).start()

    def ag_finish(part, digit):
        if digit == 3 and not plan.scatter:
            return
        for k in range(1, count[digit]):
            ag_copy(part, digit, k).wait()

    def part_steps(part):
        steps = [functools.partial(rs_start, part, 0)]
        for digit in range(1, 4):
            steps.append(
                functools.partial(
                    sequence,
                    functools.partial(rs_finish, part, digit - 1),
                    functools.partial(rs_start, part, digit),
                )
            )
        steps.append(
            functools.partial(
                sequence, functools.partial(rs_finish, part, 3), functools.partial(ag_start, part, 3)
            )
        )
        for digit in (2, 1, 0):
            steps.append(
                functools.partial(
                    sequence,
                    functools.partial(ag_finish, part, digit + 1),
                    functools.partial(ag_start, part, digit),
                )
            )
        steps.append(functools.partial(ag_finish, part, 0))
        return steps

    all_steps = [part_steps(part) for part in range(len(plan.parts))]

    def step(part, number):
        all_steps[part][number]()

    at_place = {}
    reached_step = [0] * (len(plan.parts) + 1)
    for place, parts_here in ORDER.items():
        at_place[place] = []
        for part in parts_here:
            reached_step[part] += 1
            at_place[place].append((part, reached_step[part]))

    def advance(place):
        for part, number in at_place.get(place, ()):
            if part < 0:
                vec_finish(number - 1)
                if number < 4:
                    vec_start(number)
            else:
                step(part, number)

    load_o.wait()
    load_up.wait()
    res = tok[...].astype(F32) + dot(att[...], wo[...]) + vec(4)
    mid[...] = res
    center = res - mean(res)
    rstd = lax.rsqrt(mean(center * center) + EPSILON)
    normed = center * rstd
    n2[...] = normed
    stats[1] = jnp.broadcast_to(rstd, (span, LANES))
    second[...] = (normed * vec(5) + vec(6)).astype(BF16)
    racc[...] = jnp.zeros_like(racc)
    dsec[...] = jnp.zeros_like(dsec)
    for copy in load_1:
        copy.wait()
    load_2.wait()
    curve = math.sqrt(2.0 / math.pi)

    def feed(t, carry):
        w2_rows = pl.ds(pl.multiple_of(t * tile, tile), tile)
        pre = dot(second[...], w1[t]) + inb[pl.ds(t, 1), :]
        square = pre * pre
        bend = jnp.tanh(curve * (pre + 0.044715 * (square * pre)))
        half = 0.5 * (1.0 + bend)
        act = (pre * half).astype(BF16)
        slope = half + 0.5 * pre * (1.0 - bend * bend) * (curve * (1.0 + 3 * 0.044715 * square))
        upstream = up[...]
        racc[...] += dot(act, w2[w2_rows])
        d_pre = (dot_nt(upstream, w2[w2_rows]) * slope).astype(BF16)
        base = 2 * t * tile
        grads[rows_at(base, tile)] = dot_tn(act, upstream).astype(BF16)
        grads[rows_at(base + tile, tile)] = dot_tn(second[...], d_pre).astype(BF16)
        rs_start(2 * t, 0)
        rs_start(2 * t + 1, 0)
        vstage[0, pl.ds(V_INNB + t, 1), :] = total(d_pre.astype(F32))
        dsec[...] += dot_nt(d_pre, w1[t])

        for when in range(tiles):
            if f"f{when}" in ORDER:
                pl.when(t == when)(functools.partial(advance, f"f{when}"))

        return carry

    lax.fori_loop(0, tiles, feed, 0)
    out_ref[0] = (mid[...] + racc[...] + vec(7)).astype(BF16)

    up_f = up[...].astype(F32)
    vstage[0, V_OUTB : V_OUTB + 1] = total(up_f)
    d_second, normed = dsec[...], n2[...]
    scaled = d_second * vec(5)
    vstage[0, V_MIDG : V_MIDG + 1] = total(d_second * normed)
    vstage[0, V_MIDS : V_MIDS + 1] = total(d_second)
    d_mid = up_f + (scaled - mean(scaled) - normed * mean(scaled * normed)) * stats[1][:, :1]
    mid[...] = d_mid
    d_branch = d_mid.astype(BF16)
    vstage[0, V_OB : V_OB + 1] = total(d_branch.astype(F32))
    grads[2 * hidden : 2 * hidden + width] = dot_tn(att[...], d_branch).astype(BF16)
    rs_start(2 * tiles, 0)
    advance("ln2")
    d_att = dot_nt(d_branch, wo[...]).astype(BF16)
    for b in range(pairs):
        dah[b] = d_att[:, b * LANES : (b + 1) * LANES]

    def attend_back(i, carry):
        c, b = i // pairs, i % pairs
        q2 = two_heads(qh[b, chunk_rows(c)])
        g2 = two_heads(dah[b, chunk_rows(c)])
        low = probs[i]
        prob = low.astype(F32)
        d_prob = dot_nt(g2, slots[c, value_at + b])
        weighted = prob * d_prob
        d_score = (weighted - prob * jnp.sum(weighted, axis=1, keepdims=True)).astype(BF16)
        d_query = merge_heads(dot(d_score, slots[c, b])) * (1.0 / math.sqrt(HEAD_DIM))
        dq[chunk_rows(c), pair_lanes(b)] = d_query.astype(BF16)
        dslots[c, b] = dot_tn(d_score, q2)
        dslots[c, pairs + b] = dot_tn(low, g2)
        for when in range(plan.chunks * pairs):
            if f"b{when}" in ORDER:
                pl.when(i == when)(functools.partial(advance, f"b{when}"))

        return carry

    lax.fori_loop(0, plan.chunks * pairs, attend_back, 0)

    def fold(b, carry):
        for c in range(plan.chunks):
            for s0, kind, at, n in slot_pieces(c):
                piece = dslots[c, b, s0 : s0 + n]
                if kind == "own":
                    parts_done = own_done[c].get((s0, at))
                    seen = parts_done if parts_done is not None else 0
                    if seen:
                        own[b, at : at + seen] += piece[:seen]
                    if seen < n:
                        own[b, at + seen : at + n] = piece[seen:]
                elif own_done[c].get((s0, kind)):
                    side = 0 if kind == "low" else 1
                    hsend[side, b, at : at + n] = (
                        hsend[side, b, at : at + n].astype(F32) + piece
                    ).astype(BF16)
                else:
                    side = 0 if kind == "low" else 1
                    hsend[side, b, at : at + n] = piece.astype(BF16)
        far = dslots[0, b, plan.far_slot :]
        for c in range(1, plan.chunks):
            far = far + dslots[c, b, plan.far_slot :]
        back = dot_tn(select, far.astype(BF16))
        for s in range(seq):
            fsend[s, b] = back[s * far_rows : (s + 1) * far_rows].astype(BF16)
        return carry

    own_done = []
    reached, halo_seen = {}, set()
    for c in range(plan.chunks):
        done = {}
        for s0, kind, at, n in slot_pieces(c):
            if kind == "own":
                lv = max(v for v in range(near + 1) if level_start(v) <= at)
                limit = reached.get(lv, level_start(lv))
                done[(s0, at)] = max(0, min(limit, at + n) - at)
                reached[lv] = max(limit, at + n)
            else:
                done[(s0, kind)] = (kind, at) in halo_seen
                halo_seen.add((kind, at))
        own_done.append(done)

    lax.fori_loop(0, blocks, fold, 0)

    back_halo = Halo(hsend, hrecv, back_send, back_recv)
    back_far = Far(
        lambda other: fsend.at[other], lambda k: frecv.at[k - 1], fback_send, fback_recv
    )
    back_far.start()
    back_halo.start()
    advance("fold")

    d_query = dq[...]
    vstage[0, V_QB : V_QB + 1] = total(d_query.astype(F32))
    off_c = 2 * hidden + width
    grads[off_c : off_c + width] = dot_tn(first[...], d_query).astype(BF16)
    d_first = dot_nt(d_query, wq[...])
    racc[...] = d_first
    rs_start(2 * tiles + 1, 0)
    advance("q")

    back_halo.wait()
    back_far.wait()
    for lv in range(near + 1):
        at, n = level_start(lv), span >> lv
        lo, hi = lv * NR, (lv + 1) * NR
        own[:, at : at + NR] += hrecv[0, :, lo:hi].astype(F32)
        own[:, at + n - NR : at + n] += hrecv[1, :, lo:hi].astype(F32)
    far_sum = fsend[seq_id].astype(F32)
    for k in range(1, seq):
        far_sum = far_sum + frecv[k - 1].astype(F32)
    coarse[far_at:] = jnp.zeros((plan.coarse_rows - far_at, 2 * width), BF16)
    for b in range(blocks):
        cols = slice(b * LANES, (b + 1) * LANES)
        coarse[:far_at, cols] = own[b, span : span + far_at].astype(BF16)
        coarse[far_at : far_at + far_rows, cols] = far_sum[b].astype(BF16)
    for half in range(2):
        passed = dot(spread[...], coarse[:, half * width : (half + 1) * width])
        for b in range(pairs):
            cols = slice((half * pairs + b) * LANES, (half * pairs + b + 1) * LANES)
            dkv[:, cols] = (
                own[half * pairs + b, :span] + passed[:, b * LANES : (b + 1) * LANES]
            ).astype(BF16)
    d_keys, d_values = dkv[:, :width], dkv[:, width:]
    vstage[0, V_VB : V_VB + 1] = total(d_values.astype(F32))
    grads[off_c + width : off_c + 2 * width] = dot_tn(first[...], d_keys).astype(BF16)
    grads[off_c + 2 * width : off_c + 3 * width] = dot_tn(first[...], d_values).astype(BF16)
    rs_start(2 * tiles + 2, 0)
    rs_start(2 * tiles + 3, 0)
    advance("dkv")
    d_first = racc[...] + dot_nt(d_keys, wk[...]) + dot_nt(d_values, wv[...])
    normed = n1[...]
    scaled = d_first * vec(0)
    vstage[0, V_PREG : V_PREG + 1] = total(d_first * normed)
    vstage[0, V_PRES : V_PRES + 1] = total(d_first)
    d_in = mid[...] + (scaled - mean(scaled) - normed * mean(scaled * normed)) * stats[0][:, :1]
    gin_ref[0] = d_in.astype(BF16)

    vec_received = [vrecv0, vrecv1, vrecv2, vrecv3]

    def vec_copy(digit, k):
        _, device = peer(digit, k)
        return remote(
            vstage.at[digit], vec_received[digit].at[index[digit]],
            vec_send.at[digit, k - 1], vec_recv.at[digit, k - 1], device,
        )

    def vec_start(digit):
        for k in range(1, count[digit]):
            vec_copy(digit, k).start()

    def vec_finish(digit):
        for k in range(1, count[digit]):
            vec_copy(digit, k).wait()
        acc = jnp.zeros((VEC_ROWS, width), F32)
        for s in range(count[digit]):
            acc = acc + jnp.where(index[digit] == s, vstage[digit], vec_received[digit][s])
        if digit == 3:
            vout_ref[...] = acc
        else:
            vstage[digit + 1] = acc

    vec_start(0)
    advance("ln1")


def unpack_kernel(
    width, tiles, red_ref, vec_ref, out_in, gin_in,
    query_ref, key_ref, value_ref, output_ref, inner_ref, outer_ref,
    preg_ref, pres_ref, qb_ref, vb_ref, ob_ref, midg_ref, mids_ref, outb_ref, innb_ref,
    out_ref, gin_ref, wide, out_sem, through_sem,
):
    targets = []
    for t in range(tiles):
        rows = slice(t * width, (t + 1) * width)
        targets.append(outer_ref.at[rows])
        targets.append(inner_ref.at[:, rows])
    targets += [output_ref, query_ref, key_ref, value_ref]

    def put(i):
        return pltpu.make_async_copy(wide.at[i], targets[i], out_sem.at[i])

    def give(i):
        return pltpu.make_async_copy(
            (out_in, gin_in)[i], (out_ref, gin_ref)[i], through_sem.at[i]
        )

    for i in range(2):
        give(i).start()
    for i in range(len(targets)):
        wide[i] = red_ref[i * width : (i + 1) * width].astype(F32)
        put(i).start()
    for row, ref in (
        (V_PREG, preg_ref), (V_PRES, pres_ref), (V_QB, qb_ref), (V_VB, vb_ref), (V_OB, ob_ref),
        (V_MIDG, midg_ref), (V_MIDS, mids_ref), (V_OUTB, outb_ref),
    ):
        ref[...] = vec_ref[row]
    for t in range(tiles):
        innb_ref[t * width : (t + 1) * width] = vec_ref[V_INNB + t]
    for i in range(len(targets)):
        put(i).wait()
    for i in range(2):
        give(i).wait()


def shards(
    rows, seq,
    tokens, segment_ids, prenorm_gain, prenorm_shift, query_proj, query_bias, key_proj, value_proj,
    value_bias, output_proj, output_bias, midnorm_gain, midnorm_shift, inner_proj, inner_bias,
    outer_proj, outer_bias, upstream,
):
    _, span, width = tokens.shape
    hidden = inner_proj.shape[1]
    plan = Plan(rows, seq, span, width, hidden)
    tiles = hidden // width
    pairs = width // LANES
    count = plan.counts
    most = max(count) - 1
    vmem = pl.BlockSpec(memory_space=pltpu.VMEM)
    hbm = pl.BlockSpec(memory_space=pl.ANY)
    grad_rows = plan.grad_rows
    rest = [grad_rows // 2, grad_rows // 4, grad_rows // 4 // count[2]]
    last = rest[2] // seq if plan.scatter else rest[2]
    dma = pltpu.SemaphoreType.DMA
    items = plan.chunks * pairs
    n_parts = len(plan.parts)
    scratch = [
        pltpu.VMEM((span, width), BF16),
        pltpu.VMEM((span, width), BF16),
        pltpu.VMEM((width, width), BF16),
        pltpu.VMEM((width, width), BF16),
        pltpu.VMEM((width, width), BF16),
        pltpu.VMEM((width, width), BF16),
        pltpu.VMEM((tiles, width, width), BF16),
        pltpu.VMEM((hidden, width), BF16),
        pltpu.VMEM((span, width), F32),
        pltpu.VMEM((span, width), F32),
        pltpu.VMEM((span, width), F32),
        pltpu.VMEM((span, width), F32),
        pltpu.VMEM((span, width), F32),
        pltpu.VMEM((span, width), BF16),
        pltpu.VMEM((span, width), BF16),
        pltpu.VMEM((pairs, span, LANES), BF16),
        pltpu.VMEM((span, width), BF16),
        pltpu.VMEM((pairs, span, LANES), BF16),
        pltpu.VMEM((span, width), BF16),
        pltpu.VMEM((2 * pairs + 1, span + plan.far_row, LANES), BF16),
        pltpu.VMEM((2, 2 * pairs + 1, plan.edge, LANES), BF16),
        pltpu.VMEM((2, 2 * pairs + 1, plan.edge, LANES), BF16),
        pltpu.VMEM((seq, plan.far_rows, width + LANES), BF16),
        pltpu.VMEM((seq, plan.far_rows, width), BF16),
        pltpu.VMEM((plan.chunks, 2 * pairs + 1, plan.slots, LANES), BF16),
        pltpu.VMEM((plan.chunks, plan.chunk, plan.slots), F32),
        pltpu.VMEM((items, 2 * plan.chunk, plan.slots), BF16),
        pltpu.VMEM((plan.chunks, 2 * pairs, plan.slots, LANES), F32),
        pltpu.VMEM((2 * pairs, span + plan.far_row, LANES), F32),
        pltpu.VMEM((2, 2 * pairs, plan.edge, LANES), BF16),
        pltpu.VMEM((2, 2 * pairs, plan.edge, LANES), BF16),
        pltpu.VMEM((seq, 2 * pairs, plan.far_rows, LANES), BF16),
        pltpu.VMEM((seq - 1, 2 * pairs, plan.far_rows, LANES), BF16),
        pltpu.VMEM((plan.coarse_rows, 2 * width), BF16),
        pltpu.VMEM((span, plan.coarse_rows), BF16),
        pltpu.VMEM((span, 2 * width), BF16),
        pltpu.VMEM((grad_rows, width), BF16),
        pltpu.VMEM((count[0] - 1, rest[0], width), BF16),
        pltpu.VMEM((count[1] - 1, rest[1], width), BF16),
        pltpu.VMEM((count[2] - 1, rest[2], width), BF16),
        pltpu.VMEM((count[3] - 1, last, width), BF16),
        pltpu.VMEM((4, VEC_ROWS, width), F32),
        pltpu.VMEM((count[0], VEC_ROWS, width), F32),
        pltpu.VMEM((count[1], VEC_ROWS, width), F32),
        pltpu.VMEM((count[2], VEC_ROWS, width), F32),
        pltpu.VMEM((count[3], VEC_ROWS, width), F32),
        pltpu.VMEM((2, span, LANES), F32),
        pltpu.VMEM((tiles, width), F32),
        dma((7 + tiles,)),
        dma((2, 2)), dma((2, 2)),
        dma((2, seq - 1)), dma((2, seq - 1)),
        dma((2,)), dma((2,)),
        dma((seq - 1,)), dma((seq - 1,)),
        dma((n_parts, 4, most)), dma((n_parts, 4, most)),
        dma((n_parts, 4, most)), dma((n_parts, 4, most)),
        dma((4, most)), dma((4, most)),
    ]
    layer_output, input_grad, reduced, vecs = pl.pallas_call(
        functools.partial(layer_kernel, plan),
        out_shape=(
            pltpu.VMEM(tokens.shape, BF16),
            pltpu.VMEM(tokens.shape, BF16),
            pltpu.VMEM((grad_rows, width), BF16),
            pltpu.VMEM((VEC_ROWS, width), F32),
        ),
        in_specs=[
            hbm, vmem, vmem, vmem, hbm, vmem, hbm, hbm, vmem, hbm, vmem, vmem, vmem, hbm, vmem, hbm,
            vmem, hbm,
        ],
        out_specs=(vmem, vmem, vmem, vmem),
        scratch_shapes=scratch,
        compiler_params=pltpu.CompilerParams(
            collective_id=0, has_side_effects=True, vmem_limit_bytes=50 * 1024 * 1024
        ),
        name="layer",
    )(
        tokens, segment_ids, prenorm_gain, prenorm_shift, query_proj, query_bias, key_proj,
        value_proj, value_bias, output_proj, output_bias, midnorm_gain, midnorm_shift, inner_proj,
        inner_bias, outer_proj, outer_bias, upstream,
    )
    matrix = jax.ShapeDtypeStruct((width, width), F32)
    vector = jax.ShapeDtypeStruct((width,), F32)
    grads = pl.pallas_call(
        functools.partial(unpack_kernel, width, tiles),
        out_shape=(
            matrix, matrix, matrix, matrix,
            jax.ShapeDtypeStruct((width, hidden), F32),
            jax.ShapeDtypeStruct((hidden, width), F32),
            vector, vector, vector, vector, vector, vector, vector, vector,
            jax.ShapeDtypeStruct((hidden,), F32),
            jax.ShapeDtypeStruct(tokens.shape, BF16),
            jax.ShapeDtypeStruct(tokens.shape, BF16),
        ),
        in_specs=[vmem] * 4,
        out_specs=(hbm,) * 6 + (vmem,) * 9 + (hbm,) * 2,
        scratch_shapes=[
            pltpu.VMEM((n_parts, width, width), F32),
            dma((n_parts,)), dma((2,)),
        ],
        compiler_params=pltpu.CompilerParams(vmem_limit_bytes=24 * 1024 * 1024),
        name="unpack",
    )(reduced, vecs, layer_output, input_grad)
    (query_g, key_g, value_g, output_g, inner_g, outer_g,
     preg, pres, qb, vb, ob, midg, mids, outb, innb, layer_output, input_grad) = grads
    return (
        layer_output, input_grad, preg, pres, query_g, qb, key_g, value_g, vb, output_g, ob,
        midg, mids, inner_g, innb, outer_g, outb,
    )


def solution(mesh):
    split, ids, whole = P("rows", "seq", None), P("rows", "seq"), P()
    in_specs = (split, ids) + (whole,) * 15 + (split,)
    out_specs = (split, split) + (whole,) * 15
    return jax.shard_map(
        functools.partial(shards, mesh.shape["rows"], mesh.shape["seq"]),
        mesh=mesh, in_specs=in_specs, out_specs=out_specs, check_vma=False,
    )
```
